32 devices in a mesh: section: 4 (over y, x), expert: 8 (over z, core).
Axes of the slice: x: 2, y: 2, z: 4, core: 2. Of those that a mesh axis runs over, the one named last changes fastest.
Arguments:
- section_inputs: float32 [4, 1024, 2048], P('section', 'expert'), may hold values from -6 to 6
- stored_inputs: float32 [4, 1024, 2048], P('section', 'expert'), may hold values from -6 to 6
- out_grads: bfloat16 [4, 1024, 2048], P('section', 'expert'), may hold values from -6 to 6
- fwd_routes: int32 [4, 1024, 2], P('section', 'expert'), may hold values from 0 to 3, all different within a row; in each aligned block of 128 rows (0 to 127, 128 to 255, ..., all dimensions but the last counted through in order) at most 80 rows name the same one
- fwd_gates: float32 [4, 1024, 2], P('section', 'expert'), may hold values from 0.2 to 1
- fwd_modulation: float32 [4, 3, 2048], P('section'), may hold values from -3 to 3
- bwd_routes: int32 [4, 1024, 2], P('section', 'expert'), may hold values from 0 to 3, all different within a row; in each aligned block of 128 rows (0 to 127, 128 to 255, ..., all dimensions but the last counted through in order) at most 80 rows name the same one
- bwd_gates: float32 [4, 1024, 2], P('section', 'expert'), may hold values from 0.2 to 1
- bwd_modulation: float32 [4, 3, 2048], P('section'), may hold values from -3 to 3
- up_weight: bfloat16 [4, 8, 2048, 1024], P('section', 'expert'), may hold values from -0.125 to 0.125
- down_weight: bfloat16 [4, 8, 1024, 2048], P('section', 'expert'), may hold values from -0.125 to 0.125
Outputs:
- next_inputs: float32 [4, 1024, 2048], P('section', 'expert')
- input_grads: bfloat16 [4, 1024, 2048], P('section', 'expert')
The draws below stay inside these ranges and needn't reach their ends.
Inputs may be any that keep to these rules, and one draw needn't show every extreme that they name: `fwd_routes`: A token names two different experts. In the rows of one index of expert (aligned blocks of 128 rows of a section) no expert is named more than 80 times, a bound that some block reaches. `bwd_routes`: A token names two different experts. In the rows of one index of expert (aligned blocks of 128 rows of a section) no expert is named more than 80 times, a bound that some block reaches.
All inputs are finite; a program needn't handle non-finite values.
Results may differ from the reference program's by a relative error of at most 0.0042.
Values may be sent and summed in bfloat16 or wider, within the bound.
A program may use at most 128 MiB of HBM per device.

```python
import math
import jax
import jax.numpy as jnp
import numpy as np
from jax import lax

D = 2048
FF = 2048
FF_DEV = 1024
TOK_DEV = 128
TOKENS = 1024
EXPERTS = 4
CAP = 80
N_SECTION = 4
N_EXPERT = 8


def levels(rng, dims, split, smallest, top_value):
    def one(position, shards_of):
        draws = jax.random.uniform(jax.random.fold_in(jax.random.fold_in(rng, 6), position), (shards_of,), jnp.float32, smallest / len(split), top_value / len(split))
        return jnp.repeat(jnp.exp(draws), dims[position] // shards_of).reshape((-1,) + (1,) * (len(dims) - position - 1))

    gain = one(*split[0])
    for cut in split[1:]:
        gain = gain * one(*cut)
    return gain


def routed_block(key, own, number, rows, number_of, top, limit, lean):
    ranking = jax.random.permutation(key, number_of)
    crowded, ordinary = load_shares(number_of, rows * top, limit, lean, True), load_shares(number_of, rows * top, limit, lean, False)
    places = jnp.arange(number_of)

    def named(tallies, turn):
        used = int((tallies > 0).sum())
        fixed = max(1, used // 4)
        passed = fixed + (places - fixed + turn * (used - fixed)) % max(1, number_of - fixed)
        return jnp.zeros((number_of,), jnp.int32).at[ranking[jnp.where(places < fixed, places, passed)]].set(jnp.asarray(tallies, jnp.int32))

    tallies = jnp.where(number % 4 == 0, named(crowded, number // 4), named(ordinary, number - number // 4 - 1))
    mixed = jax.random.permutation(jax.random.fold_in(own, 3), number_of)
    giver, receiver = mixed[0:number_of // 2 * 2:2], mixed[1:number_of // 2 * 2:2]
    slack = jnp.minimum(tallies[giver] - 1, limit - tallies[receiver]) // 2
    slack = jnp.where((giver == ranking[0]) | (receiver == ranking[0]) | (tallies[receiver] == 0), 0, jnp.maximum(slack, 0))
    passed = jax.random.randint(jax.random.fold_in(own, 4), (number_of // 2,), 0, 1 << 20) % (slack + 1)
    tallies = tallies.at[giver].add(-passed).at[receiver].add(passed)
    items = jnp.searchsorted(jnp.cumsum(tallies), jnp.arange(rows * top), side="right").astype(jnp.int32)
    table = items.reshape(top, rows).T
    table = table[jax.random.permutation(jax.random.fold_in(own, 1), rows)]
    turn = jax.random.randint(jax.random.fold_in(own, 2), (rows, 1), 0, top)
    return jnp.take_along_axis(table, (jnp.arange(top)[None, :] + turn) % top, axis=1)


def load_shares(count, total, most, slope, full):
    weights = [(1 << 20) // math.isqrt(standing ** slope) + 1 for standing in range(1, count + 1)]
    largest = most if full else min(most, max(-(-total // count), total * weights[0] // sum(weights)))
    least = 1 if total - largest >= count - 1 else 0
    counts, rest = [largest] + [least] * (count - 1), total - largest - least * (count - 1)
    while rest > 0:
        movable = [i for i in range(1, count) if counts[i] < largest] or [i for i in range(1, count) if counts[i] < most]
        whole, remaining = sum([weights[i] for i in movable]), rest
        for i in movable:
            more = min(most - counts[i], max(1, remaining * weights[i] // whole), rest)
            counts[i] = counts[i] + more
            rest = rest - more
    return np.array(counts)


def normal_values(stream_key, dims, width, most, split=(), held_as=jnp.bfloat16):
    drawn = width * jax.random.normal(stream_key, dims, jnp.float32)
    if split:
        drawn = drawn * levels(stream_key, dims, split, -0.22, 0.18)
    return jnp.clip(drawn, -most, most).astype(held_as)


def setup_inputs(seed: int = 0) -> dict:
    keys = jax.random.split(jax.random.key(seed), 12)
    section_inputs = normal_values(keys[0], (N_SECTION, TOKENS, D), 1.0, 6.0, ((0, 4), (1, 8)), jnp.float32)
    stored_inputs = normal_values(keys[1], (N_SECTION, TOKENS, D), 1.0, 6.0, ((0, 4), (1, 8)), jnp.float32)
    out_grads = normal_values(keys[2], (N_SECTION, TOKENS, D), 1.0, 6.0, ((0, 4), (1, 8)))
    fwd_routes_keys = jax.random.split(jax.random.fold_in(keys[3], 1), N_SECTION * TOKENS // TOK_DEV)
    fwd_routes_turns = jax.random.permutation(jax.random.fold_in(keys[3], 3), N_SECTION * TOKENS // TOK_DEV)
    fwd_routes = jax.vmap(lambda own, number: routed_block(jax.random.fold_in(keys[3], 2), own, number, TOK_DEV, EXPERTS, 2, CAP, 2))(fwd_routes_keys, fwd_routes_turns).reshape((N_SECTION, TOKENS, 2))
    fwd_gates = jnp.clip(0.2 + 0.8 * jax.random.uniform(keys[4], (N_SECTION, TOKENS, 2), jnp.float32) ** levels(keys[4], (N_SECTION, TOKENS, 2), ((0, 4), (1, 8)), -0.2, 0.2), 0.2, 1.0)
    fwd_modulation = normal_values(keys[5], (N_SECTION, 3, D), 0.5, 3.0, ((0, 4),), jnp.float32)
    bwd_routes_keys = jax.random.split(jax.random.fold_in(keys[6], 1), N_SECTION * TOKENS // TOK_DEV)
    bwd_routes_turns = jax.random.permutation(jax.random.fold_in(keys[6], 3), N_SECTION * TOKENS // TOK_DEV)
    bwd_routes = jax.vmap(lambda own, number: routed_block(jax.random.fold_in(keys[6], 2), own, number, TOK_DEV, EXPERTS, 2, CAP, 2))(bwd_routes_keys, bwd_routes_turns).reshape((N_SECTION, TOKENS, 2))
    bwd_gates = jnp.clip(0.2 + 0.8 * jax.random.uniform(keys[7], (N_SECTION, TOKENS, 2), jnp.float32) ** levels(keys[7], (N_SECTION, TOKENS, 2), ((0, 4), (1, 8)), -0.2, 0.2), 0.2, 1.0)
    bwd_modulation = normal_values(keys[8], (N_SECTION, 3, D), 0.5, 3.0, ((0, 4),), jnp.float32)
    up_weight = normal_values(keys[9], (N_SECTION, N_EXPERT, D, FF_DEV), D ** -0.5, 0.125, ((0, 4), (1, 8)))
    down_weight = normal_values(keys[10], (N_SECTION, N_EXPERT, FF_DEV, D), FF ** -0.5, 0.125, ((0, 4), (1, 8)))
    return dict(section_inputs=section_inputs, stored_inputs=stored_inputs, out_grads=out_grads, fwd_routes=fwd_routes, fwd_gates=fwd_gates, fwd_modulation=fwd_modulation, bwd_routes=bwd_routes, bwd_gates=bwd_gates, bwd_modulation=bwd_modulation, up_weight=up_weight, down_weight=down_weight)


norm_eps = 1e-06

def layer_norm(tok_rows):
    mean_row = lax.optimization_barrier(jnp.mean(tok_rows, axis=-1, keepdims=True))
    centered = tok_rows - mean_row
    variance = lax.optimization_barrier(jnp.mean(centered * centered, axis=-1, keepdims=True))
    inv_std = lax.rsqrt(variance + norm_eps)
    return (centered * inv_std, inv_std)

def slot_numbers(routes):
    flat_ids = routes.reshape(-1).astype(jnp.int32)
    choose = (flat_ids[:, None] == jnp.arange(EXPERTS, dtype=jnp.int32)[None, :]).astype(jnp.int32)
    before = jnp.cumsum(choose, axis=0) - choose
    return (flat_ids, lax.optimization_barrier(jnp.sum(before * choose, axis=1)).astype(jnp.int32))

def place_rows(flat_ids, slot_index, pair_values):
    empty = jnp.zeros((EXPERTS, N_EXPERT * CAP, D), pair_values.dtype)
    return empty.at[flat_ids, slot_index].set(pair_values)

def one_section(packed):
    inputs, stored, grads, fwd_routes, fwd_gates, fwd_mod, bwd_routes, bwd_gates, bwd_mod, up_w, down_w = packed
    up_all = up_w.reshape(EXPERTS, 2, D, FF_DEV).astype(jnp.float32)
    down_all = down_w.reshape(EXPERTS, 2, FF_DEV, D).astype(jnp.float32)
    normed, _ = layer_norm(inputs)
    hidden = (normed * (1.0 + fwd_mod[1]) + fwd_mod[0]).astype(jnp.bfloat16)
    flat_ids, slot_index = slot_numbers(fwd_routes)
    rows = place_rows(flat_ids, slot_index, jnp.repeat(hidden, 2, axis=0)).astype(jnp.float32)
    pre_act = jnp.einsum('erd,ejdf->ejrf', rows, up_all)
    activation = jax.nn.gelu(pre_act).astype(jnp.bfloat16).astype(jnp.float32)
    partial_value = jnp.einsum('ejrf,ejfd->ejrd', activation, down_all).astype(jnp.bfloat16).astype(jnp.float32)
    summed = partial_value[:, 0] + partial_value[:, 1]
    pair_out = summed[flat_ids, slot_index].reshape(TOKENS, 2, D)
    moe_out = lax.optimization_barrier(jnp.sum(pair_out * fwd_gates[:, :, None], axis=1))
    out_fwd = inputs + fwd_mod[2] * moe_out
    normed_b, inv_b = layer_norm(stored)
    hidden_b = (normed_b * (1.0 + bwd_mod[1]) + bwd_mod[0]).astype(jnp.bfloat16)
    grad_rows = grads.astype(jnp.float32)
    pair_grads = (bwd_gates[:, :, None] * (bwd_mod[2] * grad_rows)[:, None, :]).astype(jnp.bfloat16).reshape(2 * TOKENS, D)
    flat_b, slot_b = slot_numbers(bwd_routes)
    rows_h = place_rows(flat_b, slot_b, jnp.repeat(hidden_b, 2, axis=0)).astype(jnp.float32)
    rows_g = place_rows(flat_b, slot_b, pair_grads).astype(jnp.float32)
    pre_b = jnp.einsum('erd,ejdf->ejrf', rows_h, up_all)
    act_grad = jnp.einsum('erd,ejfd->ejrf', rows_g, down_all)
    pre_grad = jax.vjp(jax.nn.gelu, pre_b)[1](act_grad)[0].astype(jnp.bfloat16).astype(jnp.float32)
    part_b = jnp.einsum('ejrf,ejdf->ejrd', pre_grad, up_all).astype(jnp.bfloat16).astype(jnp.float32)
    summed_b = part_b[:, 0] + part_b[:, 1]
    dhidden = lax.optimization_barrier(jnp.sum(summed_b[flat_b, slot_b].reshape(TOKENS, 2, D), axis=1))
    dnorm = dhidden * (1.0 + bwd_mod[1])
    mean_one = lax.optimization_barrier(jnp.mean(dnorm, axis=-1, keepdims=True))
    mean_two = lax.optimization_barrier(jnp.mean(dnorm * normed_b, axis=-1, keepdims=True))
    section_grad = (grad_rows + (dnorm - mean_one - normed_b * mean_two) * inv_b).astype(jnp.bfloat16)
    return (out_fwd, section_grad)

def reference(section_inputs, stored_inputs, out_grads, fwd_routes, fwd_gates, fwd_modulation, bwd_routes, bwd_gates, bwd_modulation, up_weight, down_weight):
    out_fwd, section_grad = lax.map(one_section, (section_inputs, stored_inputs, out_grads, fwd_routes, fwd_gates, fwd_modulation, bwd_routes, bwd_gates, bwd_modulation, up_weight, down_weight))
    next_inputs = jnp.concatenate([jnp.zeros_like(out_fwd[:1]), out_fwd[:-1]], axis=0)
    input_grads = jnp.concatenate([section_grad[1:], jnp.zeros_like(section_grad[:1])], axis=0)
    return (next_inputs, input_grads)
```

```python
import functools

import jax
import jax.numpy as jnp
from jax import lax
from jax.experimental import pallas as pl
from jax.experimental.pallas import tpu as pltpu
from jax.sharding import PartitionSpec as P

norm_eps = 1e-06
F32, BF16 = jnp.float32, jnp.bfloat16
MESH = pl.DeviceIdType.MESH
ROOT, CUBE = 0.7978845608028654, 0.044715


def flip(index, mask, bits):
    total = 0
    for b in range(bits):
        bit = (index // (1 << b)) % 2
        total = total + (1 << b) * (1 - bit if mask >> b & 1 else bit)
    return total


def dot(a, b, ca=1, cb=0):
    return lax.dot_general(a, b, (((ca,), (cb,)), ((), ())), preferred_element_type=F32)


def slot_masks(routes, capacity, slots):
    count = routes.shape[0]
    lanes = lax.broadcasted_iota(jnp.int32, (count, 128), 1)
    hits = [routes[:, k : k + 1] == lanes for k in range(2)]
    choose = jnp.where(hits[0] | hits[1], 1.0, 0.0).astype(BF16)
    row = lax.broadcasted_iota(jnp.int32, (count, count), 0)
    col = lax.broadcasted_iota(jnp.int32, (count, count), 1)
    before = dot(jnp.where(col < row, 1.0, 0.0).astype(BF16), choose)
    places = lax.broadcasted_iota(jnp.int32, (count, slots), 1)
    masks = []
    for k in range(2):
        rank = jnp.sum(jnp.where(hits[k], before, 0.0), axis=1, keepdims=True)
        masks.append(places == routes[:, k : k + 1] * capacity + rank.astype(jnp.int32))
    return masks


def many_chips(
    sections, units, capacity,
    x_ref, st_ref, og_ref, fr_ref, fg_ref, fm_ref, br_ref, bg_ref, bm_ref, up_hbm, down_hbm,
    next_ref, grad_ref,
    up, down, snd_f, snd_r, snd_g, rcv_f, rcv_r, rcv_g, act, dgelu,
    px_f, px_b, pin_f, pin_b, ret_f, ret_b, rr_f, rr_b,
    hid, pair0, pair1, normed_b, inv_b, out_f, dh, out_b,
    w_sem, in_send, in_recv, fw_send, fw_recv, px_send, px_recv, rt_send, rt_recv,
    sf_send, sf_recv, sb_send, sb_recv,
):
    s, me = lax.axis_index("section"), lax.axis_index("expert")
    experts = units // 2
    bits = units.bit_length() - 1
    chip, core = me // 2, me % 2
    count, width = x_ref.shape
    half = width // 2
    hidden_units = up.shape[1]
    rows = units * capacity
    slots = experts * capacity
    tile = 256
    group = 16
    order = list(range(1, units))
    peer = {k: flip(me, k, bits) for k in order}

    w_up = pltpu.make_async_copy(up_hbm, up, w_sem.at[0])
    w_down = pltpu.make_async_copy(down_hbm, down, w_sem.at[1])
    w_up.start()
    w_down.start()

    barrier = pltpu.get_barrier_semaphore()
    for k in order:
        pl.semaphore_signal(barrier, inc=1, device_id=(s, peer[k]), device_id_type=MESH)
    for step in (1, sections - 1):
        pl.semaphore_signal(
            barrier, inc=1, device_id=((s + step) % sections, me), device_id_type=MESH
        )

    def remote(src, dst, send, recv, section, unit):
        return pltpu.make_async_remote_copy(
            src_ref=src, dst_ref=dst, send_sem=send, recv_sem=recv,
            device_id=(section, unit), device_id_type=MESH,
        )

    def inbound(phase, snd, rcv):
        copies = {}
        for k in order:
            d = peer[k]
            if k == 1:
                src, dst = snd.at[chip], rcv.at[:, me]
            else:
                src, dst = snd.at[d // 2, d % 2], rcv.at[d % 2, me]
            copies[k] = remote(src, dst, in_send.at[phase, k], in_recv.at[phase, k], s, d)
        return copies

    def hand_on(phase, rcv):
        copies = {}
        for k in order:
            if k > 1:
                block = rcv.at[core, peer[k]]
                copies[k] = remote(
                    block, block, fw_send.at[phase, k], fw_recv.at[phase, k], s, peer[1]
                )
        return copies

    def keep_own(snd, rcv):
        for h in range(2):
            rcv[h, me] = snd[chip, h]

    def receive(ins, fws):
        for k in order:
            ins[k].wait_recv()
            if k > 1:
                fws[k].start()
        for k in order:
            if k > 1:
                fws[k].wait_recv()

    def normalise(src, mod, keep):
        @pl.loop(0, count // group)
        def _(i):
            at = pl.ds(pl.multiple_of(i * group, group), group)
            x = src[at, :]
            centered = x - jnp.mean(x, axis=1, keepdims=True)
            inv = lax.rsqrt(jnp.mean(centered * centered, axis=1, keepdims=True) + norm_eps)
            normed = centered * inv
            hid[at, :] = (normed * (1.0 + mod[1:2, :]) + mod[0:1, :]).astype(BF16)
            if keep:
                normed_b[at, :] = normed
                inv_b[at, :] = jnp.broadcast_to(inv, (group, 128))

    def pack(terms, snd):
        for h in range(2):
            @pl.loop(0, half // tile)
            def _(n):
                src = pl.ds(pl.multiple_of(h * half + n * tile, tile), tile)
                value = sum(dot(mask, ref[:, src], 0, 0) for mask, ref in terms).astype(BF16)
                for e in range(experts):
                    snd[e, h, :, pl.ds(pl.multiple_of(n * tile, tile), tile)] = value[
                        e * capacity : (e + 1) * capacity, :
                    ]

    def onehot(mask):
        return jnp.where(mask, 1.0, 0.0).astype(BF16)

    normalise(x_ref, fm_ref, False)
    fwd = slot_masks(fr_ref[...], capacity, slots)
    pack([(onehot(fwd[0] | fwd[1]), hid)], snd_f)
    pl.semaphore_wait(barrier, units + 1)
    in_f, fw_f = inbound(0, snd_f, rcv_f), hand_on(0, rcv_f)
    for k in order:
        in_f[k].start()
    keep_own(snd_f, rcv_f)

    normalise(st_ref, bm_ref, True)
    bwd = slot_masks(br_ref[...], capacity, slots)
    bwd_hot = [onehot(mask) for mask in bwd]
    pack([(bwd_hot[0] + bwd_hot[1], hid)], snd_r)
    in_r, fw_r = inbound(1, snd_r, rcv_r), hand_on(1, rcv_r)
    for k in order:
        in_r[k].start()
    keep_own(snd_r, rcv_r)

    @pl.loop(0, count // group)
    def _(i):
        at = pl.ds(pl.multiple_of(i * group, group), group)
        scaled = bm_ref[2:3, :] * og_ref[at, :].astype(F32)
        pair0[at, :] = (bg_ref[at, 0:1] * scaled).astype(BF16)
        pair1[at, :] = (bg_ref[at, 1:2] * scaled).astype(BF16)

    pack([(bwd_hot[0], pair0), (bwd_hot[1], pair1)], snd_g)
    in_g, fw_g = inbound(2, snd_g, rcv_g), hand_on(2, rcv_g)
    for k in order:
        in_g[k].start()
    keep_own(snd_g, rcv_g)

    def flat(ref, h):
        return ref[h].reshape(rows, half)

    def cols(n, base=0):
        return pl.ds(pl.multiple_of(base + n * tile, tile), tile)

    def exchange(phase, px, pin, ret, result):
        def fill(dst, h):
            @pl.loop(0, half // tile)
            def _(n):
                value = result(h, n).astype(BF16).reshape(units, capacity, tile)
                dst[:, :, cols(n)] = value

        fill(px, 1 - core)
        swap = remote(px, pin, px_send.at[phase], px_recv.at[phase], s, peer[1])
        swap.start()
        fill(ret, core)
        swap.wait_recv()

        @pl.loop(0, units)
        def _(u):
            ret[u] = (ret[u].astype(F32) + pin[u].astype(F32)).astype(BF16)

        return swap

    def give_back(phase, ret, rr):
        copies = {}
        for k in order:
            copies[k] = remote(
                ret.at[peer[k]], rr.at[core, chip],
                rt_send.at[phase, k], rt_recv.at[phase, k], s, peer[k],
            )
            copies[k].start()
        rr[core, chip] = ret[me]
        return copies

    receive(in_f, fw_f)
    w_up.wait()
    w_down.wait()

    @pl.loop(0, hidden_units // tile)
    def _(n):
        pre = dot(flat(rcv_f, 0), up[:half, cols(n)]) + dot(flat(rcv_f, 1), up[half:, cols(n)])
        t = jnp.tanh(ROOT * (pre + CUBE * pre * pre * pre))
        act[:, cols(n)] = (0.5 * pre * (1.0 + t)).astype(BF16)

    swap_f = exchange(
        0, px_f, pin_f, ret_f, lambda h, n: dot(act[...], down[:, cols(n, h * half)])
    )
    back_f = give_back(0, ret_f, rr_f)

    receive(in_r, fw_r)

    @pl.loop(0, hidden_units // tile)
    def _(n):
        pre = dot(flat(rcv_r, 0), up[:half, cols(n)]) + dot(flat(rcv_r, 1), up[half:, cols(n)])
        t = jnp.tanh(ROOT * (pre + CUBE * pre * pre * pre))
        slope = ROOT * (1.0 + 3.0 * CUBE * pre * pre)
        dgelu[:, cols(n)] = 0.5 * (1.0 + t) + 0.5 * pre * (1.0 - t * t) * slope

    receive(in_g, fw_g)

    @pl.loop(0, hidden_units // tile)
    def _(n):
        back = dot(flat(rcv_g, 0), down[cols(n), :half], 1, 1) + dot(
            flat(rcv_g, 1), down[cols(n), half:], 1, 1
        )
        act[:, cols(n)] = (back * dgelu[:, cols(n)]).astype(BF16)

    swap_b = exchange(
        1, px_b, pin_b, ret_b, lambda h, n: dot(act[...], up[cols(n, h * half), :], 1, 1)
    )
    back_b = give_back(1, ret_b, rr_b)

    weight = sum(jnp.where(fwd[k], fg_ref[:, k : k + 1], 0.0) for k in range(2))
    high = weight.astype(BF16)
    low = (weight - high.astype(F32)).astype(BF16)
    for k in order:
        back_f[k].wait_recv()
    sends_f = []
    for h in range(2):
        side = pl.ds(h * half, half)

        @pl.loop(0, half // tile)
        def _(n):
            got = rr_f[h, :, :, cols(n)].reshape(slots, tile)
            moe = dot(high, got) + dot(low, got)
            at = cols(n, h * half)
            out_f[:, at] = x_ref[:, at] + fm_ref[2:3, at] * moe

        copy = remote(
            out_f.at[:, side], next_ref.at[:, side], sf_send.at[h], sf_recv.at[h],
            (s + 1) % sections, me,
        )
        sends_f.append(copy)

        @pl.when(s < sections - 1)
        def _():
            copy.start()

    @pl.when(s == 0)
    def _():
        next_ref[...] = jnp.zeros_like(next_ref)

    @pl.when(s == sections - 1)
    def _():
        grad_ref[...] = jnp.zeros_like(grad_ref)

    for k in order:
        back_b[k].wait_recv()
    both = bwd_hot[0] + bwd_hot[1]
    for h in range(2):
        @pl.loop(0, half // tile)
        def _(n):
            got = rr_b[h, :, :, cols(n)].reshape(slots, tile)
            dh[:, cols(n, h * half)] = dot(both, got)

    pieces = 4
    part = count // pieces
    sends_b = []
    for p in range(pieces):
        @pl.loop(0, part // group)
        def _(i):
            at = pl.ds(pl.multiple_of(p * part + i * group, group), group)
            dnorm = dh[at, :] * (1.0 + bm_ref[1:2, :])
            normed = normed_b[at, :]
            one = jnp.mean(dnorm, axis=1, keepdims=True)
            two = jnp.mean(dnorm * normed, axis=1, keepdims=True)
            out_b[at, :] = (
                og_ref[at, :].astype(F32) + (dnorm - one - normed * two) * inv_b[at, 0:1]
            ).astype(BF16)

        piece = pl.ds(p * part, part)
        copy = remote(
            out_b.at[piece], grad_ref.at[piece], sb_send.at[p], sb_recv.at[p],
            (s + sections - 1) % sections, me,
        )
        sends_b.append(copy)

        @pl.when(s > 0)
        def _():
            copy.start()

    for copies in (in_f, in_r, in_g, fw_f, fw_r, fw_g, back_f, back_b):
        for copy in copies.values():
            copy.wait_send()
    swap_f.wait_send()
    swap_b.wait_send()

    @pl.when(s < sections - 1)
    def _():
        for copy in sends_f:
            copy.wait_send()
        for copy in sends_b:
            copy.wait_recv()

    @pl.when(s > 0)
    def _():
        for copy in sends_f:
            copy.wait_recv()
        for copy in sends_b:
            copy.wait_send()


def run_many(
    section_inputs,
    stored_inputs,
    out_grads,
    fwd_routes,
    fwd_gates,
    fwd_modulation,
    bwd_routes,
    bwd_gates,
    bwd_modulation,
    up_weight,
    down_weight,
):
    sections, units = lax.axis_size("section"), lax.axis_size("expert")
    experts = units // 2
    count, width = section_inputs.shape[1:]
    hidden_units = up_weight.shape[3]
    half = width // 2
    capacity = -(-min(count, 5 * count // (2 * experts)) // 16) * 16
    rows = units * capacity

    def vmem(dtype, *shape):
        return pltpu.VMEM(shape, dtype)

    def dma(*shape):
        return pltpu.SemaphoreType.DMA(shape)

    scratch = [
        vmem(BF16, width, hidden_units),
        vmem(BF16, hidden_units, width),
        *[vmem(BF16, experts, 2, capacity, half)] * 3,
        *[vmem(BF16, 2, units, capacity, half)] * 3,
        vmem(BF16, rows, hidden_units),
        vmem(F32, rows, hidden_units),
        *[vmem(BF16, units, capacity, half)] * 6,
        *[vmem(BF16, 2, experts, capacity, half)] * 2,
        *[vmem(BF16, count, width)] * 3,
        vmem(F32, count, width),
        vmem(F32, count, 128),
        *[vmem(F32, count, width)] * 2,
        vmem(BF16, count, width),
        dma(2),
        *[dma(3, units)] * 4,
        *[dma(2)] * 2,
        *[dma(2, units)] * 2,
        *[dma(2)] * 2,
        *[dma(4)] * 2,
    ]
    in_vmem = pl.BlockSpec(memory_space=pltpu.VMEM)
    in_hbm = pl.BlockSpec(memory_space=pl.ANY)
    flops = 10 * rows * width * hidden_units
    next_inputs, input_grads = pl.pallas_call(
        functools.partial(many_chips, sections, units, capacity),
        out_shape=(
            jax.ShapeDtypeStruct((count, width), F32),
            jax.ShapeDtypeStruct((count, width), BF16),
        ),
        in_specs=[in_vmem] * 9 + [in_hbm] * 2,
        out_specs=(in_vmem, in_vmem),
        scratch_shapes=scratch,
        compiler_params=pltpu.CompilerParams(
            collective_id=0, has_side_effects=True, vmem_limit_bytes=67043328
        ),
        cost_estimate=pl.CostEstimate(
            flops=flops, bytes_accessed=4 * width * hidden_units, transcendentals=0
        ),
    )(
        section_inputs[0], stored_inputs[0], out_grads[0], fwd_routes[0], fwd_gates[0],
        fwd_modulation[0], bwd_routes[0], bwd_gates[0], bwd_modulation[0],
        up_weight[0, 0], down_weight[0, 0],
    )
    return next_inputs[None], input_grads[None]


def two_sided(
    sections, units, capacity, chunks, pieces,
    x_hbm, st_hbm, og_hbm, fr_ref, fg_ref, fm_ref, br_ref, bg_ref, bm_ref, up_hbm, down_hbm,
    next_ref, grad_ref,
    up, down, x_v, x_prev, st_v, dense, near, cross, snd_p, relay, rows, act, agrad,
    res, ret_p, ret_x, comb, den, normed_b, inv_b, m_out, m_in, dh, out_b,
    meta, picks, gate,
    load_sem, w_send, w_recv, meta_send, meta_recv, x_send, x_recv, near_send, near_recv,
    cross_send, cross_recv, part_send, part_recv, relay_send, relay_recv,
    retp_send, retp_recv, retx_send, retx_recv, den_send, den_recv,
    sf_send, sf_recv, sb_send, sb_recv,
):
    s, me = lax.axis_index("section"), lax.axis_index("expert")
    z, c = me // 2, me % 2
    odd, side = z % 2, z // 2
    inner = odd + side - 2 * odd * side
    seat = 1 - inner
    partner = z + 1 - 2 * odd
    crossing = [2 - side, 3 - 3 * side]
    is_inner, is_outer = inner == 1, inner == 0
    count, width = x_v.shape
    hidden = up.shape[2]
    every = 4 * capacity
    tile, group = 256, 16
    chunk, piece = width // chunks, width // pieces
    OG, HB, HF = 0, 1, 2
    FWD, BWD = 0, 1
    scope = jax.named_scope

    def unit(chip):
        return 2 * chip + c

    def remote(src, dst, send, recv, section, to):
        return pltpu.make_async_remote_copy(
            src_ref=src, dst_ref=dst, send_sem=send, recv_sem=recv,
            device_id=(section, to), device_id_type=MESH,
        )

    def cols(n, size):
        return pl.ds(pl.multiple_of(n * size, size), size)

    loads = [
        pltpu.make_async_copy(og_hbm, dense.at[OG], load_sem.at[0]),
        pltpu.make_async_copy(st_hbm, st_v, load_sem.at[1]),
        pltpu.make_async_copy(x_hbm, x_v, load_sem.at[2]),
        pltpu.make_async_copy(up_hbm, up.at[c], load_sem.at[3]),
        pltpu.make_async_copy(down_hbm, down.at[c], load_sem.at[4]),
    ]
    for load in loads[:3]:
        load.start()

    barrier = pltpu.get_barrier_semaphore()
    for chip in (partner, crossing[0], crossing[1]):
        pl.semaphore_signal(barrier, inc=1, device_id=(s, unit(chip)), device_id_type=MESH)
    twin = me + 1 - 2 * c
    pl.semaphore_signal(barrier, inc=1, device_id=(s, twin), device_id_type=MESH)
    for step in (1, sections - 1):
        pl.semaphore_signal(
            barrier, inc=1, device_id=((s + step) % sections, me), device_id_type=MESH
        )

    meta[0, 0:2, :] = fr_ref[...].astype(F32)
    meta[0, 2:4, :] = fg_ref[...]
    meta[0, 4:6, :] = br_ref[...].astype(F32)
    meta[0, 6:8, :] = bg_ref[...]

    metas = [
        remote(meta.at[0], meta.at[1], meta_send.at[0], meta_recv.at[0], s, unit(partner)),
        remote(
            meta.at[0], meta.at[2 + seat], meta_send.at[1], meta_recv.at[1 + seat],
            s, unit(crossing[0]),
        ),
        remote(
            meta.at[0], meta.at[2 + seat], meta_send.at[2], meta_recv.at[1 + seat],
            s, unit(crossing[1]),
        ),
    ]
    shares = w_send.shape[1]

    def twin_copy(w, p, slot):
        src, dst = ((up_hbm, up), (down_hbm, down))[w]
        size = src.shape[0] // shares
        at = pl.ds(p * size, size)
        return remote(src.at[at], dst.at[slot, at], w_send.at[w, p], w_recv.at[w, p], s, twin)

    def near_copy(q, n):
        at = cols(n, chunk)
        return remote(
            dense.at[q, :, at], near.at[q, :, at],
            near_send.at[q, n], near_recv.at[q, n], s, unit(partner),
        )

    def cross_copy(q, i, n):
        at = cols(n, chunk)
        src = dense if i == 0 else near
        return remote(
            src.at[q, :, at], cross.at[q, i, :, at],
            cross_send.at[q, i, n], cross_recv.at[q, i, n], s, unit(crossing[0]),
        )

    def part_copy(q, n):
        at = cols(n, chunk)
        return remote(
            snd_p.at[q, :, at], rows.at[q, 1, :, at],
            part_send.at[q, n], part_recv.at[q, n], s, unit(partner),
        )

    def relay_copy(q, i, n):
        at = cols(n, chunk)
        return remote(
            relay.at[q, i, :, at], rows.at[q, 2 + i, :, at],
            relay_send.at[q, i, n], relay_recv.at[q, i, n], s, unit(partner),
        )

    def retp_copy(r, n):
        at = cols(n, piece)
        return remote(
            res.at[r, 1, :, at], ret_p.at[r, :, at],
            retp_send.at[r, n], retp_recv.at[r, n], s, unit(partner),
        )

    def retx_copy(r, i, n):
        at = cols(n, piece)
        return remote(
            res.at[r, 2 + i, :, at], ret_x.at[r, i, :, at],
            retx_send.at[r, i, n], retx_recv.at[r, i, n], s, unit(partner),
        )

    def den_copy(r, i, n):
        at = cols(n, piece)
        return remote(
            comb.at[r, i, :, at], den.at[r, :, at],
            den_send.at[r, i, n], den_recv.at[r, n], s, unit(crossing[i]),
        )

    x_copy = remote(x_v, x_prev, x_send, x_recv, (s + 1) % sections, me)

    def ahead_copy(n):
        at = cols(n, piece)
        return remote(
            m_out.at[:, at], m_in.at[:, at], sf_send.at[n], sf_recv.at[n],
            (s + 1) % sections, me,
        )

    parts = sb_send.shape[0]
    part = count // parts

    def back_copy(p):
        at = cols(p, part)
        return remote(
            out_b.at[at], grad_ref.at[at], sb_send.at[p], sb_recv.at[p],
            (s + sections - 1) % sections, me,
        )

    def each_chunk(body):
        pl.loop(0, chunks)(body)

    def each_piece(body):
        pl.loop(0, pieces)(body)

    row16 = lax.broadcasted_iota(jnp.int32, (16, count), 0)
    named = jnp.where(row16 % 2 == 0, z, partner).astype(F32)
    forward = row16 < 2
    earlier = lax.broadcasted_iota(jnp.int32, (count, count), 0)
    later = lax.broadcasted_iota(jnp.int32, (count, count), 1)
    upper = jnp.where(earlier < later, 1.0, 0.0).astype(BF16)
    places = lax.broadcasted_iota(jnp.int32, (capacity, count), 0).astype(F32)

    def find(j):
        first = jnp.where(forward, meta[j, 0:1, :], meta[j, 4:5, :]) == named
        second = jnp.where(forward, meta[j, 1:2, :], meta[j, 5:6, :]) == named
        weight = jnp.where(
            first,
            jnp.where(forward, meta[j, 2:3, :], meta[j, 6:7, :]),
            jnp.where(forward, meta[j, 3:4, :], meta[j, 7:8, :]),
        )
        chosen = first | second
        before = dot(jnp.where(chosen, 1.0, 0.0).astype(BF16), upper)
        place = jnp.where(chosen, before, -1.0)
        for b in range(2):
            for k in range(2):
                row = slice(2 * b + k, 2 * b + k + 1)
                hit = places == place[row]
                picks[b, j, k] = jnp.where(hit, 1.0, 0.0).astype(BF16)
                if k == 0:
                    value = jnp.sum(jnp.where(hit, weight[row], 0.0), axis=1, keepdims=True)
                    gate[b, j] = jnp.broadcast_to(value, (capacity, 128))

    def pack_own(q, b):
        @each_chunk
        def _(n):
            at = cols(n, chunk)

            @pl.when(is_inner)
            def _():
                snd_p[q, :, at] = dot(picks[b, 0, 1], dense[q, :, at]).astype(BF16)
                part_copy(q, n).start()

            rows[q, 0, :, at] = dot(picks[b, 0, 0], dense[q, :, at]).astype(BF16)

    def normalise(src, mod, q, keep):
        @pl.loop(0, count // group)
        def _(i):
            at = pl.ds(pl.multiple_of(i * group, group), group)
            x = src[at, :]
            centered = x - jnp.mean(x, axis=1, keepdims=True)
            inv = lax.rsqrt(jnp.mean(centered * centered, axis=1, keepdims=True) + norm_eps)
            normed = centered * inv
            dense[q, at, :] = (normed * (1.0 + mod[1]) + mod[0]).astype(BF16)
            if keep:
                normed_b[at, :] = normed
                inv_b[at, :] = jnp.broadcast_to(inv, (group, 128))

    def send_near(q):
        @pl.when(is_outer)
        def _():
            each_chunk(lambda n: near_copy(q, n).start())

    def send_cross(q):
        @pl.when(is_inner)
        def _():
            each_chunk(lambda n: cross_copy(q, 0, n).start())

    def hand_over(q, b):
        @pl.when(is_inner)
        def _():
            @each_chunk
            def _(n):
                at = cols(n, chunk)
                near_copy(q, n).wait_recv()
                cross_copy(q, 1, n).start()
                rows[q, 1, :, at] = dot(picks[b, 1, 0], near[q, :, at]).astype(BF16)

    def pass_on(q, b, i, n):
        at = cols(n, chunk)
        cross_copy(q, i, n).wait_recv()
        relay[q, i, :, at] = dot(picks[b, 2 + i, 1], cross[q, i, :, at]).astype(BF16)
        relay_copy(q, i, n).start()
        rows[q, 2 + i, :, at] = dot(picks[b, 2 + i, 0], cross[q, i, :, at]).astype(BF16)

    def gather(q, b, i):
        @pl.when(is_inner)
        def _():
            each_chunk(lambda n: pass_on(q, b, i, n))

    def gathered(q):
        @pl.when(is_outer)
        def _():
            @each_chunk
            def _(n):
                part_copy(q, n).wait_recv()
                for i in range(2):
                    relay_copy(q, i, n).wait_recv()

    def flat(q):
        return rows[q].reshape(every, width)

    def give(r, n, value):
        at = cols(n, piece)
        value = value.astype(BF16).reshape(4, capacity, piece)
        for j in range(4):
            res[r, j, :, at] = value[j]

        @pl.when(is_outer)
        def _():
            for i in range(2):
                retx_copy(r, i, n).start()

        @pl.when(is_inner)
        def _():
            retp_copy(r, n).start()

    def give_late(r):
        @pl.when(is_outer)
        def _():
            each_piece(lambda n: retp_copy(r, n).start())

    def combine(r, b, n):
        at = cols(n, piece)
        for i in range(2):
            retx_copy(r, i, n).wait_recv()
            total = dot(picks[b, 2 + i, 0], res[r, 2 + i, :, at], 0, 0) + dot(
                picks[b, 2 + i, 1], ret_x[r, i, :, at], 0, 0
            )
            comb[r, i, :, at] = total.astype(BF16)
            den_copy(r, i, n).start()

    def own_total(r, b, n):
        at = cols(n, piece)
        retp_copy(r, n).wait_recv()
        den_copy(r, 0, n).wait_recv()
        return (
            dot(picks[b, 0, 0], res[r, 0, :, at], 0, 0)
            + dot(picks[b, 0, 1], ret_p[r, :, at], 0, 0)
            + den[r, :, at].astype(F32)
        )

    with scope("bar"):
        pl.semaphore_wait(barrier, 6)
    for copy in metas:
        copy.start()
    with scope("load0"):
        loads[0].wait()
        send_near(OG)
        send_cross(OG)
        loads[4].start()
        loads[3].start()
    with scope("find0"):
        find(0)
    with scope("pk_og"):
        pack_own(OG, BWD)
    twin_copy(1, 0, c).start()
    with scope("norm1"):
        loads[1].wait()
        normalise(st_v, bm_ref, HB, True)
        send_near(HB)
    twin_copy(1, 1, c).start()
    with scope("pk_hb"):
        pack_own(HB, BWD)
    twin_copy(1, 2, c).start()
    with scope("norm2"):
        loads[2].wait()

        @pl.when(s < sections - 1)
        def _():
            x_copy.start()

        normalise(x_v, fm_ref, HF, False)
        send_near(HF)
        pack_own(HF, FWD)
    twin_copy(1, 3, c).start()
    for j in range(1, 4):
        with scope(f"meta{j}"):
            remote(
                meta.at[0], meta.at[j], meta_send.at[j - 1], meta_recv.at[j - 1],
                s, unit(partner),
            ).wait_recv()
            find(j)
    with scope("over_og"):
        hand_over(OG, BWD)
        send_cross(HB)
    twin_copy(0, 0, c).start()
    with scope("gat_og0"):
        gather(OG, BWD, 0)
    twin_copy(0, 1, c).start()
    with scope("over_hb"):
        hand_over(HB, BWD)
        send_cross(HF)
    twin_copy(0, 2, c).start()
    with scope("gat_og1"):
        gather(OG, BWD, 1)
    with scope("gathered_og"):
        gathered(OG)
    twin_copy(0, 3, c).start()

    with scope("pair"):
        for j in range(4):
            @pl.loop(0, width // tile)
            def _(n):
                at = cols(n, tile)
                scaled = bm_ref[2, :, at] * rows[OG, j, :, at].astype(F32)
                rows[OG, j, :, at] = (gate[BWD, j, :, 0:1] * scaled).astype(BF16)

    with scope("wts"):
        loads[4].wait()
        for p in range(shares):
            twin_copy(1, p, 1 - c).wait_recv()

    with scope("agrad"):
        for h in range(2):
            @pl.loop(0, hidden // tile)
            def _(n):
                at = pl.ds(pl.multiple_of(h * hidden + n * tile, tile), tile)
                agrad[:, at] = dot(flat(OG), down[h, cols(n, tile), :], 1, 1)

    with scope("gat_hb0"):
        gather(HB, BWD, 0)
    with scope("over_hf"):
        hand_over(HF, FWD)
    with scope("gat_hb1"):
        gather(HB, BWD, 1)
    with scope("gathered_hb"):
        gathered(HB)
        loads[3].wait()
        for p in range(shares):
            twin_copy(0, p, 1 - c).wait_recv()

    with scope("pre"):
        for h in range(2):
            @pl.loop(0, hidden // tile)
            def _(n):
                at = pl.ds(pl.multiple_of(h * hidden + n * tile, tile), tile)
                pre = dot(flat(HB), up[h, :, cols(n, tile)])
                t = jnp.tanh(ROOT * (pre + CUBE * pre * pre * pre))
                slope = ROOT * (1.0 + 3.0 * CUBE * pre * pre)
                dgelu = 0.5 * (1.0 + t) + 0.5 * pre * (1.0 - t * t) * slope
                act[:, at] = (agrad[:, at] * dgelu).astype(BF16)

    with scope("partb"):
        @each_piece
        def _(n):
            at = cols(n, piece)
            give(
                BWD, n,
                dot(act[:, :hidden], up[0, at, :], 1, 1)
                + dot(act[:, hidden:], up[1, at, :], 1, 1),
            )

        give_late(BWD)

    with scope("gat_hf0"):
        gather(HF, FWD, 0)
    with scope("comb_b"):
        @pl.when(is_inner)
        def _():
            per = pieces // chunks

            @each_chunk
            def _(n):
                for k in range(per):
                    combine(BWD, BWD, n * per + k)
                with scope("gat_hf1"):
                    pass_on(HF, FWD, 1, n)

    with scope("gathered_hf"):
        gathered(HF)

    with scope("up"):
        for h in range(2):
            @pl.loop(0, hidden // tile)
            def _(n):
                at = pl.ds(pl.multiple_of(h * hidden + n * tile, tile), tile)
                pre = dot(flat(HF), up[h, :, cols(n, tile)])
                t = jnp.tanh(ROOT * (pre + CUBE * pre * pre * pre))
                act[:, at] = (0.5 * pre * (1.0 + t)).astype(BF16)

    weight = gate[FWD, :, :, 0:1].reshape(every, 1)

    with scope("down"):
        @each_piece
        def _(n):
            at = cols(n, piece)
            value = dot(act[:, :hidden], down[0, :, at]) + dot(act[:, hidden:], down[1, :, at])
            give(FWD, n, weight * value)

        give_late(FWD)

    with scope("comb_f"):
        @pl.when(is_inner)
        def _():
            each_piece(lambda n: combine(FWD, FWD, n))

    @pl.when(s == 0)
    def _():
        next_ref[...] = jnp.zeros_like(next_ref)

    @pl.when(s == sections - 1)
    def _():
        grad_ref[...] = jnp.zeros_like(grad_ref)

    with scope("own_b"):
        @each_piece
        def _(n):
            dh[:, cols(n, piece)] = own_total(BWD, BWD, n)

    with scope("fin_b"):
        for p in range(parts):
            @pl.loop(0, part // group)
            def _(i):
                at = pl.ds(pl.multiple_of(p * part + i * group, group), group)
                dnorm = dh[at, :] * (1.0 + bm_ref[1])
                normed = normed_b[at, :]
                one = jnp.mean(dnorm, axis=1, keepdims=True)
                two = jnp.mean(dnorm * normed, axis=1, keepdims=True)
                out_b[at, :] = (
                    dense[OG, at, :].astype(F32) + (dnorm - one - normed * two) * inv_b[at, 0:1]
                ).astype(BF16)

            @pl.when(s > 0)
            def _():
                back_copy(p).start()

    def arrive(n):
        at = cols(n, piece)

        @pl.when(s > 0)
        def _():
            ahead_copy(n).wait_recv()
            next_ref[:, at] = x_prev[:, at] + m_in[:, at].astype(F32)

    with scope("own_f"):
        @pl.when(s > 0)
        def _():
            x_copy.wait_recv()

        lag = 2

        @each_piece
        def _(n):
            at = cols(n, piece)
            m_out[:, at] = (fm_ref[2, :, at] * own_total(FWD, FWD, n)).astype(BF16)

            @pl.when(s < sections - 1)
            def _():
                ahead_copy(n).start()

            @pl.when(n >= lag)
            def _():
                arrive(n - lag)

        for n in range(pieces - lag, pieces):
            arrive(n)

    with scope("tail_send"):
        for copy in metas:
            copy.wait_send()
        for p in range(shares):
            for w in range(2):
                twin_copy(w, p, c).wait_send()

        @each_chunk
        def _(n):
            for q in range(3):
                @pl.when(is_outer)
                def _():
                    near_copy(q, n).wait_send()

                @pl.when(is_inner)
                def _():
                    part_copy(q, n).wait_send()
                    for i in range(2):
                        cross_copy(q, i, n).wait_send()
                        relay_copy(q, i, n).wait_send()

        @each_piece
        def _(n):
            for r in range(2):
                retp_copy(r, n).wait_send()

                @pl.when(is_outer)
                def _():
                    for i in range(2):
                        retx_copy(r, i, n).wait_send()

                @pl.when(is_inner)
                def _():
                    for i in range(2):
                        den_copy(r, i, n).wait_send()

    with scope("tail_hop"):
        @pl.when(s < sections - 1)
        def _():
            x_copy.wait_send()
            each_piece(lambda n: ahead_copy(n).wait_send())
            pl.loop(0, parts)(lambda p: back_copy(p).wait_recv())

        @pl.when(s > 0)
        def _():
            pl.loop(0, parts)(lambda p: back_copy(p).wait_send())


def run_two_sided(
    section_inputs,
    stored_inputs,
    out_grads,
    fwd_routes,
    fwd_gates,
    fwd_modulation,
    bwd_routes,
    bwd_gates,
    bwd_modulation,
    up_weight,
    down_weight,
):
    sections, units = lax.axis_size("section"), lax.axis_size("expert")
    experts = units // 2
    count, width = section_inputs.shape[1:]
    hidden = up_weight.shape[3]
    capacity = -(-min(count, 5 * count // (2 * experts)) // 16) * 16
    every = 4 * capacity
    chunks, pieces, parts = 4, 8, 4

    def vmem(dtype, *shape):
        return pltpu.VMEM(shape, dtype)

    def dma(*shape):
        return pltpu.SemaphoreType.DMA(shape)

    scratch = [
        vmem(BF16, 2, width, hidden),
        vmem(BF16, 2, hidden, width),
        *[vmem(F32, count, width)] * 3,
        *[vmem(BF16, 3, count, width)] * 2,
        vmem(BF16, 3, 2, count, width),
        vmem(BF16, 3, capacity, width),
        vmem(BF16, 3, 2, capacity, width),
        vmem(BF16, 3, 4, capacity, width),
        vmem(BF16, every, 2 * hidden),
        vmem(F32, every, 2 * hidden),
        vmem(BF16, 2, 4, capacity, width),
        vmem(BF16, 2, capacity, width),
        vmem(BF16, 2, 2, capacity, width),
        vmem(BF16, 2, 2, count, width),
        vmem(BF16, 2, count, width),
        vmem(F32, count, width),
        vmem(F32, count, 128),
        *[vmem(BF16, count, width)] * 2,
        vmem(F32, count, width),
        vmem(BF16, count, width),
        vmem(F32, 4, 8, count),
        vmem(BF16, 2, 4, 2, capacity, count),
        vmem(F32, 2, 4, capacity, 128),
        dma(5),
        *[dma(2, 4)] * 2,
        *[dma(3)] * 2,
        *[pltpu.SemaphoreType.DMA] * 2,
        *[dma(3, chunks)] * 2,
        *[dma(3, 2, chunks)] * 2,
        *[dma(3, chunks)] * 2,
        *[dma(3, 2, chunks)] * 2,
        *[dma(2, pieces)] * 2,
        *[dma(2, 2, pieces)] * 2,
        dma(2, 2, pieces),
        dma(2, pieces),
        *[dma(pieces)] * 2,
        *[dma(parts)] * 2,
    ]
    in_vmem = pl.BlockSpec(memory_space=pltpu.VMEM)
    in_hbm = pl.BlockSpec(memory_space=pl.ANY)
    flops = 20 * every * width * hidden
    next_inputs, input_grads = pl.pallas_call(
        functools.partial(two_sided, sections, units, capacity, chunks, pieces),
        out_shape=(
            jax.ShapeDtypeStruct((count, width), F32),
            jax.ShapeDtypeStruct((count, width), BF16),
        ),
        in_specs=[in_hbm] * 3 + [in_vmem] * 6 + [in_hbm] * 2,
        out_specs=(in_vmem, in_vmem),
        scratch_shapes=scratch,
        compiler_params=pltpu.CompilerParams(
            collective_id=1, has_side_effects=True, vmem_limit_bytes=67043328
        ),
        cost_estimate=pl.CostEstimate(
            flops=flops, bytes_accessed=4 * width * hidden, transcendentals=0
        ),
    )(
        section_inputs[0], stored_inputs[0], out_grads[0],
        fwd_routes[0].T, fwd_gates[0].T, jnp.transpose(fwd_modulation, (1, 0, 2)),
        bwd_routes[0].T, bwd_gates[0].T, jnp.transpose(bwd_modulation, (1, 0, 2)),
        up_weight[0, 0], down_weight[0, 0],
    )
    return next_inputs[None], input_grads[None]


def on_device(*arrays):
    sides, inner_and_outer = 2, 2
    line = lax.axis_size("expert") == 2 * sides * inner_and_outer
    return (run_two_sided if line else run_many)(*arrays)


def solution(mesh):
    tokens = P("section", "expert", None)
    shared = P("section", None, None)
    weights = P("section", "expert", None, None)
    placed = (tokens,) * 5 + (shared,) + (tokens,) * 2 + (shared,) + (weights,) * 2
    return jax.shard_map(
        on_device,
        mesh=mesh,
        in_specs=placed,
        out_specs=(tokens, tokens),
        check_vma=False,
    )
```

```python
import functools

import jax
import jax.numpy as jnp
from jax import lax
from jax.experimental import pallas as pl
from jax.experimental.pallas import tpu as pltpu
from jax.sharding import PartitionSpec as P

norm_eps = 1e-06
F32, BF16 = jnp.float32, jnp.bfloat16
MESH = pl.DeviceIdType.MESH
ROOT, CUBE = 0.7978845608028654, 0.044715


def flip(index, mask, bits):
    total = 0
    for b in range(bits):
        bit = (index // (1 << b)) % 2
        total = total + (1 << b) * (1 - bit if mask >> b & 1 else bit)
    return total


def dot(a, b, ca=1, cb=0):
    return lax.dot_general(a, b, (((ca,), (cb,)), ((), ())), preferred_element_type=F32)


def slot_masks(routes, capacity, slots):
    count = routes.shape[0]
    lanes = lax.broadcasted_iota(jnp.int32, (count, 128), 1)
    hits = [routes[:, k : k + 1] == lanes for k in range(2)]
    choose = jnp.where(hits[0] | hits[1], 1.0, 0.0).astype(BF16)
    row = lax.broadcasted_iota(jnp.int32, (count, count), 0)
    col = lax.broadcasted_iota(jnp.int32, (count, count), 1)
    before = dot(jnp.where(col < row, 1.0, 0.0).astype(BF16), choose)
    places = lax.broadcasted_iota(jnp.int32, (count, slots), 1)
    masks = []
    for k in range(2):
        rank = jnp.sum(jnp.where(hits[k], before, 0.0), axis=1, keepdims=True)
        masks.append(places == routes[:, k : k + 1] * capacity + rank.astype(jnp.int32))
    return masks


def many_chips(
    sections, units, capacity,
    x_ref, st_ref, og_ref, fr_ref, fg_ref, fm_ref, br_ref, bg_ref, bm_ref, up_hbm, down_hbm,
    next_ref, grad_ref,
    up, down, snd_f, snd_r, snd_g, rcv_f, rcv_r, rcv_g, act, dgelu,
    px_f, px_b, pin_f, pin_b, ret_f, ret_b, rr_f, rr_b,
    hid, pair0, pair1, normed_b, inv_b, out_f, dh, out_b,
    w_sem, in_send, in_recv, fw_send, fw_recv, px_send, px_recv, rt_send, rt_recv,
    sf_send, sf_recv, sb_send, sb_recv,
):
    s, me = lax.axis_index("section"), lax.axis_index("expert")
    experts = units // 2
    bits = units.bit_length() - 1
    chip, core = me // 2, me % 2
    count, width = x_ref.shape
    half = width // 2
    hidden_units = up.shape[1]
    rows = units * capacity
    slots = experts * capacity
    tile = 256
    group = 16
    order = list(range(1, units))
    peer = {k: flip(me, k, bits) for k in order}

    w_up = pltpu.make_async_copy(up_hbm, up, w_sem.at[0])
    w_down = pltpu.make_async_copy(down_hbm, down, w_sem.at[1])
    w_up.start()
    w_down.start()

    barrier = pltpu.get_barrier_semaphore()
    for k in order:
        pl.semaphore_signal(barrier, inc=1, device_id=(s, peer[k]), device_id_type=MESH)
    for step in (1, sections - 1):
        pl.semaphore_signal(
            barrier, inc=1, device_id=((s + step) % sections, me), device_id_type=MESH
        )

    def remote(src, dst, send, recv, section, unit):
        return pltpu.make_async_remote_copy(
            src_ref=src, dst_ref=dst, send_sem=send, recv_sem=recv,
            device_id=(section, unit), device_id_type=MESH,
        )

    def inbound(phase, snd, rcv):
        copies = {}
        for k in order:
            d = peer[k]
            if k == 1:
                src, dst = snd.at[chip], rcv.at[:, me]
            else:
                src, dst = snd.at[d // 2, d % 2], rcv.at[d % 2, me]
            copies[k] = remote(src, dst, in_send.at[phase, k], in_recv.at[phase, k], s, d)
        return copies

    def hand_on(phase, rcv):
        copies = {}
        for k in order:
            if k > 1:
                block = rcv.at[core, peer[k]]
                copies[k] = remote(
                    block, block, fw_send.at[phase, k], fw_recv.at[phase, k], s, peer[1]
                )
        return copies

    def keep_own(snd, rcv):
        for h in range(2):
            rcv[h, me] = snd[chip, h]

    def receive(ins, fws):
        for k in order:
            ins[k].wait_recv()
            if k > 1:
                fws[k].start()
        for k in order:
            if k > 1:
                fws[k].wait_recv()

    def normalise(src, mod, keep):
        @pl.loop(0, count // group)
        def _(i):
            at = pl.ds(pl.multiple_of(i * group, group), group)
            x = src[at, :]
            centered = x - jnp.mean(x, axis=1, keepdims=True)
            inv = lax.rsqrt(jnp.mean(centered * centered, axis=1, keepdims=True) + norm_eps)
            normed = centered * inv
            hid[at, :] = (normed * (1.0 + mod[1:2, :]) + mod[0:1, :]).astype(BF16)
            if keep:
                normed_b[at, :] = normed
                inv_b[at, :] = jnp.broadcast_to(inv, (group, 128))

    def pack(terms, snd):
        for h in range(2):
            @pl.loop(0, half // tile)
            def _(n):
                src = pl.ds(pl.multiple_of(h * half + n * tile, tile), tile)
                value = sum(dot(mask, ref[:, src], 0, 0) for mask, ref in terms).astype(BF16)
                for e in range(experts):
                    snd[e, h, :, pl.ds(pl.multiple_of(n * tile, tile), tile)] = value[
                        e * capacity : (e + 1) * capacity, :
                    ]

    def onehot(mask):
        return jnp.where(mask, 1.0, 0.0).astype(BF16)

    normalise(x_ref, fm_ref, False)
    fwd = slot_masks(fr_ref[...], capacity, slots)
    pack([(onehot(fwd[0] | fwd[1]), hid)], snd_f)
    pl.semaphore_wait(barrier, units + 1)
    in_f, fw_f = inbound(0, snd_f, rcv_f), hand_on(0, rcv_f)
    for k in order:
        in_f[k].start()
    keep_own(snd_f, rcv_f)

    normalise(st_ref, bm_ref, True)
    bwd = slot_masks(br_ref[...], capacity, slots)
    bwd_hot = [onehot(mask) for mask in bwd]
    pack([(bwd_hot[0] + bwd_hot[1], hid)], snd_r)
    in_r, fw_r = inbound(1, snd_r, rcv_r), hand_on(1, rcv_r)
    for k in order:
        in_r[k].start()
    keep_own(snd_r, rcv_r)

    @pl.loop(0, count // group)
    def _(i):
        at = pl.ds(pl.multiple_of(i * group, group), group)
        scaled = bm_ref[2:3, :] * og_ref[at, :].astype(F32)
        pair0[at, :] = (bg_ref[at, 0:1] * scaled).astype(BF16)
        pair1[at, :] = (bg_ref[at, 1:2] * scaled).astype(BF16)

    pack([(bwd_hot[0], pair0), (bwd_hot[1], pair1)], snd_g)
    in_g, fw_g = inbound(2, snd_g, rcv_g), hand_on(2, rcv_g)
    for k in order:
        in_g[k].start()
    keep_own(snd_g, rcv_g)

    def flat(ref, h):
        return ref[h].reshape(rows, half)

    def cols(n, base=0):
        return pl.ds(pl.multiple_of(base + n * tile, tile), tile)

    def exchange(phase, px, pin, ret, result):
        def fill(dst, h):
            @pl.loop(0, half // tile)
            def _(n):
                value = result(h, n).astype(BF16).reshape(units, capacity, tile)
                dst[:, :, cols(n)] = value

        fill(px, 1 - core)
        swap = remote(px, pin, px_send.at[phase], px_recv.at[phase], s, peer[1])
        swap.start()
        fill(ret, core)
        swap.wait_recv()

        @pl.loop(0, units)
        def _(u):
            ret[u] = (ret[u].astype(F32) + pin[u].astype(F32)).astype(BF16)

        return swap

    def give_back(phase, ret, rr):
        copies = {}
        for k in order:
            copies[k] = remote(
                ret.at[peer[k]], rr.at[core, chip],
                rt_send.at[phase, k], rt_recv.at[phase, k], s, peer[k],
            )
            copies[k].start()
        rr[core, chip] = ret[me]
        return copies

    receive(in_f, fw_f)
    w_up.wait()
    w_down.wait()

    @pl.loop(0, hidden_units // tile)
    def _(n):
        pre = dot(flat(rcv_f, 0), up[:half, cols(n)]) + dot(flat(rcv_f, 1), up[half:, cols(n)])
        t = jnp.tanh(ROOT * (pre + CUBE * pre * pre * pre))
        act[:, cols(n)] = (0.5 * pre * (1.0 + t)).astype(BF16)

    swap_f = exchange(
        0, px_f, pin_f, ret_f, lambda h, n: dot(act[...], down[:, cols(n, h * half)])
    )
    back_f = give_back(0, ret_f, rr_f)

    receive(in_r, fw_r)

    @pl.loop(0, hidden_units // tile)
    def _(n):
        pre = dot(flat(rcv_r, 0), up[:half, cols(n)]) + dot(flat(rcv_r, 1), up[half:, cols(n)])
        t = jnp.tanh(ROOT * (pre + CUBE * pre * pre * pre))
        slope = ROOT * (1.0 + 3.0 * CUBE * pre * pre)
        dgelu[:, cols(n)] = 0.5 * (1.0 + t) + 0.5 * pre * (1.0 - t * t) * slope

    receive(in_g, fw_g)

    @pl.loop(0, hidden_units // tile)
    def _(n):
        back = dot(flat(rcv_g, 0), down[cols(n), :half], 1, 1) + dot(
            flat(rcv_g, 1), down[cols(n), half:], 1, 1
        )
        act[:, cols(n)] = (back * dgelu[:, cols(n)]).astype(BF16)

    swap_b = exchange(
        1, px_b, pin_b, ret_b, lambda h, n: dot(act[...], up[cols(n, h * half), :], 1, 1)
    )
    back_b = give_back(1, ret_b, rr_b)

    weight = sum(jnp.where(fwd[k], fg_ref[:, k : k + 1], 0.0) for k in range(2))
    high = weight.astype(BF16)
    low = (weight - high.astype(F32)).astype(BF16)
    for k in order:
        back_f[k].wait_recv()
    sends_f = []
    for h in range(2):
        side = pl.ds(h * half, half)

        @pl.loop(0, half // tile)
        def _(n):
            got = rr_f[h, :, :, cols(n)].reshape(slots, tile)
            moe = dot(high, got) + dot(low, got)
            at = cols(n, h * half)
            out_f[:, at] = x_ref[:, at] + fm_ref[2:3, at] * moe

        copy = remote(
            out_f.at[:, side], next_ref.at[:, side], sf_send.at[h], sf_recv.at[h],
            (s + 1) % sections, me,
        )
        sends_f.append(copy)

        @pl.when(s < sections - 1)
        def _():
            copy.start()

    @pl.when(s == 0)
    def _():
        next_ref[...] = jnp.zeros_like(next_ref)

    @pl.when(s == sections - 1)
    def _():
        grad_ref[...] = jnp.zeros_like(grad_ref)

    for k in order:
        back_b[k].wait_recv()
    both = bwd_hot[0] + bwd_hot[1]
    for h in range(2):
        @pl.loop(0, half // tile)
        def _(n):
            got = rr_b[h, :, :, cols(n)].reshape(slots, tile)
            dh[:, cols(n, h * half)] = dot(both, got)

    pieces = 4
    part = count // pieces
    sends_b = []
    for p in range(pieces):
        @pl.loop(0, part // group)
        def _(i):
            at = pl.ds(pl.multiple_of(p * part + i * group, group), group)
            dnorm = dh[at, :] * (1.0 + bm_ref[1:2, :])
            normed = normed_b[at, :]
            one = jnp.mean(dnorm, axis=1, keepdims=True)
            two = jnp.mean(dnorm * normed, axis=1, keepdims=True)
            out_b[at, :] = (
                og_ref[at, :].astype(F32) + (dnorm - one - normed * two) * inv_b[at, 0:1]
            ).astype(BF16)

        piece = pl.ds(p * part, part)
        copy = remote(
            out_b.at[piece], grad_ref.at[piece], sb_send.at[p], sb_recv.at[p],
            (s + sections - 1) % sections, me,
        )
        sends_b.append(copy)

        @pl.when(s > 0)
        def _():
            copy.start()

    for copies in (in_f, in_r, in_g, fw_f, fw_r, fw_g, back_f, back_b):
        for copy in copies.values():
            copy.wait_send()
    swap_f.wait_send()
    swap_b.wait_send()

    @pl.when(s < sections - 1)
    def _():
        for copy in sends_f:
            copy.wait_send()
        for copy in sends_b:
            copy.wait_recv()

    @pl.when(s > 0)
    def _():
        for copy in sends_f:
            copy.wait_recv()
        for copy in sends_b:
            copy.wait_send()


def run_many(
    section_inputs,
    stored_inputs,
    out_grads,
    fwd_routes,
    fwd_gates,
    fwd_modulation,
    bwd_routes,
    bwd_gates,
    bwd_modulation,
    up_weight,
    down_weight,
):
    sections, units = lax.axis_size("section"), lax.axis_size("expert")
    experts = units // 2
    count, width = section_inputs.shape[1:]
    hidden_units = up_weight.shape[3]
    half = width // 2
    capacity = -(-min(count, 5 * count // (2 * experts)) // 16) * 16
    rows = units * capacity

    def vmem(dtype, *shape):
        return pltpu.VMEM(shape, dtype)

    def dma(*shape):
        return pltpu.SemaphoreType.DMA(shape)

    scratch = [
        vmem(BF16, width, hidden_units),
        vmem(BF16, hidden_units, width),
        *[vmem(BF16, experts, 2, capacity, half)] * 3,
        *[vmem(BF16, 2, units, capacity, half)] * 3,
        vmem(BF16, rows, hidden_units),
        vmem(F32, rows, hidden_units),
        *[vmem(BF16, units, capacity, half)] * 6,
        *[vmem(BF16, 2, experts, capacity, half)] * 2,
        *[vmem(BF16, count, width)] * 3,
        vmem(F32, count, width),
        vmem(F32, count, 128),
        *[vmem(F32, count, width)] * 2,
        vmem(BF16, count, width),
        dma(2),
        *[dma(3, units)] * 4,
        *[dma(2)] * 2,
        *[dma(2, units)] * 2,
        *[dma(2)] * 2,
        *[dma(4)] * 2,
    ]
    in_vmem = pl.BlockSpec(memory_space=pltpu.VMEM)
    in_hbm = pl.BlockSpec(memory_space=pl.ANY)
    flops = 10 * rows * width * hidden_units
    next_inputs, input_grads = pl.pallas_call(
        functools.partial(many_chips, sections, units, capacity),
        out_shape=(
            jax.ShapeDtypeStruct((count, width), F32),
            jax.ShapeDtypeStruct((count, width), BF16),
        ),
        in_specs=[in_vmem] * 9 + [in_hbm] * 2,
        out_specs=(in_vmem, in_vmem),
        scratch_shapes=scratch,
        compiler_params=pltpu.CompilerParams(
            collective_id=0, has_side_effects=True, vmem_limit_bytes=67043328
        ),
        cost_estimate=pl.CostEstimate(
            flops=flops, bytes_accessed=4 * width * hidden_units, transcendentals=0
        ),
    )(
        section_inputs[0], stored_inputs[0], out_grads[0], fwd_routes[0], fwd_gates[0],
        fwd_modulation[0], bwd_routes[0], bwd_gates[0], bwd_modulation[0],
        up_weight[0, 0], down_weight[0, 0],
    )
    return next_inputs[None], input_grads[None]


def two_sided(
    sections, units, capacity, chunks, pieces,
    x_hbm, st_hbm, og_hbm, fr_hbm, fg_hbm, fm_hbm, br_hbm, bg_hbm, bm_hbm, up_hbm, down_hbm,
    next_ref, grad_ref,
    fr_ref, fg_ref, fm_ref, br_ref, bg_ref, bm_ref,
    up, down, x_v, x_prev, st_v, dense, near, cross, snd_p, relay, rows, act, agrad,
    res, ret_p, ret_x, comb, den, normed_b, inv_b, m_out, m_in, dh, out_b,
    meta, picks, gate,
    load_sem, small_sem, send_sem, w_recv, meta_send, meta_recv, x_recv, near_recv,
    cross_recv, rows_recv, retp_recv, retx_recv, den_recv, den_all_recv, sf_recv, sb_recv,
):
    s, me = lax.axis_index("section"), lax.axis_index("expert")
    z, c = me // 2, me % 2
    odd, side = z % 2, z // 2
    inner = odd + side - 2 * odd * side
    seat = 1 - inner
    partner = z + 1 - 2 * odd
    crossing = [2 - side, 3 - 3 * side]
    is_inner, is_outer = inner == 1, inner == 0
    count, width = x_v.shape
    hidden = up.shape[2]
    every = 4 * capacity
    tile, group = 256, 16
    chunk, piece = width // chunks, width // pieces
    OG, HB, HF = 0, 1, 2
    FWD, BWD = 0, 1
    scope = jax.named_scope

    def unit(chip):
        return 2 * chip + c

    def remote(src, dst, send, recv, section, to):
        return pltpu.make_async_remote_copy(
            src_ref=src, dst_ref=dst, send_sem=send, recv_sem=recv,
            device_id=(section, to), device_id_type=MESH,
        )

    def cols(n, size):
        return pl.ds(pl.multiple_of(n * size, size), size)

    loads = [
        pltpu.make_async_copy(og_hbm, dense.at[OG], load_sem.at[0]),
        pltpu.make_async_copy(st_hbm, st_v, load_sem.at[1]),
        pltpu.make_async_copy(x_hbm, x_v, load_sem.at[2]),
        pltpu.make_async_copy(up_hbm, up.at[c], load_sem.at[3]),
        pltpu.make_async_copy(down_hbm, down.at[c], load_sem.at[4]),
    ]
    smalls = [
        pltpu.make_async_copy(src, dst, small_sem.at[k])
        for k, (src, dst) in enumerate([
            (fr_hbm, fr_ref), (fg_hbm, fg_ref), (br_hbm, br_ref), (bg_hbm, bg_ref),
            (bm_hbm, bm_ref), (fm_hbm, fm_ref),
        ])
    ]
    for load in smalls[:4] + loads[:3] + smalls[4:]:
        load.start()

    barrier = pltpu.get_barrier_semaphore()
    for chip in (partner, crossing[0], crossing[1]):
        pl.semaphore_signal(barrier, inc=1, device_id=(s, unit(chip)), device_id_type=MESH)
    twin = me + 1 - 2 * c
    pl.semaphore_signal(barrier, inc=1, device_id=(s, twin), device_id_type=MESH)
    for step in (1, sections - 1):
        pl.semaphore_signal(
            barrier, inc=1, device_id=((s + step) % sections, me), device_id_type=MESH
        )

    for load in smalls[:4]:
        load.wait()
    meta[0, 0:2, :] = fr_ref[...].astype(F32)
    meta[0, 2:4, :] = fg_ref[...]
    meta[0, 4:6, :] = br_ref[...].astype(F32)
    meta[0, 6:8, :] = bg_ref[...]

    metas = [
        remote(meta.at[0], meta.at[1], meta_send.at[0], meta_recv.at[0], s, unit(partner)),
        remote(
            meta.at[0], meta.at[2 + seat], meta_send.at[1], meta_recv.at[1 + seat],
            s, unit(crossing[0]),
        ),
        remote(
            meta.at[0], meta.at[2 + seat], meta_send.at[2], meta_recv.at[1 + seat],
            s, unit(crossing[1]),
        ),
    ]
    shares = 4
    S_UP, S_DOWN, S_NEAR, S_CROSS, S_PART, S_RELAY, S_RETP, S_RETX, S_DEN, S_AHEAD, S_BACK, S_X = [
        send_sem.at[k] for k in range(12)
    ]

    def twin_share(w, p):
        src, dst, sem = ((up_hbm, up, S_UP), (down_hbm, down, S_DOWN))[w]
        size = src.shape[0] // shares
        at = pl.ds(p * size, size)
        return remote(src.at[at], dst.at[c, at], sem, w_recv.at[w], s, twin)

    def twin_whole(w, slot):
        src, dst, sem = ((up_hbm, up, S_UP), (down_hbm, down, S_DOWN))[w]
        return remote(src, dst.at[slot], sem, w_recv.at[w], s, twin)

    def near_copy(q, n):
        at = cols(n, chunk)
        return remote(
            dense.at[q, :, at], near.at[q, :, at],
            S_NEAR, near_recv.at[q, n], s, unit(partner),
        )

    def cross_copy(q, i, n):
        at = cols(n, chunk)
        src = dense if i == 0 else near
        return remote(
            src.at[q, :, at], cross.at[q, i, :, at],
            S_CROSS, cross_recv.at[q, i, n], s, unit(crossing[0]),
        )

    def part_copy(q, n):
        at = cols(n, chunk)
        return remote(
            snd_p.at[q, :, at], rows.at[q, 1, :, at],
            S_PART, rows_recv.at[q], s, unit(partner),
        )

    def relay_copy(q, i, n):
        at = cols(n, chunk)
        return remote(
            relay.at[q, i, :, at], rows.at[q, 2 + i, :, at],
            S_RELAY, rows_recv.at[q], s, unit(partner),
        )

    def retp_copy(r, n):
        at = cols(n, piece)
        return remote(
            res.at[r, 1, :, at], ret_p.at[r, :, at],
            S_RETP, retp_recv.at[r], s, unit(partner),
        )

    def retx_copy(r, i, n):
        at = cols(n, piece)
        return remote(
            res.at[r, 2 + i, :, at], ret_x.at[r, i, :, at],
            S_RETX, retx_recv.at[r, n], s, unit(partner),
        )

    def den_copy(r, i, n):
        at = cols(n, piece)
        return remote(
            comb.at[r, i, :, at], den.at[r, :, at],
            S_DEN, den_all_recv.at[0] if r == BWD else den_recv.at[n], s, unit(crossing[i]),
        )

    x_copy = remote(x_v, x_prev, S_X, x_recv.at[0], (s + 1) % sections, me)

    def ahead_copy(n):
        at = cols(n, piece)
        return remote(
            m_out.at[:, at], m_in.at[:, at], S_AHEAD, sf_recv.at[n],
            (s + 1) % sections, me,
        )

    parts = 4
    part = count // parts

    def back_copy(p):
        at = cols(p, part)
        return remote(
            out_b.at[at], grad_ref.at[at], S_BACK, sb_recv.at[0],
            (s + sections - 1) % sections, me,
        )

    def each_chunk(body):
        pl.loop(0, chunks)(body)

    def each_piece(body):
        pl.loop(0, pieces)(body)

    row16 = lax.broadcasted_iota(jnp.int32, (16, count), 0)
    named = jnp.where(row16 % 2 == 0, z, partner).astype(F32)
    forward = row16 < 2
    earlier = lax.broadcasted_iota(jnp.int32, (count, count), 0)
    later = lax.broadcasted_iota(jnp.int32, (count, count), 1)
    upper = jnp.where(earlier < later, 1.0, 0.0).astype(BF16)
    places = lax.broadcasted_iota(jnp.int32, (capacity, count), 0).astype(F32)

    def find(j):
        first = jnp.where(forward, meta[j, 0:1, :], meta[j, 4:5, :]) == named
        second = jnp.where(forward, meta[j, 1:2, :], meta[j, 5:6, :]) == named
        weight = jnp.where(
            first,
            jnp.where(forward, meta[j, 2:3, :], meta[j, 6:7, :]),
            jnp.where(forward, meta[j, 3:4, :], meta[j, 7:8, :]),
        )
        chosen = first | second
        before = dot(jnp.where(chosen, 1.0, 0.0).astype(BF16), upper)
        place = jnp.where(chosen, before, -1.0)
        for b in range(2):
            for k in range(2):
                row = slice(2 * b + k, 2 * b + k + 1)
                hit = places == place[row]
                picks[b, j, k] = jnp.where(hit, 1.0, 0.0).astype(BF16)
                if k == 0:
                    value = jnp.sum(jnp.where(hit, weight[row], 0.0), axis=1, keepdims=True)
                    gate[b, j] = jnp.broadcast_to(value, (capacity, 128))

    def pack_own(q, b):
        @each_chunk
        def _(n):
            at = cols(n, chunk)

            @pl.when(is_inner)
            def _():
                snd_p[q, :, at] = dot(picks[b, 0, 1], dense[q, :, at]).astype(BF16)
                part_copy(q, n).start()

            rows[q, 0, :, at] = dot(picks[b, 0, 0], dense[q, :, at]).astype(BF16)

    def normalise(src, mod, q, keep):
        @pl.loop(0, count // group)
        def _(i):
            at = pl.ds(pl.multiple_of(i * group, group), group)
            x = src[at, :]
            centered = x - jnp.mean(x, axis=1, keepdims=True)
            inv = lax.rsqrt(jnp.mean(centered * centered, axis=1, keepdims=True) + norm_eps)
            normed = centered * inv
            dense[q, at, :] = (normed * (1.0 + mod[1]) + mod[0]).astype(BF16)
            if keep:
                normed_b[at, :] = normed
                inv_b[at, :] = jnp.broadcast_to(inv, (group, 128))

    def send_near(q):
        @pl.when(is_outer)
        def _():
            each_chunk(lambda n: near_copy(q, n).start())

    def send_cross(q):
        @pl.when(is_inner)
        def _():
            each_chunk(lambda n: cross_copy(q, 0, n).start())

    def hand_over(q, b):
        @pl.when(is_inner)
        def _():
            @each_chunk
            def _(n):
                at = cols(n, chunk)
                near_copy(q, n).wait_recv()
                cross_copy(q, 1, n).start()
                rows[q, 1, :, at] = dot(picks[b, 1, 0], near[q, :, at]).astype(BF16)

    def pass_on(q, b, i, n):
        at = cols(n, chunk)
        cross_copy(q, i, n).wait_recv()
        relay[q, i, :, at] = dot(picks[b, 2 + i, 1], cross[q, i, :, at]).astype(BF16)
        relay_copy(q, i, n).start()
        rows[q, 2 + i, :, at] = dot(picks[b, 2 + i, 0], cross[q, i, :, at]).astype(BF16)

    def gather(q, b, i):
        @pl.when(is_inner)
        def _():
            each_chunk(lambda n: pass_on(q, b, i, n))

    def gathered(q):
        @pl.when(is_outer)
        def _():
            got = rows.at[q, 1:4]
            remote(got, got, S_RELAY, rows_recv.at[q], s, unit(partner)).wait_recv()

    def flat(q):
        return rows[q].reshape(every, width)

    def give(r, n, value):
        at = cols(n, piece)
        value = value.astype(BF16).reshape(4, capacity, piece)
        for j in range(4):
            res[r, j, :, at] = value[j]

        @pl.when(is_outer)
        def _():
            for i in range(2):
                retx_copy(r, i, n).start()

    def give_late(r):
        each_piece(lambda n: retp_copy(r, n).start())

    def combine(r, b, n):
        at = cols(n, piece)
        got = ret_x.at[r, :, :, at]
        remote(got, got, S_RETX, retx_recv.at[r, n], s, unit(partner)).wait_recv()
        for i in range(2):
            total = dot(picks[b, 2 + i, 0], res[r, 2 + i, :, at], 0, 0) + dot(
                picks[b, 2 + i, 1], ret_x[r, i, :, at], 0, 0
            )
            comb[r, i, :, at] = total.astype(BF16)
            den_copy(r, i, n).start()

    def wait_returned(r):
        got = ret_p.at[r]
        remote(got, got, S_RETP, retp_recv.at[r], s, unit(partner)).wait_recv()

    def own_total(r, b, n):
        at = cols(n, piece)
        if r == FWD:
            den_copy(r, 0, n).wait_recv()
        return (
            dot(picks[b, 0, 0], res[r, 0, :, at], 0, 0)
            + dot(picks[b, 0, 1], ret_p[r, :, at], 0, 0)
            + den[r, :, at].astype(F32)
        )

    with scope("bar"):
        pl.semaphore_wait(barrier, 6)
    for copy in metas:
        copy.start()
    with scope("load0"):
        loads[0].wait()
        send_near(OG)
        send_cross(OG)
        loads[4].start()
        loads[3].start()
    with scope("find0"):
        find(0)
    with scope("pk_og"):
        pack_own(OG, BWD)
    twin_share(1, 0).start()
    with scope("norm1"):
        loads[1].wait()
        smalls[4].wait()
        normalise(st_v, bm_ref, HB, True)
        send_near(HB)
    twin_share(1, 1).start()
    with scope("pk_hb"):
        pack_own(HB, BWD)
    twin_share(1, 2).start()
    with scope("norm2"):
        loads[2].wait()
        smalls[5].wait()

        @pl.when(s < sections - 1)
        def _():
            x_copy.start()

        normalise(x_v, fm_ref, HF, False)
        send_near(HF)
        pack_own(HF, FWD)
    twin_share(1, 3).start()
    for j in range(1, 4):
        with scope(f"meta{j}"):
            remote(
                meta.at[0], meta.at[j], meta_send.at[j - 1], meta_recv.at[j - 1],
                s, unit(partner),
            ).wait_recv()
            find(j)
    with scope("over_og"):
        hand_over(OG, BWD)
        send_cross(HB)
    twin_share(0, 0).start()
    with scope("gat_og0"):
        gather(OG, BWD, 0)
    twin_share(0, 1).start()
    with scope("over_hb"):
        hand_over(HB, BWD)
        send_cross(HF)
    twin_share(0, 2).start()
    with scope("gat_og1"):
        gather(OG, BWD, 1)
    with scope("gathered_og"):
        gathered(OG)
    twin_share(0, 3).start()

    with scope("pair"):
        for j in range(4):
            @pl.loop(0, width // tile)
            def _(n):
                at = cols(n, tile)
                scaled = bm_ref[2, :, at] * rows[OG, j, :, at].astype(F32)
                rows[OG, j, :, at] = (gate[BWD, j, :, 0:1] * scaled).astype(BF16)

    with scope("wts"):
        loads[4].wait()
        twin_whole(1, 1 - c).wait_recv()

    with scope("agrad"):
        for h in range(2):
            @pl.loop(0, hidden // tile)
            def _(n):
                at = pl.ds(pl.multiple_of(h * hidden + n * tile, tile), tile)
                agrad[:, at] = dot(flat(OG), down[h, cols(n, tile), :], 1, 1)

    with scope("gat_hb0"):
        gather(HB, BWD, 0)
    with scope("over_hf"):
        hand_over(HF, FWD)
    with scope("gat_hb1"):
        gather(HB, BWD, 1)
    with scope("gathered_hb"):
        gathered(HB)
        loads[3].wait()
        twin_whole(0, 1 - c).wait_recv()

    with scope("pre"):
        for h in range(2):
            @pl.loop(0, hidden // tile)
            def _(n):
                at = pl.ds(pl.multiple_of(h * hidden + n * tile, tile), tile)
                pre = dot(flat(HB), up[h, :, cols(n, tile)])
                t = jnp.tanh(ROOT * (pre + CUBE * pre * pre * pre))
                slope = ROOT * (1.0 + 3.0 * CUBE * pre * pre)
                dgelu = 0.5 * (1.0 + t) + 0.5 * pre * (1.0 - t * t) * slope
                act[:, at] = (agrad[:, at] * dgelu).astype(BF16)

    with scope("partb"):
        @each_piece
        def _(n):
            at = cols(n, piece)
            give(
                BWD, n,
                dot(act[:, :hidden], up[0, at, :], 1, 1)
                + dot(act[:, hidden:], up[1, at, :], 1, 1),
            )

        @pl.when(is_outer)
        def _():
            give_late(BWD)

    with scope("gat_hf0"):
        gather(HF, FWD, 0)
    with scope("comb_b"):
        @pl.when(is_inner)
        def _():
            per = pieces // chunks

            @each_chunk
            def _(n):
                for k in range(per):
                    combine(BWD, BWD, n * per + k)
                with scope("gat_hf1"):
                    pass_on(HF, FWD, 1, n)

        @pl.when(is_inner)
        def _():
            give_late(BWD)

    with scope("gathered_hf"):
        gathered(HF)

    with scope("up"):
        for h in range(2):
            @pl.loop(0, hidden // tile)
            def _(n):
                at = pl.ds(pl.multiple_of(h * hidden + n * tile, tile), tile)
                pre = dot(flat(HF), up[h, :, cols(n, tile)])
                t = jnp.tanh(ROOT * (pre + CUBE * pre * pre * pre))
                act[:, at] = (0.5 * pre * (1.0 + t)).astype(BF16)

    weight = gate[FWD, :, :, 0:1].reshape(every, 1)

    with scope("down"):
        @each_piece
        def _(n):
            at = cols(n, piece)
            value = dot(act[:, :hidden], down[0, :, at]) + dot(act[:, hidden:], down[1, :, at])
            give(FWD, n, weight * value)

        give_late(FWD)

    with scope("comb_f"):
        @pl.when(is_inner)
        def _():
            each_piece(lambda n: combine(FWD, FWD, n))

    @pl.when(s == 0)
    def _():
        next_ref[...] = jnp.zeros_like(next_ref)

    @pl.when(s == sections - 1)
    def _():
        grad_ref[...] = jnp.zeros_like(grad_ref)

    with scope("own_b"):
        wait_returned(BWD)
        got = den.at[BWD]
        remote(got, got, S_DEN, den_all_recv.at[0], s, unit(partner)).wait_recv()

        @each_piece
        def _(n):
            dh[:, cols(n, piece)] = own_total(BWD, BWD, n)

    with scope("fin_b"):
        for p in range(parts):
            @pl.loop(0, part // group)
            def _(i):
                at = pl.ds(pl.multiple_of(p * part + i * group, group), group)
                dnorm = dh[at, :] * (1.0 + bm_ref[1])
                normed = normed_b[at, :]
                one = jnp.mean(dnorm, axis=1, keepdims=True)
                two = jnp.mean(dnorm * normed, axis=1, keepdims=True)
                out_b[at, :] = (
                    dense[OG, at, :].astype(F32) + (dnorm - one - normed * two) * inv_b[at, 0:1]
                ).astype(BF16)

            @pl.when(s > 0)
            def _():
                back_copy(p).start()

    def arrive(n):
        at = cols(n, piece)

        @pl.when(s > 0)
        def _():
            ahead_copy(n).wait_recv()
            next_ref[:, at] = x_prev[:, at] + m_in[:, at].astype(F32)

    with scope("own_f"):
        @pl.when(s > 0)
        def _():
            x_copy.wait_recv()

        wait_returned(FWD)
        lag = 2

        @each_piece
        def _(n):
            at = cols(n, piece)
            m_out[:, at] = (fm_ref[2, :, at] * own_total(FWD, FWD, n)).astype(BF16)

            @pl.when(s < sections - 1)
            def _():
                ahead_copy(n).start()

            @pl.when(n >= lag)
            def _():
                arrive(n - lag)

        for n in range(pieces - lag, pieces):
            arrive(n)

    with scope("tail_send"):
        def sent(sem, src):
            remote(src, src, sem, rows_recv.at[0], s, unit(partner)).wait_send()

        for copy in metas:
            copy.wait_send()
        for w in range(2):
            twin_whole(w, c).wait_send()
        sent(S_RETP, res.at[:, 1])

        @pl.when(is_outer)
        def _():
            sent(S_NEAR, dense)
            sent(S_RETX, res.at[:, 2:4])

        @pl.when(is_inner)
        def _():
            sent(S_PART, snd_p)
            sent(S_CROSS, cross)
            sent(S_RELAY, relay)
            sent(S_DEN, comb)

    with scope("tail_hop"):
        @pl.when(s < sections - 1)
        def _():
            x_copy.wait_send()
            sent(S_AHEAD, m_out)
            remote(grad_ref, grad_ref, S_BACK, sb_recv.at[0], s, twin).wait_recv()

        @pl.when(s > 0)
        def _():
            sent(S_BACK, out_b)


def run_two_sided(
    section_inputs,
    stored_inputs,
    out_grads,
    fwd_routes,
    fwd_gates,
    fwd_modulation,
    bwd_routes,
    bwd_gates,
    bwd_modulation,
    up_weight,
    down_weight,
):
    sections, units = lax.axis_size("section"), lax.axis_size("expert")
    experts = units // 2
    count, width = section_inputs.shape[1:]
    hidden = up_weight.shape[3]
    capacity = -(-min(count, 5 * count // (2 * experts)) // 16) * 16
    every = 4 * capacity
    chunks, pieces = 4, 8

    def vmem(dtype, *shape):
        return pltpu.VMEM(shape, dtype)

    def dma(*shape):
        return pltpu.SemaphoreType.DMA(shape)

    scratch = [
        vmem(jnp.int32, 2, count),
        vmem(F32, 2, count),
        vmem(F32, 3, 1, width),
        vmem(jnp.int32, 2, count),
        vmem(F32, 2, count),
        vmem(F32, 3, 1, width),
        vmem(BF16, 2, width, hidden),
        vmem(BF16, 2, hidden, width),
        *[vmem(F32, count, width)] * 3,
        *[vmem(BF16, 3, count, width)] * 2,
        vmem(BF16, 3, 2, count, width),
        vmem(BF16, 3, capacity, width),
        vmem(BF16, 3, 2, capacity, width),
        vmem(BF16, 3, 4, capacity, width),
        vmem(BF16, every, 2 * hidden),
        vmem(F32, every, 2 * hidden),
        vmem(BF16, 2, 4, capacity, width),
        vmem(BF16, 2, capacity, width),
        vmem(BF16, 2, 2, capacity, width),
        vmem(BF16, 2, 2, count, width),
        vmem(BF16, 2, count, width),
        vmem(F32, count, width),
        vmem(F32, count, 128),
        *[vmem(BF16, count, width)] * 2,
        vmem(F32, count, width),
        vmem(BF16, count, width),
        vmem(F32, 4, 8, count),
        vmem(BF16, 2, 4, 2, capacity, count),
        vmem(F32, 2, 4, capacity, 128),
        dma(5),
        dma(6),
        dma(12),
        dma(2),
        *[dma(3)] * 2,
        dma(1),
        dma(3, chunks),
        dma(3, 2, chunks),
        dma(3),
        dma(2),
        dma(2, pieces),
        dma(pieces),
        dma(1),
        dma(pieces),
        dma(1),
    ]
    in_vmem = pl.BlockSpec(memory_space=pltpu.VMEM)
    in_hbm = pl.BlockSpec(memory_space=pltpu.HBM)
    flops = 20 * every * width * hidden
    next_inputs, input_grads = pl.pallas_call(
        functools.partial(two_sided, sections, units, capacity, chunks, pieces),
        out_shape=(
            jax.ShapeDtypeStruct((count, width), F32),
            jax.ShapeDtypeStruct((count, width), BF16),
        ),
        in_specs=[in_hbm] * 11,
        out_specs=(in_vmem, in_vmem),
        scratch_shapes=scratch,
        compiler_params=pltpu.CompilerParams(
            collective_id=1, has_side_effects=True, vmem_limit_bytes=50 << 20
        ),
        cost_estimate=pl.CostEstimate(
            flops=flops, bytes_accessed=4 * width * hidden, transcendentals=0
        ),
    )(*[pltpu.with_memory_space_constraint(array, pltpu.HBM) for array in (
        section_inputs[0], stored_inputs[0], out_grads[0],
        fwd_routes[0].T, fwd_gates[0].T, jnp.transpose(fwd_modulation, (1, 0, 2)),
        bwd_routes[0].T, bwd_gates[0].T, jnp.transpose(bwd_modulation, (1, 0, 2)),
        up_weight[0, 0], down_weight[0, 0],
    )])
    return next_inputs[None], input_grads[None]


def on_device(*arrays):
    sides, inner_and_outer = 2, 2
    line = lax.axis_size("expert") == 2 * sides * inner_and_outer
    return (run_two_sided if line else run_many)(*arrays)


def solution(mesh):
    tokens = P("section", "expert", None)
    shared = P("section", None, None)
    weights = P("section", "expert", None, None)
    placed = (tokens,) * 5 + (shared,) + (tokens,) * 2 + (shared,) + (weights,) * 2
    return jax.shard_map(
        on_device,
        mesh=mesh,
        in_specs=placed,
        out_specs=(tokens, tokens),
        check_vma=False,
    )
```

```python
import functools

import jax
import jax.numpy as jnp
from jax import lax
from jax.experimental import pallas as pl
from jax.experimental.pallas import tpu as pltpu
from jax.sharding import PartitionSpec as P

norm_eps = 1e-06
F32, BF16 = jnp.float32, jnp.bfloat16
MESH = pl.DeviceIdType.MESH
ROOT, CUBE = 0.7978845608028654, 0.044715


def flip(index, mask, bits):
    total = 0
    for b in range(bits):
        bit = (index // (1 << b)) % 2
        total = total + (1 << b) * (1 - bit if mask >> b & 1 else bit)
    return total


def dot(a, b, ca=1, cb=0):
    return lax.dot_general(a, b, (((ca,), (cb,)), ((), ())), preferred_element_type=F32)


def slot_masks(routes, capacity, slots):
    count = routes.shape[0]
    lanes = lax.broadcasted_iota(jnp.int32, (count, 128), 1)
    hits = [routes[:, k : k + 1] == lanes for k in range(2)]
    choose = jnp.where(hits[0] | hits[1], 1.0, 0.0).astype(BF16)
    row = lax.broadcasted_iota(jnp.int32, (count, count), 0)
    col = lax.broadcasted_iota(jnp.int32, (count, count), 1)
    before = dot(jnp.where(col < row, 1.0, 0.0).astype(BF16), choose)
    places = lax.broadcasted_iota(jnp.int32, (count, slots), 1)
    masks = []
    for k in range(2):
        rank = jnp.sum(jnp.where(hits[k], before, 0.0), axis=1, keepdims=True)
        masks.append(places == routes[:, k : k + 1] * capacity + rank.astype(jnp.int32))
    return masks


def many_chips(
    sections, units, capacity,
    x_ref, st_ref, og_ref, fr_ref, fg_ref, fm_ref, br_ref, bg_ref, bm_ref, up_hbm, down_hbm,
    next_ref, grad_ref,
    up, down, snd_f, snd_r, snd_g, rcv_f, rcv_r, rcv_g, act, dgelu,
    px_f, px_b, pin_f, pin_b, ret_f, ret_b, rr_f, rr_b,
    hid, pair0, pair1, normed_b, inv_b, out_f, dh, out_b,
    w_sem, in_send, in_recv, fw_send, fw_recv, px_send, px_recv, rt_send, rt_recv,
    sf_send, sf_recv, sb_send, sb_recv,
):
    s, me = lax.axis_index("section"), lax.axis_index("expert")
    experts = units // 2
    bits = units.bit_length() - 1
    chip, core = me // 2, me % 2
    count, width = x_ref.shape
    half = width // 2
    hidden_units = up.shape[1]
    rows = units * capacity
    slots = experts * capacity
    tile = 256
    group = 16
    order = list(range(1, units))
    peer = {k: flip(me, k, bits) for k in order}

    w_up = pltpu.make_async_copy(up_hbm, up, w_sem.at[0])
    w_down = pltpu.make_async_copy(down_hbm, down, w_sem.at[1])
    w_up.start()
    w_down.start()

    barrier = pltpu.get_barrier_semaphore()
    for k in order:
        pl.semaphore_signal(barrier, inc=1, device_id=(s, peer[k]), device_id_type=MESH)
    for step in (1, sections - 1):
        pl.semaphore_signal(
            barrier, inc=1, device_id=((s + step) % sections, me), device_id_type=MESH
        )

    def remote(src, dst, send, recv, section, unit):
        return pltpu.make_async_remote_copy(
            src_ref=src, dst_ref=dst, send_sem=send, recv_sem=recv,
            device_id=(section, unit), device_id_type=MESH,
        )

    def inbound(phase, snd, rcv):
        copies = {}
        for k in order:
            d = peer[k]
            if k == 1:
                src, dst = snd.at[chip], rcv.at[:, me]
            else:
                src, dst = snd.at[d // 2, d % 2], rcv.at[d % 2, me]
            copies[k] = remote(src, dst, in_send.at[phase, k], in_recv.at[phase, k], s, d)
        return copies

    def hand_on(phase, rcv):
        copies = {}
        for k in order:
            if k > 1:
                block = rcv.at[core, peer[k]]
                copies[k] = remote(
                    block, block, fw_send.at[phase, k], fw_recv.at[phase, k], s, peer[1]
                )
        return copies

    def keep_own(snd, rcv):
        for h in range(2):
            rcv[h, me] = snd[chip, h]

    def receive(ins, fws):
        for k in order:
            ins[k].wait_recv()
            if k > 1:
                fws[k].start()
        for k in order:
            if k > 1:
                fws[k].wait_recv()

    def normalise(src, mod, keep):
        @pl.loop(0, count // group)
        def _(i):
            at = pl.ds(pl.multiple_of(i * group, group), group)
            x = src[at, :]
            centered = x - jnp.mean(x, axis=1, keepdims=True)
            inv = lax.rsqrt(jnp.mean(centered * centered, axis=1, keepdims=True) + norm_eps)
            normed = centered * inv
            hid[at, :] = (normed * (1.0 + mod[1:2, :]) + mod[0:1, :]).astype(BF16)
            if keep:
                normed_b[at, :] = normed
                inv_b[at, :] = jnp.broadcast_to(inv, (group, 128))

    def pack(terms, snd):
        for h in range(2):
            @pl.loop(0, half // tile)
            def _(n):
                src = pl.ds(pl.multiple_of(h * half + n * tile, tile), tile)
                value = sum(dot(mask, ref[:, src], 0, 0) for mask, ref in terms).astype(BF16)
                for e in range(experts):
                    snd[e, h, :, pl.ds(pl.multiple_of(n * tile, tile), tile)] = value[
                        e * capacity : (e + 1) * capacity, :
                    ]

    def onehot(mask):
        return jnp.where(mask, 1.0, 0.0).astype(BF16)

    normalise(x_ref, fm_ref, False)
    fwd = slot_masks(fr_ref[...], capacity, slots)
    pack([(onehot(fwd[0] | fwd[1]), hid)], snd_f)
    pl.semaphore_wait(barrier, units + 1)
    in_f, fw_f = inbound(0, snd_f, rcv_f), hand_on(0, rcv_f)
    for k in order:
        in_f[k].start()
    keep_own(snd_f, rcv_f)

    normalise(st_ref, bm_ref, True)
    bwd = slot_masks(br_ref[...], capacity, slots)
    bwd_hot = [onehot(mask) for mask in bwd]
    pack([(bwd_hot[0] + bwd_hot[1], hid)], snd_r)
    in_r, fw_r = inbound(1, snd_r, rcv_r), hand_on(1, rcv_r)
    for k in order:
        in_r[k].start()
    keep_own(snd_r, rcv_r)

    @pl.loop(0, count // group)
    def _(i):
        at = pl.ds(pl.multiple_of(i * group, group), group)
        scaled = bm_ref[2:3, :] * og_ref[at, :].astype(F32)
        pair0[at, :] = (bg_ref[at, 0:1] * scaled).astype(BF16)
        pair1[at, :] = (bg_ref[at, 1:2] * scaled).astype(BF16)

    pack([(bwd_hot[0], pair0), (bwd_hot[1], pair1)], snd_g)
    in_g, fw_g = inbound(2, snd_g, rcv_g), hand_on(2, rcv_g)
    for k in order:
        in_g[k].start()
    keep_own(snd_g, rcv_g)

    def flat(ref, h):
        return ref[h].reshape(rows, half)

    def cols(n, base=0):
        return pl.ds(pl.multiple_of(base + n * tile, tile), tile)

    def exchange(phase, px, pin, ret, result):
        def fill(dst, h):
            @pl.loop(0, half // tile)
            def _(n):
                value = result(h, n).astype(BF16).reshape(units, capacity, tile)
                dst[:, :, cols(n)] = value

        fill(px, 1 - core)
        swap = remote(px, pin, px_send.at[phase], px_recv.at[phase], s, peer[1])
        swap.start()
        fill(ret, core)
        swap.wait_recv()

        @pl.loop(0, units)
        def _(u):
            ret[u] = (ret[u].astype(F32) + pin[u].astype(F32)).astype(BF16)

        return swap

    def give_back(phase, ret, rr):
        copies = {}
        for k in order:
            copies[k] = remote(
                ret.at[peer[k]], rr.at[core, chip],
                rt_send.at[phase, k], rt_recv.at[phase, k], s, peer[k],
            )
            copies[k].start()
        rr[core, chip] = ret[me]
        return copies

    receive(in_f, fw_f)
    w_up.wait()
    w_down.wait()

    @pl.loop(0, hidden_units // tile)
    def _(n):
        pre = dot(flat(rcv_f, 0), up[:half, cols(n)]) + dot(flat(rcv_f, 1), up[half:, cols(n)])
        t = jnp.tanh(ROOT * (pre + CUBE * pre * pre * pre))
        act[:, cols(n)] = (0.5 * pre * (1.0 + t)).astype(BF16)

    swap_f = exchange(
        0, px_f, pin_f, ret_f, lambda h, n: dot(act[...], down[:, cols(n, h * half)])
    )
    back_f = give_back(0, ret_f, rr_f)

    receive(in_r, fw_r)

    @pl.loop(0, hidden_units // tile)
    def _(n):
        pre = dot(flat(rcv_r, 0), up[:half, cols(n)]) + dot(flat(rcv_r, 1), up[half:, cols(n)])
        t = jnp.tanh(ROOT * (pre + CUBE * pre * pre * pre))
        slope = ROOT * (1.0 + 3.0 * CUBE * pre * pre)
        dgelu[:, cols(n)] = 0.5 * (1.0 + t) + 0.5 * pre * (1.0 - t * t) * slope

    receive(in_g, fw_g)

    @pl.loop(0, hidden_units // tile)
    def _(n):
        back = dot(flat(rcv_g, 0), down[cols(n), :half], 1, 1) + dot(
            flat(rcv_g, 1), down[cols(n), half:], 1, 1
        )
        act[:, cols(n)] = (back * dgelu[:, cols(n)]).astype(BF16)

    swap_b = exchange(
        1, px_b, pin_b, ret_b, lambda h, n: dot(act[...], up[cols(n, h * half), :], 1, 1)
    )
    back_b = give_back(1, ret_b, rr_b)

    weight = sum(jnp.where(fwd[k], fg_ref[:, k : k + 1], 0.0) for k in range(2))
    high = weight.astype(BF16)
    low = (weight - high.astype(F32)).astype(BF16)
    for k in order:
        back_f[k].wait_recv()
    sends_f = []
    for h in range(2):
        side = pl.ds(h * half, half)

        @pl.loop(0, half // tile)
        def _(n):
            got = rr_f[h, :, :, cols(n)].reshape(slots, tile)
            moe = dot(high, got) + dot(low, got)
            at = cols(n, h * half)
            out_f[:, at] = x_ref[:, at] + fm_ref[2:3, at] * moe

        copy = remote(
            out_f.at[:, side], next_ref.at[:, side], sf_send.at[h], sf_recv.at[h],
            (s + 1) % sections, me,
        )
        sends_f.append(copy)

        @pl.when(s < sections - 1)
        def _():
            copy.start()

    @pl.when(s == 0)
    def _():
        next_ref[...] = jnp.zeros_like(next_ref)

    @pl.when(s == sections - 1)
    def _():
        grad_ref[...] = jnp.zeros_like(grad_ref)

    for k in order:
        back_b[k].wait_recv()
    both = bwd_hot[0] + bwd_hot[1]
    for h in range(2):
        @pl.loop(0, half // tile)
        def _(n):
            got = rr_b[h, :, :, cols(n)].reshape(slots, tile)
            dh[:, cols(n, h * half)] = dot(both, got)

    pieces = 4
    part = count // pieces
    sends_b = []
    for p in range(pieces):
        @pl.loop(0, part // group)
        def _(i):
            at = pl.ds(pl.multiple_of(p * part + i * group, group), group)
            dnorm = dh[at, :] * (1.0 + bm_ref[1:2, :])
            normed = normed_b[at, :]
            one = jnp.mean(dnorm, axis=1, keepdims=True)
            two = jnp.mean(dnorm * normed, axis=1, keepdims=True)
            out_b[at, :] = (
                og_ref[at, :].astype(F32) + (dnorm - one - normed * two) * inv_b[at, 0:1]
            ).astype(BF16)

        piece = pl.ds(p * part, part)
        copy = remote(
            out_b.at[piece], grad_ref.at[piece], sb_send.at[p], sb_recv.at[p],
            (s + sections - 1) % sections, me,
        )
        sends_b.append(copy)

        @pl.when(s > 0)
        def _():
            copy.start()

    for copies in (in_f, in_r, in_g, fw_f, fw_r, fw_g, back_f, back_b):
        for copy in copies.values():
            copy.wait_send()
    swap_f.wait_send()
    swap_b.wait_send()

    @pl.when(s < sections - 1)
    def _():
        for copy in sends_f:
            copy.wait_send()
        for copy in sends_b:
            copy.wait_recv()

    @pl.when(s > 0)
    def _():
        for copy in sends_f:
            copy.wait_recv()
        for copy in sends_b:
            copy.wait_send()


def run_many(
    section_inputs,
    stored_inputs,
    out_grads,
    fwd_routes,
    fwd_gates,
    fwd_modulation,
    bwd_routes,
    bwd_gates,
    bwd_modulation,
    up_weight,
    down_weight,
):
    sections, units = lax.axis_size("section"), lax.axis_size("expert")
    experts = units // 2
    count, width = section_inputs.shape[1:]
    hidden_units = up_weight.shape[3]
    half = width // 2
    capacity = -(-min(count, 5 * count // (2 * experts)) // 16) * 16
    rows = units * capacity

    def vmem(dtype, *shape):
        return pltpu.VMEM(shape, dtype)

    def dma(*shape):
        return pltpu.SemaphoreType.DMA(shape)

    scratch = [
        vmem(BF16, width, hidden_units),
        vmem(BF16, hidden_units, width),
        *[vmem(BF16, experts, 2, capacity, half)] * 3,
        *[vmem(BF16, 2, units, capacity, half)] * 3,
        vmem(BF16, rows, hidden_units),
        vmem(F32, rows, hidden_units),
        *[vmem(BF16, units, capacity, half)] * 6,
        *[vmem(BF16, 2, experts, capacity, half)] * 2,
        *[vmem(BF16, count, width)] * 3,
        vmem(F32, count, width),
        vmem(F32, count, 128),
        *[vmem(F32, count, width)] * 2,
        vmem(BF16, count, width),
        dma(2),
        *[dma(3, units)] * 4,
        *[dma(2)] * 2,
        *[dma(2, units)] * 2,
        *[dma(2)] * 2,
        *[dma(4)] * 2,
    ]
    in_vmem = pl.BlockSpec(memory_space=pltpu.VMEM)
    in_hbm = pl.BlockSpec(memory_space=pl.ANY)
    flops = 10 * rows * width * hidden_units
    next_inputs, input_grads = pl.pallas_call(
        functools.partial(many_chips, sections, units, capacity),
        out_shape=(
            jax.ShapeDtypeStruct((count, width), F32),
            jax.ShapeDtypeStruct((count, width), BF16),
        ),
        in_specs=[in_vmem] * 9 + [in_hbm] * 2,
        out_specs=(in_vmem, in_vmem),
        scratch_shapes=scratch,
        compiler_params=pltpu.CompilerParams(
            collective_id=0, has_side_effects=True, vmem_limit_bytes=67043328
        ),
        cost_estimate=pl.CostEstimate(
            flops=flops, bytes_accessed=4 * width * hidden_units, transcendentals=0
        ),
    )(
        section_inputs[0], stored_inputs[0], out_grads[0], fwd_routes[0], fwd_gates[0],
        fwd_modulation[0], bwd_routes[0], bwd_gates[0], bwd_modulation[0],
        up_weight[0, 0], down_weight[0, 0],
    )
    return next_inputs[None], input_grads[None]


def two_sided(
    sections, units, capacity, chunks, pieces,
    x_hbm, st_hbm, og_hbm, fr_hbm, fg_hbm, fm_hbm, br_hbm, bg_hbm, bm_hbm, up_hbm, down_hbm,
    next_ref, grad_ref,
    fr_ref, fg_ref, fm_ref, br_ref, bg_ref, bm_ref,
    up, down, x_v, x_prev, st_v, dense, near, cross, snd_p, relay, rows, act, agrad,
    res, ret_p, ret_x, comb, den, normed_b, inv_b, m_out, m_in, dh, out_b,
    meta, picks, gate,
    load_sem, small_sem, send_sem, near_send, w_recv, meta_send, meta_recv, x_recv, near_recv,
    cross_recv, rows_recv, retp_recv, retx_recv, den_recv, den_all_recv, sf_recv, sb_recv,
):
    s, me = lax.axis_index("section"), lax.axis_index("expert")
    z, c = me // 2, me % 2
    odd, side = z % 2, z // 2
    inner = odd + side - 2 * odd * side
    seat = 1 - inner
    partner = z + 1 - 2 * odd
    crossing = [2 - side, 3 - 3 * side]
    is_inner, is_outer = inner == 1, inner == 0
    count, width = x_v.shape
    hidden = up.shape[2]
    every = 4 * capacity
    tile, group = 256, 16
    chunk, piece = width // chunks, width // pieces
    OG, HB, HF = 0, 1, 2
    FWD, BWD = 0, 1
    scope = jax.named_scope

    def unit(chip):
        return 2 * chip + c

    def remote(src, dst, send, recv, section, to):
        return pltpu.make_async_remote_copy(
            src_ref=src, dst_ref=dst, send_sem=send, recv_sem=recv,
            device_id=(section, to), device_id_type=MESH,
        )

    def cols(n, size):
        return pl.ds(pl.multiple_of(n * size, size), size)

    loads = [
        pltpu.make_async_copy(og_hbm, dense.at[OG], load_sem.at[0]),
        pltpu.make_async_copy(st_hbm, st_v, load_sem.at[1]),
        pltpu.make_async_copy(x_hbm, x_v, load_sem.at[2]),
        pltpu.make_async_copy(up_hbm, up.at[c], load_sem.at[3]),
        pltpu.make_async_copy(down_hbm, down.at[c], load_sem.at[4]),
    ]
    smalls = [
        pltpu.make_async_copy(src, dst, small_sem.at[k])
        for k, (src, dst) in enumerate([
            (fr_hbm, fr_ref), (fg_hbm, fg_ref), (br_hbm, br_ref), (bg_hbm, bg_ref),
            (bm_hbm, bm_ref), (fm_hbm, fm_ref),
        ])
    ]
    for load in smalls[:4] + loads[:3] + smalls[4:]:
        load.start()

    barrier = pltpu.get_barrier_semaphore()
    for chip in (partner, crossing[0], crossing[1]):
        pl.semaphore_signal(barrier, inc=1, device_id=(s, unit(chip)), device_id_type=MESH)
    twin = me + 1 - 2 * c
    pl.semaphore_signal(barrier, inc=1, device_id=(s, twin), device_id_type=MESH)
    for step in (1, sections - 1):
        pl.semaphore_signal(
            barrier, inc=1, device_id=((s + step) % sections, me), device_id_type=MESH
        )

    for load in smalls[:4]:
        load.wait()
    meta[0, 0:2, :] = fr_ref[...].astype(F32)
    meta[0, 2:4, :] = fg_ref[...]
    meta[0, 4:6, :] = br_ref[...].astype(F32)
    meta[0, 6:8, :] = bg_ref[...]

    metas = [
        remote(meta.at[0], meta.at[1], meta_send.at[0], meta_recv.at[0], s, unit(partner)),
        remote(
            meta.at[0], meta.at[2 + seat], meta_send.at[1], meta_recv.at[1 + seat],
            s, unit(crossing[0]),
        ),
        remote(
            meta.at[0], meta.at[2 + seat], meta_send.at[2], meta_recv.at[1 + seat],
            s, unit(crossing[1]),
        ),
    ]
    shares = 4
    S_UP, S_DOWN, S_CROSS, S_PART, S_RELAY, S_RETP, S_RETX, S_DEN, S_AHEAD, S_BACK, S_X = [
        send_sem.at[k] for k in range(11)
    ]
    S_NEAR = near_send

    def twin_share(w, p):
        src, dst, sem = ((up_hbm, up, S_UP), (down_hbm, down, S_DOWN))[w]
        size = src.shape[0] // shares
        at = pl.ds(p * size, size)
        return remote(src.at[at], dst.at[c, at], sem, w_recv.at[w], s, twin)

    def twin_whole(w, slot):
        src, dst, sem = ((up_hbm, up, S_UP), (down_hbm, down, S_DOWN))[w]
        return remote(src, dst.at[slot], sem, w_recv.at[w], s, twin)

    def near_copy(q, n):
        at = cols(n, chunk)
        return remote(
            dense.at[q, :, at], near.at[q, :, at],
            S_NEAR.at[q], near_recv.at[q, n], s, unit(partner),
        )

    def cross_copy(q, i, n):
        at = cols(n, chunk)
        src = dense if i == 0 else near
        return remote(
            src.at[q, :, at], cross.at[q, i, :, at],
            S_CROSS, cross_recv.at[q, i, n], s, unit(crossing[0]),
        )

    def part_copy(q, n):
        at = cols(n, chunk)
        return remote(
            snd_p.at[q, :, at], rows.at[q, 1, :, at],
            S_PART, rows_recv.at[q], s, unit(partner),
        )

    def relay_copy(q, i, n):
        at = cols(n, chunk)
        return remote(
            relay.at[q, i, :, at], rows.at[q, 2 + i, :, at],
            S_RELAY, rows_recv.at[q], s, unit(partner),
        )

    def retp_copy(r, n):
        at = cols(n, piece)
        return remote(
            res.at[r, 1, :, at], ret_p.at[r, :, at],
            S_RETP, retp_recv.at[r], s, unit(partner),
        )

    def retx_copy(r, i, n):
        at = cols(n, piece)
        return remote(
            res.at[r, 2 + i, :, at], ret_x.at[r, i, :, at],
            S_RETX, retx_recv.at[r, n], s, unit(partner),
        )

    def den_copy(r, i, n):
        at = cols(n, piece)
        return remote(
            comb.at[r, i, :, at], den.at[r, :, at],
            S_DEN, den_all_recv.at[0] if r == BWD else den_recv.at[n], s, unit(crossing[i]),
        )

    x_copy = remote(x_v, x_prev, S_X, x_recv.at[0], (s + 1) % sections, me)

    def ahead_copy(n):
        at = cols(n, piece)
        return remote(
            m_out.at[:, at], m_in.at[:, at], S_AHEAD, sf_recv.at[n],
            (s + 1) % sections, me,
        )

    parts = 4
    part = count // parts

    def back_copy(p):
        at = cols(p, part)
        return remote(
            out_b.at[at], grad_ref.at[at], S_BACK, sb_recv.at[0],
            (s + sections - 1) % sections, me,
        )

    def each_chunk(body):
        pl.loop(0, chunks)(body)

    def each_piece(body):
        pl.loop(0, pieces)(body)

    row16 = lax.broadcasted_iota(jnp.int32, (16, count), 0)
    named = jnp.where(row16 % 2 == 0, z, partner).astype(F32)
    forward = row16 < 2
    earlier = lax.broadcasted_iota(jnp.int32, (count, count), 0)
    later = lax.broadcasted_iota(jnp.int32, (count, count), 1)
    upper = jnp.where(earlier < later, 1.0, 0.0).astype(BF16)
    places = lax.broadcasted_iota(jnp.int32, (capacity, count), 0).astype(F32)

    def find(j):
        first = jnp.where(forward, meta[j, 0:1, :], meta[j, 4:5, :]) == named
        second = jnp.where(forward, meta[j, 1:2, :], meta[j, 5:6, :]) == named
        weight = jnp.where(
            first,
            jnp.where(forward, meta[j, 2:3, :], meta[j, 6:7, :]),
            jnp.where(forward, meta[j, 3:4, :], meta[j, 7:8, :]),
        )
        chosen = first | second
        before = dot(jnp.where(chosen, 1.0, 0.0).astype(BF16), upper)
        place = jnp.where(chosen, before, -1.0)
        for b in range(2):
            for k in range(2):
                row = slice(2 * b + k, 2 * b + k + 1)
                hit = places == place[row]
                picks[b, j, k] = jnp.where(hit, 1.0, 0.0).astype(BF16)
                if k == 0:
                    value = jnp.sum(jnp.where(hit, weight[row], 0.0), axis=1, keepdims=True)
                    gate[b, j] = jnp.broadcast_to(value, (capacity, 128))

    def pack_own(q, b):
        @each_chunk
        def _(n):
            at = cols(n, chunk)

            @pl.when(is_inner)
            def _():
                snd_p[q, :, at] = dot(picks[b, 0, 1], dense[q, :, at]).astype(BF16)
                part_copy(q, n).start()

            rows[q, 0, :, at] = dot(picks[b, 0, 0], dense[q, :, at]).astype(BF16)

    def normalise(src, mod, q, keep):
        @pl.loop(0, count // group)
        def _(i):
            at = pl.ds(pl.multiple_of(i * group, group), group)
            x = src[at, :]
            centered = x - jnp.mean(x, axis=1, keepdims=True)
            inv = lax.rsqrt(jnp.mean(centered * centered, axis=1, keepdims=True) + norm_eps)
            normed = centered * inv
            dense[q, at, :] = (normed * (1.0 + mod[1]) + mod[0]).astype(BF16)
            if keep:
                normed_b[at, :] = normed
                inv_b[at, :] = jnp.broadcast_to(inv, (group, 128))

    def send_near(q):
        @pl.when(is_outer)
        def _():
            each_chunk(lambda n: near_copy(q, n).start())

    def send_cross(q, first, last):
        @pl.when(is_inner)
        def _():
            pl.loop(first, last)(lambda n: cross_copy(q, 0, n).start())

    def hand_over(q, b):
        @pl.when(is_inner)
        def _():
            @each_chunk
            def _(n):
                at = cols(n, chunk)
                near_copy(q, n).wait_recv()
                cross_copy(q, 1, n).start()
                rows[q, 1, :, at] = dot(picks[b, 1, 0], near[q, :, at]).astype(BF16)

    def pass_on(q, b, i, n):
        at = cols(n, chunk)
        cross_copy(q, i, n).wait_recv()
        relay[q, i, :, at] = dot(picks[b, 2 + i, 1], cross[q, i, :, at]).astype(BF16)
        relay_copy(q, i, n).start()
        rows[q, 2 + i, :, at] = dot(picks[b, 2 + i, 0], cross[q, i, :, at]).astype(BF16)

    def gather(q, b, i):
        @pl.when(is_inner)
        def _():
            each_chunk(lambda n: pass_on(q, b, i, n))

    def gathered(q):
        @pl.when(is_outer)
        def _():
            got = rows.at[q, 1:4]
            remote(got, got, S_RELAY, rows_recv.at[q], s, unit(partner)).wait_recv()

    def flat(q):
        return rows[q].reshape(every, width)

    def give(r, n, value):
        at = cols(n, piece)
        value = value.astype(BF16).reshape(4, capacity, piece)
        for j in range(4):
            res[r, j, :, at] = value[j]

        @pl.when(is_outer)
        def _():
            for i in range(2):
                retx_copy(r, i, n).start()

    def give_late(r):
        each_piece(lambda n: retp_copy(r, n).start())

    def combine(r, b, n):
        at = cols(n, piece)
        got = ret_x.at[r, :, :, at]
        remote(got, got, S_RETX, retx_recv.at[r, n], s, unit(partner)).wait_recv()
        for i in range(2):
            total = dot(picks[b, 2 + i, 0], res[r, 2 + i, :, at], 0, 0) + dot(
                picks[b, 2 + i, 1], ret_x[r, i, :, at], 0, 0
            )
            comb[r, i, :, at] = total.astype(BF16)
            den_copy(r, i, n).start()

    def wait_returned(r):
        got = ret_p.at[r]
        remote(got, got, S_RETP, retp_recv.at[r], s, unit(partner)).wait_recv()

    def own_total(r, b, n):
        at = cols(n, piece)
        if r == FWD:
            den_copy(r, 0, n).wait_recv()
        return (
            dot(picks[b, 0, 0], res[r, 0, :, at], 0, 0)
            + dot(picks[b, 0, 1], ret_p[r, :, at], 0, 0)
            + den[r, :, at].astype(F32)
        )

    with scope("bar"):
        pl.semaphore_wait(barrier, 6)
    for copy in metas:
        copy.start()
    with scope("load0"):
        loads[0].wait()
        send_near(OG)
        send_cross(OG, 0, chunks)
        loads[4].start()
        loads[3].start()
    with scope("find0"):
        find(0)
    with scope("pk_og"):
        pack_own(OG, BWD)
    with scope("norm1"):
        loads[1].wait()
        smalls[4].wait()
        normalise(st_v, bm_ref, HB, True)
        send_near(HB)
        send_cross(HB, 0, chunks // 2)
    with scope("pk_hb"):
        pack_own(HB, BWD)
    with scope("norm2"):
        loads[2].wait()
        smalls[5].wait()

        @pl.when(s < sections - 1)
        def _():
            x_copy.start()

        normalise(x_v, fm_ref, HF, False)
        send_near(HF)
        pack_own(HF, FWD)
    for j in range(1, 4):
        with scope(f"meta{j}"):
            remote(
                meta.at[0], meta.at[j], meta_send.at[j - 1], meta_recv.at[j - 1],
                s, unit(partner),
            ).wait_recv()
            find(j)
    def share(w, p):
        @pl.when(is_inner)
        def _():
            twin_share(w, p).start()

    def near_sent(q):
        @pl.when(is_outer)
        def _():
            remote(
                dense.at[q], near.at[q], S_NEAR.at[q], near_recv.at[q, 0], s, unit(partner)
            ).wait_send()

    def share_late(w, first, last):
        @pl.when(is_outer)
        def _():
            for p in range(first, last):
                twin_share(w, p).start()

    share(1, 0)
    with scope("over_og"):
        hand_over(OG, BWD)
        send_cross(HB, chunks // 2, chunks)
    share(1, 1)
    with scope("gat_og0"):
        gather(OG, BWD, 0)
    share(1, 2)
    with scope("over_hb"):
        hand_over(HB, BWD)
        send_cross(HF, 0, chunks)
    share(1, 3)
    with scope("gat_og1"):
        gather(OG, BWD, 1)
    share(0, 0)
    with scope("near_og"):
        near_sent(OG)
    share_late(1, 0, 2)
    with scope("near_hb"):
        near_sent(HB)
    share_late(1, 2, 4)
    with scope("gathered_og"):
        gathered(OG)

    with scope("pair"):
        for j in range(4):
            @pl.loop(0, width // tile)
            def _(n):
                at = cols(n, tile)
                scaled = bm_ref[2, :, at] * rows[OG, j, :, at].astype(F32)
                rows[OG, j, :, at] = (gate[BWD, j, :, 0:1] * scaled).astype(BF16)

    share(0, 1)
    with scope("wts"):
        loads[4].wait()
        twin_whole(1, 1 - c).wait_recv()

    with scope("agrad"):
        for h in range(2):
            @pl.loop(0, hidden // tile)
            def _(n):
                at = pl.ds(pl.multiple_of(h * hidden + n * tile, tile), tile)
                agrad[:, at] = dot(flat(OG), down[h, cols(n, tile), :], 1, 1)

    share(0, 2)
    with scope("near_hf"):
        near_sent(HF)
    share_late(0, 0, 4)
    with scope("gat_hb0"):
        gather(HB, BWD, 0)
    share(0, 3)
    with scope("over_hf"):
        hand_over(HF, FWD)
    with scope("gat_hb1"):
        gather(HB, BWD, 1)
    with scope("gathered_hb"):
        gathered(HB)
        loads[3].wait()
        twin_whole(0, 1 - c).wait_recv()

    with scope("pre"):
        for h in range(2):
            @pl.loop(0, hidden // tile)
            def _(n):
                at = pl.ds(pl.multiple_of(h * hidden + n * tile, tile), tile)
                pre = dot(flat(HB), up[h, :, cols(n, tile)])
                t = jnp.tanh(ROOT * (pre + CUBE * pre * pre * pre))
                slope = ROOT * (1.0 + 3.0 * CUBE * pre * pre)
                dgelu = 0.5 * (1.0 + t) + 0.5 * pre * (1.0 - t * t) * slope
                act[:, at] = (agrad[:, at] * dgelu).astype(BF16)

    with scope("partb"):
        @each_piece
        def _(n):
            at = cols(n, piece)
            give(
                BWD, n,
                dot(act[:, :hidden], up[0, at, :], 1, 1)
                + dot(act[:, hidden:], up[1, at, :], 1, 1),
            )

        @pl.when(is_outer)
        def _():
            give_late(BWD)

    with scope("gat_hf0"):
        gather(HF, FWD, 0)
    with scope("comb_b"):
        @pl.when(is_inner)
        def _():
            per = pieces // chunks

            @each_chunk
            def _(n):
                for k in range(per):
                    combine(BWD, BWD, n * per + k)
                with scope("gat_hf1"):
                    pass_on(HF, FWD, 1, n)

        @pl.when(is_inner)
        def _():
            give_late(BWD)

    with scope("gathered_hf"):
        gathered(HF)

    with scope("up"):
        for h in range(2):
            @pl.loop(0, hidden // tile)
            def _(n):
                at = pl.ds(pl.multiple_of(h * hidden + n * tile, tile), tile)
                pre = dot(flat(HF), up[h, :, cols(n, tile)])
                t = jnp.tanh(ROOT * (pre + CUBE * pre * pre * pre))
                act[:, at] = (0.5 * pre * (1.0 + t)).astype(BF16)

    weight = gate[FWD, :, :, 0:1].reshape(every, 1)

    with scope("down"):
        @each_piece
        def _(n):
            at = cols(n, piece)
            value = dot(act[:, :hidden], down[0, :, at]) + dot(act[:, hidden:], down[1, :, at])
            give(FWD, n, weight * value)

        give_late(FWD)

    with scope("comb_f"):
        @pl.when(is_inner)
        def _():
            each_piece(lambda n: combine(FWD, FWD, n))

    @pl.when(s == 0)
    def _():
        next_ref[...] = jnp.zeros_like(next_ref)

    @pl.when(s == sections - 1)
    def _():
        grad_ref[...] = jnp.zeros_like(grad_ref)

    with scope("own_b"):
        wait_returned(BWD)
        got = den.at[BWD]
        remote(got, got, S_DEN, den_all_recv.at[0], s, unit(partner)).wait_recv()

        @each_piece
        def _(n):
            dh[:, cols(n, piece)] = own_total(BWD, BWD, n)

    with scope("fin_b"):
        for p in range(parts):
            @pl.loop(0, part // group)
            def _(i):
                at = pl.ds(pl.multiple_of(p * part + i * group, group), group)
                dnorm = dh[at, :] * (1.0 + bm_ref[1])
                normed = normed_b[at, :]
                one = jnp.mean(dnorm, axis=1, keepdims=True)
                two = jnp.mean(dnorm * normed, axis=1, keepdims=True)
                out_b[at, :] = (
                    dense[OG, at, :].astype(F32) + (dnorm - one - normed * two) * inv_b[at, 0:1]
                ).astype(BF16)

            @pl.when(s > 0)
            def _():
                back_copy(p).start()

    def arrive(n):
        at = cols(n, piece)

        @pl.when(s > 0)
        def _():
            ahead_copy(n).wait_recv()
            next_ref[:, at] = x_prev[:, at] + m_in[:, at].astype(F32)

    with scope("own_f"):
        @pl.when(s > 0)
        def _():
            x_copy.wait_recv()

        wait_returned(FWD)
        lag = 2

        @each_piece
        def _(n):
            at = cols(n, piece)
            m_out[:, at] = (fm_ref[2, :, at] * own_total(FWD, FWD, n)).astype(BF16)

            @pl.when(s < sections - 1)
            def _():
                ahead_copy(n).start()

            @pl.when(n >= lag)
            def _():
                arrive(n - lag)

        for n in range(pieces - lag, pieces):
            arrive(n)

    with scope("tail_send"):
        def sent(sem, src):
            remote(src, src, sem, rows_recv.at[0], s, unit(partner)).wait_send()

        for copy in metas:
            copy.wait_send()
        for w in range(2):
            twin_whole(w, c).wait_send()
        sent(S_RETP, res.at[:, 1])

        @pl.when(is_outer)
        def _():
            sent(S_RETX, res.at[:, 2:4])

        @pl.when(is_inner)
        def _():
            sent(S_PART, snd_p)
            sent(S_CROSS, cross)
            sent(S_RELAY, relay)
            sent(S_DEN, comb)

    with scope("tail_hop"):
        @pl.when(s < sections - 1)
        def _():
            x_copy.wait_send()
            sent(S_AHEAD, m_out)
            remote(grad_ref, grad_ref, S_BACK, sb_recv.at[0], s, twin).wait_recv()

        @pl.when(s > 0)
        def _():
            sent(S_BACK, out_b)


def write_out(next_ref, grad_ref, next_hbm, grad_hbm, sem):
    copies = [
        pltpu.make_async_copy(next_ref, next_hbm, sem.at[0]),
        pltpu.make_async_copy(grad_ref, grad_hbm, sem.at[1]),
    ]
    for copy in copies:
        copy.start()
    for copy in copies:
        copy.wait()


def run_two_sided(
    section_inputs,
    stored_inputs,
    out_grads,
    fwd_routes,
    fwd_gates,
    fwd_modulation,
    bwd_routes,
    bwd_gates,
    bwd_modulation,
    up_weight,
    down_weight,
):
    sections, units = lax.axis_size("section"), lax.axis_size("expert")
    experts = units // 2
    count, width = section_inputs.shape[1:]
    hidden = up_weight.shape[3]
    capacity = -(-min(count, 5 * count // (2 * experts)) // 16) * 16
    every = 4 * capacity
    chunks, pieces = 4, 8

    def vmem(dtype, *shape):
        return pltpu.VMEM(shape, dtype)

    def dma(*shape):
        return pltpu.SemaphoreType.DMA(shape)

    scratch = [
        vmem(jnp.int32, 2, count),
        vmem(F32, 2, count),
        vmem(F32, 3, 1, width),
        vmem(jnp.int32, 2, count),
        vmem(F32, 2, count),
        vmem(F32, 3, 1, width),
        vmem(BF16, 2, width, hidden),
        vmem(BF16, 2, hidden, width),
        *[vmem(F32, count, width)] * 3,
        *[vmem(BF16, 3, count, width)] * 2,
        vmem(BF16, 3, 2, count, width),
        vmem(BF16, 3, capacity, width),
        vmem(BF16, 3, 2, capacity, width),
        vmem(BF16, 3, 4, capacity, width),
        vmem(BF16, every, 2 * hidden),
        vmem(F32, every, 2 * hidden),
        vmem(BF16, 2, 4, capacity, width),
        vmem(BF16, 2, capacity, width),
        vmem(BF16, 2, 2, capacity, width),
        vmem(BF16, 2, 2, count, width),
        vmem(BF16, 2, count, width),
        vmem(F32, count, width),
        vmem(F32, count, 128),
        *[vmem(BF16, count, width)] * 2,
        vmem(F32, count, width),
        vmem(BF16, count, width),
        vmem(F32, 4, 8, count),
        vmem(BF16, 2, 4, 2, capacity, count),
        vmem(F32, 2, 4, capacity, 128),
        dma(5),
        dma(6),
        dma(11),
        dma(3),
        dma(2),
        *[dma(3)] * 2,
        dma(1),
        dma(3, chunks),
        dma(3, 2, chunks),
        dma(3),
        dma(2),
        dma(2, pieces),
        dma(pieces),
        dma(1),
        dma(pieces),
        dma(1),
    ]
    in_vmem = pl.BlockSpec(memory_space=pltpu.VMEM)
    in_hbm = pl.BlockSpec(memory_space=pltpu.HBM)
    flops = 20 * every * width * hidden
    next_inputs, input_grads = pl.pallas_call(
        functools.partial(two_sided, sections, units, capacity, chunks, pieces),
        out_shape=(
            jax.ShapeDtypeStruct((count, width), F32),
            jax.ShapeDtypeStruct((count, width), BF16),
        ),
        in_specs=[in_hbm] * 11,
        out_specs=(in_vmem, in_vmem),
        scratch_shapes=scratch,
        compiler_params=pltpu.CompilerParams(
            collective_id=1, has_side_effects=True, vmem_limit_bytes=50 << 20
        ),
        cost_estimate=pl.CostEstimate(
            flops=flops, bytes_accessed=4 * width * hidden, transcendentals=0
        ),
    )(*[pltpu.with_memory_space_constraint(array, pltpu.HBM) for array in (
        section_inputs[0], stored_inputs[0], out_grads[0],
        fwd_routes[0].T, fwd_gates[0].T, jnp.transpose(fwd_modulation, (1, 0, 2)),
        bwd_routes[0].T, bwd_gates[0].T, jnp.transpose(bwd_modulation, (1, 0, 2)),
        up_weight[0, 0], down_weight[0, 0],
    )])
    next_inputs, input_grads = pl.pallas_call(
        write_out,
        out_shape=(
            jax.ShapeDtypeStruct((count, width), F32),
            jax.ShapeDtypeStruct((count, width), BF16),
        ),
        in_specs=[in_vmem] * 2,
        out_specs=(in_hbm, in_hbm),
        scratch_shapes=[dma(2)],
        compiler_params=pltpu.CompilerParams(vmem_limit_bytes=1 << 20),
    )(next_inputs, input_grads)
    return next_inputs[None], input_grads[None]


def on_device(*arrays):
    sides, inner_and_outer = 2, 2
    line = lax.axis_size("expert") == 2 * sides * inner_and_outer
    return (run_two_sided if line else run_many)(*arrays)


def solution(mesh):
    tokens = P("section", "expert", None)
    shared = P("section", None, None)
    weights = P("section", "expert", None, None)
    placed = (tokens,) * 5 + (shared,) + (tokens,) * 2 + (shared,) + (weights,) * 2
    return jax.shard_map(
        on_device,
        mesh=mesh,
        in_specs=placed,
        out_specs=(tokens, tokens),
        check_vma=False,
    )
```

```python
import functools

import jax
import jax.numpy as jnp
from jax import lax
from jax.experimental import pallas as pl
from jax.experimental.pallas import tpu as pltpu
from jax.sharding import PartitionSpec as P

norm_eps = 1e-06
F32, BF16 = jnp.float32, jnp.bfloat16
MESH = pl.DeviceIdType.MESH
ROOT, CUBE = 0.7978845608028654, 0.044715


def flip(index, mask, bits):
    total = 0
    for b in range(bits):
        bit = (index // (1 << b)) % 2
        total = total + (1 << b) * (1 - bit if mask >> b & 1 else bit)
    return total


def dot(a, b, ca=1, cb=0):
    return lax.dot_general(a, b, (((ca,), (cb,)), ((), ())), preferred_element_type=F32)


def slot_masks(routes, capacity, slots):
    count = routes.shape[0]
    lanes = lax.broadcasted_iota(jnp.int32, (count, 128), 1)
    hits = [routes[:, k : k + 1] == lanes for k in range(2)]
    choose = jnp.where(hits[0] | hits[1], 1.0, 0.0).astype(BF16)
    row = lax.broadcasted_iota(jnp.int32, (count, count), 0)
    col = lax.broadcasted_iota(jnp.int32, (count, count), 1)
    before = dot(jnp.where(col < row, 1.0, 0.0).astype(BF16), choose)
    places = lax.broadcasted_iota(jnp.int32, (count, slots), 1)
    masks = []
    for k in range(2):
        rank = jnp.sum(jnp.where(hits[k], before, 0.0), axis=1, keepdims=True)
        masks.append(places == routes[:, k : k + 1] * capacity + rank.astype(jnp.int32))
    return masks


def many_chips(
    sections, units, capacity,
    x_ref, st_ref, og_ref, fr_ref, fg_ref, fm_ref, br_ref, bg_ref, bm_ref, up_hbm, down_hbm,
    next_ref, grad_ref,
    up, down, snd_f, snd_r, snd_g, rcv_f, rcv_r, rcv_g, act, dgelu,
    px_f, px_b, pin_f, pin_b, ret_f, ret_b, rr_f, rr_b,
    hid, pair0, pair1, normed_b, inv_b, out_f, dh, out_b,
    w_sem, in_send, in_recv, fw_send, fw_recv, px_send, px_recv, rt_send, rt_recv,
    sf_send, sf_recv, sb_send, sb_recv,
):
    s, me = lax.axis_index("section"), lax.axis_index("expert")
    experts = units // 2
    bits = units.bit_length() - 1
    chip, core = me // 2, me % 2
    count, width = x_ref.shape
    half = width // 2
    hidden_units = up.shape[1]
    rows = units * capacity
    slots = experts * capacity
    tile = 256
    group = 16
    order = list(range(1, units))
    peer = {k: flip(me, k, bits) for k in order}

    w_up = pltpu.make_async_copy(up_hbm, up, w_sem.at[0])
    w_down = pltpu.make_async_copy(down_hbm, down, w_sem.at[1])
    w_up.start()
    w_down.start()

    barrier = pltpu.get_barrier_semaphore()
    for k in order:
        pl.semaphore_signal(barrier, inc=1, device_id=(s, peer[k]), device_id_type=MESH)
    for step in (1, sections - 1):
        pl.semaphore_signal(
            barrier, inc=1, device_id=((s + step) % sections, me), device_id_type=MESH
        )

    def remote(src, dst, send, recv, section, unit):
        return pltpu.make_async_remote_copy(
            src_ref=src, dst_ref=dst, send_sem=send, recv_sem=recv,
            device_id=(section, unit), device_id_type=MESH,
        )

    def inbound(phase, snd, rcv):
        copies = {}
        for k in order:
            d = peer[k]
            if k == 1:
                src, dst = snd.at[chip], rcv.at[:, me]
            else:
                src, dst = snd.at[d // 2, d % 2], rcv.at[d % 2, me]
            copies[k] = remote(src, dst, in_send.at[phase, k], in_recv.at[phase, k], s, d)
        return copies

    def hand_on(phase, rcv):
        copies = {}
        for k in order:
            if k > 1:
                block = rcv.at[core, peer[k]]
                copies[k] = remote(
                    block, block, fw_send.at[phase, k], fw_recv.at[phase, k], s, peer[1]
                )
        return copies

    def keep_own(snd, rcv):
        for h in range(2):
            rcv[h, me] = snd[chip, h]

    def receive(ins, fws):
        for k in order:
            ins[k].wait_recv()
            if k > 1:
                fws[k].start()
        for k in order:
            if k > 1:
                fws[k].wait_recv()

    def normalise(src, mod, keep):
        @pl.loop(0, count // group)
        def _(i):
            at = pl.ds(pl.multiple_of(i * group, group), group)
            x = src[at, :]
            centered = x - jnp.mean(x, axis=1, keepdims=True)
            inv = lax.rsqrt(jnp.mean(centered * centered, axis=1, keepdims=True) + norm_eps)
            normed = centered * inv
            hid[at, :] = (normed * (1.0 + mod[1:2, :]) + mod[0:1, :]).astype(BF16)
            if keep:
                normed_b[at, :] = normed
                inv_b[at, :] = jnp.broadcast_to(inv, (group, 128))

    def pack(terms, snd):
        for h in range(2):
            @pl.loop(0, half // tile)
            def _(n):
                src = pl.ds(pl.multiple_of(h * half + n * tile, tile), tile)
                value = sum(dot(mask, ref[:, src], 0, 0) for mask, ref in terms).astype(BF16)
                for e in range(experts):
                    snd[e, h, :, pl.ds(pl.multiple_of(n * tile, tile), tile)] = value[
                        e * capacity : (e + 1) * capacity, :
                    ]

    def onehot(mask):
        return jnp.where(mask, 1.0, 0.0).astype(BF16)

    normalise(x_ref, fm_ref, False)
    fwd = slot_masks(fr_ref[...], capacity, slots)
    pack([(onehot(fwd[0] | fwd[1]), hid)], snd_f)
    pl.semaphore_wait(barrier, units + 1)
    in_f, fw_f = inbound(0, snd_f, rcv_f), hand_on(0, rcv_f)
    for k in order:
        in_f[k].start()
    keep_own(snd_f, rcv_f)

    normalise(st_ref, bm_ref, True)
    bwd = slot_masks(br_ref[...], capacity, slots)
    bwd_hot = [onehot(mask) for mask in bwd]
    pack([(bwd_hot[0] + bwd_hot[1], hid)], snd_r)
    in_r, fw_r = inbound(1, snd_r, rcv_r), hand_on(1, rcv_r)
    for k in order:
        in_r[k].start()
    keep_own(snd_r, rcv_r)

    @pl.loop(0, count // group)
    def _(i):
        at = pl.ds(pl.multiple_of(i * group, group), group)
        scaled = bm_ref[2:3, :] * og_ref[at, :].astype(F32)
        pair0[at, :] = (bg_ref[at, 0:1] * scaled).astype(BF16)
        pair1[at, :] = (bg_ref[at, 1:2] * scaled).astype(BF16)

    pack([(bwd_hot[0], pair0), (bwd_hot[1], pair1)], snd_g)
    in_g, fw_g = inbound(2, snd_g, rcv_g), hand_on(2, rcv_g)
    for k in order:
        in_g[k].start()
    keep_own(snd_g, rcv_g)

    def flat(ref, h):
        return ref[h].reshape(rows, half)

    def cols(n, base=0):
        return pl.ds(pl.multiple_of(base + n * tile, tile), tile)

    def exchange(phase, px, pin, ret, result):
        def fill(dst, h):
            @pl.loop(0, half // tile)
            def _(n):
                value = result(h, n).astype(BF16).reshape(units, capacity, tile)
                dst[:, :, cols(n)] = value

        fill(px, 1 - core)
        swap = remote(px, pin, px_send.at[phase], px_recv.at[phase], s, peer[1])
        swap.start()
        fill(ret, core)
        swap.wait_recv()

        @pl.loop(0, units)
        def _(u):
            ret[u] = (ret[u].astype(F32) + pin[u].astype(F32)).astype(BF16)

        return swap

    def give_back(phase, ret, rr):
        copies = {}
        for k in order:
            copies[k] = remote(
                ret.at[peer[k]], rr.at[core, chip],
                rt_send.at[phase, k], rt_recv.at[phase, k], s, peer[k],
            )
            copies[k].start()
        rr[core, chip] = ret[me]
        return copies

    receive(in_f, fw_f)
    w_up.wait()
    w_down.wait()

    @pl.loop(0, hidden_units // tile)
    def _(n):
        pre = dot(flat(rcv_f, 0), up[:half, cols(n)]) + dot(flat(rcv_f, 1), up[half:, cols(n)])
        t = jnp.tanh(ROOT * (pre + CUBE * pre * pre * pre))
        act[:, cols(n)] = (0.5 * pre * (1.0 + t)).astype(BF16)

    swap_f = exchange(
        0, px_f, pin_f, ret_f, lambda h, n: dot(act[...], down[:, cols(n, h * half)])
    )
    back_f = give_back(0, ret_f, rr_f)

    receive(in_r, fw_r)

    @pl.loop(0, hidden_units // tile)
    def _(n):
        pre = dot(flat(rcv_r, 0), up[:half, cols(n)]) + dot(flat(rcv_r, 1), up[half:, cols(n)])
        t = jnp.tanh(ROOT * (pre + CUBE * pre * pre * pre))
        slope = ROOT * (1.0 + 3.0 * CUBE * pre * pre)
        dgelu[:, cols(n)] = 0.5 * (1.0 + t) + 0.5 * pre * (1.0 - t * t) * slope

    receive(in_g, fw_g)

    @pl.loop(0, hidden_units // tile)
    def _(n):
        back = dot(flat(rcv_g, 0), down[cols(n), :half], 1, 1) + dot(
            flat(rcv_g, 1), down[cols(n), half:], 1, 1
        )
        act[:, cols(n)] = (back * dgelu[:, cols(n)]).astype(BF16)

    swap_b = exchange(
        1, px_b, pin_b, ret_b, lambda h, n: dot(act[...], up[cols(n, h * half), :], 1, 1)
    )
    back_b = give_back(1, ret_b, rr_b)

    weight = sum(jnp.where(fwd[k], fg_ref[:, k : k + 1], 0.0) for k in range(2))
    high = weight.astype(BF16)
    low = (weight - high.astype(F32)).astype(BF16)
    for k in order:
        back_f[k].wait_recv()
    sends_f = []
    for h in range(2):
        side = pl.ds(h * half, half)

        @pl.loop(0, half // tile)
        def _(n):
            got = rr_f[h, :, :, cols(n)].reshape(slots, tile)
            moe = dot(high, got) + dot(low, got)
            at = cols(n, h * half)
            out_f[:, at] = x_ref[:, at] + fm_ref[2:3, at] * moe

        copy = remote(
            out_f.at[:, side], next_ref.at[:, side], sf_send.at[h], sf_recv.at[h],
            (s + 1) % sections, me,
        )
        sends_f.append(copy)

        @pl.when(s < sections - 1)
        def _():
            copy.start()

    @pl.when(s == 0)
    def _():
        next_ref[...] = jnp.zeros_like(next_ref)

    @pl.when(s == sections - 1)
    def _():
        grad_ref[...] = jnp.zeros_like(grad_ref)

    for k in order:
        back_b[k].wait_recv()
    both = bwd_hot[0] + bwd_hot[1]
    for h in range(2):
        @pl.loop(0, half // tile)
        def _(n):
            got = rr_b[h, :, :, cols(n)].reshape(slots, tile)
            dh[:, cols(n, h * half)] = dot(both, got)

    pieces = 4
    part = count // pieces
    sends_b = []
    for p in range(pieces):
        @pl.loop(0, part // group)
        def _(i):
            at = pl.ds(pl.multiple_of(p * part + i * group, group), group)
            dnorm = dh[at, :] * (1.0 + bm_ref[1:2, :])
            normed = normed_b[at, :]
            one = jnp.mean(dnorm, axis=1, keepdims=True)
            two = jnp.mean(dnorm * normed, axis=1, keepdims=True)
            out_b[at, :] = (
                og_ref[at, :].astype(F32) + (dnorm - one - normed * two) * inv_b[at, 0:1]
            ).astype(BF16)

        piece = pl.ds(p * part, part)
        copy = remote(
            out_b.at[piece], grad_ref.at[piece], sb_send.at[p], sb_recv.at[p],
            (s + sections - 1) % sections, me,
        )
        sends_b.append(copy)

        @pl.when(s > 0)
        def _():
            copy.start()

    for copies in (in_f, in_r, in_g, fw_f, fw_r, fw_g, back_f, back_b):
        for copy in copies.values():
            copy.wait_send()
    swap_f.wait_send()
    swap_b.wait_send()

    @pl.when(s < sections - 1)
    def _():
        for copy in sends_f:
            copy.wait_send()
        for copy in sends_b:
            copy.wait_recv()

    @pl.when(s > 0)
    def _():
        for copy in sends_f:
            copy.wait_recv()
        for copy in sends_b:
            copy.wait_send()


def run_many(
    section_inputs,
    stored_inputs,
    out_grads,
    fwd_routes,
    fwd_gates,
    fwd_modulation,
    bwd_routes,
    bwd_gates,
    bwd_modulation,
    up_weight,
    down_weight,
):
    sections, units = lax.axis_size("section"), lax.axis_size("expert")
    experts = units // 2
    count, width = section_inputs.shape[1:]
    hidden_units = up_weight.shape[3]
    half = width // 2
    capacity = -(-min(count, 5 * count // (2 * experts)) // 16) * 16
    rows = units * capacity

    def vmem(dtype, *shape):
        return pltpu.VMEM(shape, dtype)

    def dma(*shape):
        return pltpu.SemaphoreType.DMA(shape)

    scratch = [
        vmem(BF16, width, hidden_units),
        vmem(BF16, hidden_units, width),
        *[vmem(BF16, experts, 2, capacity, half)] * 3,
        *[vmem(BF16, 2, units, capacity, half)] * 3,
        vmem(BF16, rows, hidden_units),
        vmem(F32, rows, hidden_units),
        *[vmem(BF16, units, capacity, half)] * 6,
        *[vmem(BF16, 2, experts, capacity, half)] * 2,
        *[vmem(BF16, count, width)] * 3,
        vmem(F32, count, width),
        vmem(F32, count, 128),
        *[vmem(F32, count, width)] * 2,
        vmem(BF16, count, width),
        dma(2),
        *[dma(3, units)] * 4,
        *[dma(2)] * 2,
        *[dma(2, units)] * 2,
        *[dma(2)] * 2,
        *[dma(4)] * 2,
    ]
    in_vmem = pl.BlockSpec(memory_space=pltpu.VMEM)
    in_hbm = pl.BlockSpec(memory_space=pl.ANY)
    flops = 10 * rows * width * hidden_units
    next_inputs, input_grads = pl.pallas_call(
        functools.partial(many_chips, sections, units, capacity),
        out_shape=(
            jax.ShapeDtypeStruct((count, width), F32),
            jax.ShapeDtypeStruct((count, width), BF16),
        ),
        in_specs=[in_vmem] * 9 + [in_hbm] * 2,
        out_specs=(in_vmem, in_vmem),
        scratch_shapes=scratch,
        compiler_params=pltpu.CompilerParams(
            collective_id=0, has_side_effects=True, vmem_limit_bytes=67043328
        ),
        cost_estimate=pl.CostEstimate(
            flops=flops, bytes_accessed=4 * width * hidden_units, transcendentals=0
        ),
    )(
        section_inputs[0], stored_inputs[0], out_grads[0], fwd_routes[0], fwd_gates[0],
        fwd_modulation[0], bwd_routes[0], bwd_gates[0], bwd_modulation[0],
        up_weight[0, 0], down_weight[0, 0],
    )
    return next_inputs[None], input_grads[None]


def two_sided(
    sections, units, capacity, chunks, pieces,
    x_hbm, st_hbm, og_hbm, fr_hbm, fg_hbm, fm_hbm, br_hbm, bg_hbm, bm_hbm, up_hbm, down_hbm,
    next_ref, grad_ref,
    fr_ref, fg_ref, fm_ref, br_ref, bg_ref, bm_ref,
    up, down, x_v, x_prev, st_v, dense, near, cross, snd_p, relay, rows, act, agrad,
    res, ret_p, ret_x, comb, den, normed_b, inv_b, m_out, m_in, dh, out_b,
    meta, picks, gate,
    load_sem, small_sem, send_sem, near_send, w_recv, meta_send, meta_recv, x_recv, near_recv,
    cross_recv, rows_recv, retp_recv, retx_recv, den_recv, den_all_recv, sf_recv, sb_recv,
):
    s, me = lax.axis_index("section"), lax.axis_index("expert")
    z, c = me // 2, me % 2
    odd, side = z % 2, z // 2
    inner = odd + side - 2 * odd * side
    seat = 1 - inner
    partner = z + 1 - 2 * odd
    crossing = [2 - side, 3 - 3 * side]
    is_inner, is_outer = inner == 1, inner == 0
    count, width = x_v.shape
    hidden = up.shape[2]
    every = 4 * capacity
    tile, group = 256, 16
    chunk, piece = width // chunks, width // pieces
    OG, HB, HF = 0, 1, 2
    FWD, BWD = 0, 1
    scope = jax.named_scope

    def unit(chip):
        return 2 * chip + c

    def remote(src, dst, send, recv, section, to):
        return pltpu.make_async_remote_copy(
            src_ref=src, dst_ref=dst, send_sem=send, recv_sem=recv,
            device_id=(section, to), device_id_type=MESH,
        )

    def cols(n, size):
        return pl.ds(pl.multiple_of(n * size, size), size)

    loads = [
        pltpu.make_async_copy(og_hbm, dense.at[OG], load_sem.at[0]),
        pltpu.make_async_copy(st_hbm, st_v, load_sem.at[1]),
        pltpu.make_async_copy(x_hbm, x_v, load_sem.at[2]),
        pltpu.make_async_copy(up_hbm, up.at[c], load_sem.at[3]),
        pltpu.make_async_copy(down_hbm, down.at[c], load_sem.at[4]),
    ]
    smalls = [
        pltpu.make_async_copy(src, dst, small_sem.at[k])
        for k, (src, dst) in enumerate([
            (fr_hbm, fr_ref), (fg_hbm, fg_ref), (br_hbm, br_ref), (bg_hbm, bg_ref),
            (bm_hbm, bm_ref), (fm_hbm, fm_ref),
        ])
    ]
    for load in smalls[:4] + loads[:3] + smalls[4:]:
        load.start()

    barrier = pltpu.get_barrier_semaphore()
    for chip in (partner, crossing[0], crossing[1]):
        pl.semaphore_signal(barrier, inc=1, device_id=(s, unit(chip)), device_id_type=MESH)
    twin = me + 1 - 2 * c
    pl.semaphore_signal(barrier, inc=1, device_id=(s, twin), device_id_type=MESH)
    for step in (1, sections - 1):
        pl.semaphore_signal(
            barrier, inc=1, device_id=((s + step) % sections, me), device_id_type=MESH
        )

    for load in smalls[:4]:
        load.wait()
    meta[0, 0:2, :] = fr_ref[...].astype(F32)
    meta[0, 2:4, :] = fg_ref[...]
    meta[0, 4:6, :] = br_ref[...].astype(F32)
    meta[0, 6:8, :] = bg_ref[...]

    metas = [
        remote(meta.at[0], meta.at[1], meta_send.at[0], meta_recv.at[0], s, unit(partner)),
        remote(
            meta.at[0], meta.at[2 + seat], meta_send.at[1], meta_recv.at[1 + seat],
            s, unit(crossing[0]),
        ),
        remote(
            meta.at[0], meta.at[2 + seat], meta_send.at[2], meta_recv.at[1 + seat],
            s, unit(crossing[1]),
        ),
    ]
    shares = 4
    S_UP, S_DOWN, S_CROSS, S_PART, S_RELAY, S_RETP, S_RETX, S_DEN, S_AHEAD, S_BACK, S_X = [
        send_sem.at[k] for k in range(11)
    ]
    S_NEAR = near_send

    def twin_share(w, p):
        src, dst, sem = ((up_hbm, up, S_UP), (down_hbm, down, S_DOWN))[w]
        size = src.shape[0] // shares
        at = pl.ds(p * size, size)
        return remote(src.at[at], dst.at[c, at], sem, w_recv.at[w], s, twin)

    def twin_whole(w, slot):
        src, dst, sem = ((up_hbm, up, S_UP), (down_hbm, down, S_DOWN))[w]
        return remote(src, dst.at[slot], sem, w_recv.at[w], s, twin)

    def near_copy(q, n):
        at = cols(n, chunk)
        return remote(
            dense.at[q, :, at], near.at[q, :, at],
            S_NEAR.at[q], near_recv.at[q, n], s, unit(partner),
        )

    def cross_copy(q, i, n):
        at = cols(n, chunk)
        src = dense if i == 0 else near
        return remote(
            src.at[q, :, at], cross.at[q, i, :, at],
            S_CROSS, cross_recv.at[q, i, n], s, unit(crossing[0]),
        )

    def part_copy(q, n):
        at = cols(n, chunk)
        return remote(
            snd_p.at[q, :, at], rows.at[q, 1, :, at],
            S_PART, rows_recv.at[q], s, unit(partner),
        )

    def relay_copy(q, i, n):
        at = cols(n, chunk)
        return remote(
            relay.at[q, i, :, at], rows.at[q, 2 + i, :, at],
            S_RELAY, rows_recv.at[q], s, unit(partner),
        )

    def retp_copy(r, n):
        at = cols(n, piece)
        return remote(
            res.at[r, 1, :, at], ret_p.at[r, :, at],
            S_RETP, retp_recv.at[r], s, unit(partner),
        )

    def retx_copy(r, i, n):
        at = cols(n, piece)
        return remote(
            res.at[r, 2 + i, :, at], ret_x.at[r, i, :, at],
            S_RETX, retx_recv.at[r, n], s, unit(partner),
        )

    def den_copy(r, i, n):
        at = cols(n, piece)
        return remote(
            comb.at[r, i, :, at], den.at[r, :, at],
            S_DEN, den_all_recv.at[0] if r == BWD else den_recv.at[n], s, unit(crossing[i]),
        )

    x_copy = remote(x_v, x_prev, S_X, x_recv.at[0], (s + 1) % sections, me)

    def ahead_copy(n):
        at = cols(n, piece)
        return remote(
            m_out.at[:, at], m_in.at[:, at], S_AHEAD, sf_recv.at[n],
            (s + 1) % sections, me,
        )

    parts = 4
    part = count // parts

    def back_copy(p):
        at = cols(p, part)
        return remote(
            out_b.at[at], grad_ref.at[at], S_BACK, sb_recv.at[0],
            (s + sections - 1) % sections, me,
        )

    def each_chunk(body):
        pl.loop(0, chunks)(body)

    def each_piece(body):
        pl.loop(0, pieces)(body)

    row16 = lax.broadcasted_iota(jnp.int32, (16, count), 0)
    named = jnp.where(row16 % 2 == 0, z, partner).astype(F32)
    forward = row16 < 2
    earlier = lax.broadcasted_iota(jnp.int32, (count, count), 0)
    later = lax.broadcasted_iota(jnp.int32, (count, count), 1)
    upper = jnp.where(earlier < later, 1.0, 0.0).astype(BF16)
    places = lax.broadcasted_iota(jnp.int32, (capacity, count), 0).astype(F32)

    def find(j):
        first = jnp.where(forward, meta[j, 0:1, :], meta[j, 4:5, :]) == named
        second = jnp.where(forward, meta[j, 1:2, :], meta[j, 5:6, :]) == named
        weight = jnp.where(
            first,
            jnp.where(forward, meta[j, 2:3, :], meta[j, 6:7, :]),
            jnp.where(forward, meta[j, 3:4, :], meta[j, 7:8, :]),
        )
        chosen = first | second
        before = dot(jnp.where(chosen, 1.0, 0.0).astype(BF16), upper)
        place = jnp.where(chosen, before, -1.0)
        for b in range(2):
            for k in range(2):
                row = slice(2 * b + k, 2 * b + k + 1)
                hit = places == place[row]
                picks[b, j, k] = jnp.where(hit, 1.0, 0.0).astype(BF16)
                if k == 0:
                    value = jnp.sum(jnp.where(hit, weight[row], 0.0), axis=1, keepdims=True)
                    gate[b, j] = jnp.broadcast_to(value, (capacity, 128))

    def pack_own(q, b):
        @each_chunk
        def _(n):
            at = cols(n, chunk)

            @pl.when(is_inner)
            def _():
                snd_p[q, :, at] = dot(picks[b, 0, 1], dense[q, :, at]).astype(BF16)
                part_copy(q, n).start()

            rows[q, 0, :, at] = dot(picks[b, 0, 0], dense[q, :, at]).astype(BF16)

    def normalise(src, mod, q, keep):
        @pl.loop(0, count // group)
        def _(i):
            at = pl.ds(pl.multiple_of(i * group, group), group)
            x = src[at, :]
            centered = x - jnp.mean(x, axis=1, keepdims=True)
            inv = lax.rsqrt(jnp.mean(centered * centered, axis=1, keepdims=True) + norm_eps)
            normed = centered * inv
            dense[q, at, :] = (normed * (1.0 + mod[1]) + mod[0]).astype(BF16)
            if keep:
                normed_b[at, :] = normed
                inv_b[at, :] = jnp.broadcast_to(inv, (group, 128))

    def send_near(q):
        @pl.when(is_outer)
        def _():
            each_chunk(lambda n: near_copy(q, n).start())

    def send_cross(q, first, last):
        @pl.when(is_inner)
        def _():
            pl.loop(first, last)(lambda n: cross_copy(q, 0, n).start())

    def hand_over(q, b):
        @pl.when(is_inner)
        def _():
            @each_chunk
            def _(n):
                at = cols(n, chunk)
                near_copy(q, n).wait_recv()
                cross_copy(q, 1, n).start()
                rows[q, 1, :, at] = dot(picks[b, 1, 0], near[q, :, at]).astype(BF16)

    def pass_on(q, b, i, n):
        at = cols(n, chunk)
        cross_copy(q, i, n).wait_recv()
        relay[q, i, :, at] = dot(picks[b, 2 + i, 1], cross[q, i, :, at]).astype(BF16)
        relay_copy(q, i, n).start()
        rows[q, 2 + i, :, at] = dot(picks[b, 2 + i, 0], cross[q, i, :, at]).astype(BF16)

    def gather(q, b, i):
        @pl.when(is_inner)
        def _():
            each_chunk(lambda n: pass_on(q, b, i, n))

    def gathered(q):
        @pl.when(is_outer)
        def _():
            got = rows.at[q, 1:4]
            remote(got, got, S_RELAY, rows_recv.at[q], s, unit(partner)).wait_recv()

    def flat(q):
        return rows[q].reshape(every, width)

    def give(r, n, value):
        at = cols(n, piece)
        value = value.astype(BF16).reshape(4, capacity, piece)
        for j in range(4):
            res[r, j, :, at] = value[j]

        @pl.when(is_outer)
        def _():
            for i in range(2):
                retx_copy(r, i, n).start()

    def give_late(r):
        each_piece(lambda n: retp_copy(r, n).start())

    def combine(r, b, n):
        at = cols(n, piece)
        got = ret_x.at[r, :, :, at]
        remote(got, got, S_RETX, retx_recv.at[r, n], s, unit(partner)).wait_recv()
        for i in range(2):
            total = dot(picks[b, 2 + i, 0], res[r, 2 + i, :, at], 0, 0) + dot(
                picks[b, 2 + i, 1], ret_x[r, i, :, at], 0, 0
            )
            comb[r, i, :, at] = total.astype(BF16)
            den_copy(r, i, n).start()

    def wait_returned(r):
        got = ret_p.at[r]
        remote(got, got, S_RETP, retp_recv.at[r], s, unit(partner)).wait_recv()

    def own_total(r, b, n):
        at = cols(n, piece)
        if r == FWD:
            den_copy(r, 0, n).wait_recv()
        return (
            dot(picks[b, 0, 0], res[r, 0, :, at], 0, 0)
            + dot(picks[b, 0, 1], ret_p[r, :, at], 0, 0)
            + den[r, :, at].astype(F32)
        )

    with scope("bar"):
        pl.semaphore_wait(barrier, 6)
    for copy in metas:
        copy.start()
    with scope("load0"):
        loads[0].wait()
        send_near(OG)
        send_cross(OG, 0, chunks)
        loads[4].start()
        loads[3].start()
    with scope("find0"):
        find(0)
    with scope("pk_og"):
        pack_own(OG, BWD)
    with scope("norm1"):
        loads[1].wait()
        smalls[4].wait()
        normalise(st_v, bm_ref, HB, True)
        send_near(HB)
        send_cross(HB, 0, chunks // 2)
    with scope("pk_hb"):
        pack_own(HB, BWD)
    with scope("norm2"):
        loads[2].wait()
        smalls[5].wait()

        @pl.when(s < sections - 1)
        def _():
            x_copy.start()

        normalise(x_v, fm_ref, HF, False)
        send_near(HF)
        pack_own(HF, FWD)
    for j in range(1, 4):
        with scope(f"meta{j}"):
            remote(
                meta.at[0], meta.at[j], meta_send.at[j - 1], meta_recv.at[j - 1],
                s, unit(partner),
            ).wait_recv()
            find(j)
    def share(w, p):
        @pl.when(is_inner)
        def _():
            twin_share(w, p).start()

    def near_sent(q):
        @pl.when(is_outer)
        def _():
            remote(
                dense.at[q], near.at[q], S_NEAR.at[q], near_recv.at[q, 0], s, unit(partner)
            ).wait_send()

    def share_late(w, first, last):
        @pl.when(is_outer)
        def _():
            for p in range(first, last):
                twin_share(w, p).start()

    share(1, 0)
    with scope("over_og"):
        hand_over(OG, BWD)
        send_cross(HB, chunks // 2, chunks)
    share(1, 1)
    with scope("gat_og0"):
        gather(OG, BWD, 0)
    share(1, 2)
    with scope("over_hb"):
        hand_over(HB, BWD)
        send_cross(HF, 0, chunks)
    share(1, 3)
    with scope("gat_og1"):
        gather(OG, BWD, 1)
    share(0, 0)
    with scope("near_og"):
        near_sent(OG)
    share_late(1, 0, 2)
    with scope("near_hb"):
        near_sent(HB)
    share_late(1, 2, 4)
    with scope("gathered_og"):
        gathered(OG)

    with scope("pair"):
        for j in range(4):
            @pl.loop(0, width // tile)
            def _(n):
                at = cols(n, tile)
                scaled = bm_ref[2, :, at] * rows[OG, j, :, at].astype(F32)
                rows[OG, j, :, at] = (gate[BWD, j, :, 0:1] * scaled).astype(BF16)

    share(0, 1)
    with scope("wts"):
        loads[4].wait()
        twin_whole(1, 1 - c).wait_recv()

    with scope("agrad"):
        for h in range(2):
            @pl.loop(0, hidden // tile)
            def _(n):
                at = pl.ds(pl.multiple_of(h * hidden + n * tile, tile), tile)
                agrad[:, at] = dot(flat(OG), down[h, cols(n, tile), :], 1, 1)

    share(0, 2)
    with scope("near_hf"):
        near_sent(HF)
    share_late(0, 0, 4)
    with scope("gat_hb0"):
        gather(HB, BWD, 0)
    share(0, 3)
    with scope("over_hf"):
        hand_over(HF, FWD)
    with scope("gat_hb1"):
        gather(HB, BWD, 1)
    with scope("gathered_hb"):
        gathered(HB)
        loads[3].wait()
        twin_whole(0, 1 - c).wait_recv()

    with scope("pre"):
        for h in range(2):
            @pl.loop(0, hidden // tile)
            def _(n):
                at = pl.ds(pl.multiple_of(h * hidden + n * tile, tile), tile)
                pre = dot(flat(HB), up[h, :, cols(n, tile)])
                t = jnp.tanh(ROOT * (pre + CUBE * pre * pre * pre))
                slope = ROOT * (1.0 + 3.0 * CUBE * pre * pre)
                dgelu = 0.5 * (1.0 + t) + 0.5 * pre * (1.0 - t * t) * slope
                act[:, at] = (agrad[:, at] * dgelu).astype(BF16)

    with scope("partb"):
        @each_piece
        def _(n):
            at = cols(n, piece)
            give(
                BWD, n,
                dot(act[:, :hidden], up[0, at, :], 1, 1)
                + dot(act[:, hidden:], up[1, at, :], 1, 1),
            )

        @pl.when(is_outer)
        def _():
            give_late(BWD)

    with scope("gat_hf0"):
        gather(HF, FWD, 0)
    with scope("gat_hf1"):
        @pl.when(is_inner)
        def _():
            pl.loop(0, chunks - 1)(lambda n: pass_on(HF, FWD, 1, n))

    with scope("comb_b"):
        @pl.when(is_inner)
        def _():
            early = pieces // chunks
            pl.loop(0, early)(lambda n: combine(BWD, BWD, n))
            pass_on(HF, FWD, 1, chunks - 1)
            pl.loop(early, pieces)(lambda n: combine(BWD, BWD, n))
            give_late(BWD)

    with scope("gathered_hf"):
        gathered(HF)

    with scope("up"):
        for h in range(2):
            @pl.loop(0, hidden // tile)
            def _(n):
                at = pl.ds(pl.multiple_of(h * hidden + n * tile, tile), tile)
                pre = dot(flat(HF), up[h, :, cols(n, tile)])
                t = jnp.tanh(ROOT * (pre + CUBE * pre * pre * pre))
                act[:, at] = (0.5 * pre * (1.0 + t)).astype(BF16)

    weight = gate[FWD, :, :, 0:1].reshape(every, 1)

    with scope("down"):
        @each_piece
        def _(n):
            at = cols(n, piece)
            value = dot(act[:, :hidden], down[0, :, at]) + dot(act[:, hidden:], down[1, :, at])
            give(FWD, n, weight * value)

        give_late(FWD)

    with scope("comb_f"):
        @pl.when(is_inner)
        def _():
            pl.loop(0, pieces // 2)(lambda n: combine(FWD, FWD, n))

    @pl.when(s == 0)
    def _():
        next_ref[...] = jnp.zeros_like(next_ref)

    @pl.when(s == sections - 1)
    def _():
        grad_ref[...] = jnp.zeros_like(grad_ref)

    with scope("own_b"):
        wait_returned(BWD)
        got = den.at[BWD]
        remote(got, got, S_DEN, den_all_recv.at[0], s, unit(partner)).wait_recv()

        @each_piece
        def _(n):
            dh[:, cols(n, piece)] = own_total(BWD, BWD, n)

    with scope("fin_b"):
        for p in range(parts):
            @pl.loop(0, part // group)
            def _(i):
                at = pl.ds(pl.multiple_of(p * part + i * group, group), group)
                dnorm = dh[at, :] * (1.0 + bm_ref[1])
                normed = normed_b[at, :]
                one = jnp.mean(dnorm, axis=1, keepdims=True)
                two = jnp.mean(dnorm * normed, axis=1, keepdims=True)
                out_b[at, :] = (
                    dense[OG, at, :].astype(F32) + (dnorm - one - normed * two) * inv_b[at, 0:1]
                ).astype(BF16)

            @pl.when(s > 0)
            def _():
                back_copy(p).start()

    with scope("comb_f2"):
        @pl.when(is_inner)
        def _():
            pl.loop(pieces // 2, pieces)(lambda n: combine(FWD, FWD, n))

    def arrive(n):
        at = cols(n, piece)

        @pl.when(s > 0)
        def _():
            ahead_copy(n).wait_recv()
            next_ref[:, at] = x_prev[:, at] + m_in[:, at].astype(F32)

    with scope("own_f"):
        @pl.when(s > 0)
        def _():
            x_copy.wait_recv()

        wait_returned(FWD)
        lag = 2

        @each_piece
        def _(n):
            at = cols(n, piece)
            m_out[:, at] = (fm_ref[2, :, at] * own_total(FWD, FWD, n)).astype(BF16)

            @pl.when(s < sections - 1)
            def _():
                ahead_copy(n).start()

            @pl.when(n >= lag)
            def _():
                arrive(n - lag)

        for n in range(pieces - lag, pieces):
            arrive(n)

    with scope("tail_send"):
        def sent(sem, src):
            remote(src, src, sem, rows_recv.at[0], s, unit(partner)).wait_send()

        for copy in metas:
            copy.wait_send()
        for w in range(2):
            twin_whole(w, c).wait_send()
        sent(S_RETP, res.at[:, 1])

        @pl.when(is_outer)
        def _():
            sent(S_RETX, res.at[:, 2:4])

        @pl.when(is_inner)
        def _():
            sent(S_PART, snd_p)
            sent(S_CROSS, cross)
            sent(S_RELAY, relay)
            sent(S_DEN, comb)

    with scope("tail_hop"):
        @pl.when(s < sections - 1)
        def _():
            x_copy.wait_send()
            sent(S_AHEAD, m_out)
            remote(grad_ref, grad_ref, S_BACK, sb_recv.at[0], s, twin).wait_recv()

        @pl.when(s > 0)
        def _():
            sent(S_BACK, out_b)


def write_out(next_ref, grad_ref, next_hbm, grad_hbm, sem):
    copies = [
        pltpu.make_async_copy(next_ref, next_hbm, sem.at[0]),
        pltpu.make_async_copy(grad_ref, grad_hbm, sem.at[1]),
    ]
    for copy in copies:
        copy.start()
    for copy in copies:
        copy.wait()


def run_two_sided(
    section_inputs,
    stored_inputs,
    out_grads,
    fwd_routes,
    fwd_gates,
    fwd_modulation,
    bwd_routes,
    bwd_gates,
    bwd_modulation,
    up_weight,
    down_weight,
):
    sections, units = lax.axis_size("section"), lax.axis_size("expert")
    experts = units // 2
    count, width = section_inputs.shape[1:]
    hidden = up_weight.shape[3]
    capacity = -(-min(count, 5 * count // (2 * experts)) // 16) * 16
    every = 4 * capacity
    chunks, pieces = 4, 8

    def vmem(dtype, *shape):
        return pltpu.VMEM(shape, dtype)

    def dma(*shape):
        return pltpu.SemaphoreType.DMA(shape)

    scratch = [
        vmem(jnp.int32, 2, count),
        vmem(F32, 2, count),
        vmem(F32, 3, 1, width),
        vmem(jnp.int32, 2, count),
        vmem(F32, 2, count),
        vmem(F32, 3, 1, width),
        vmem(BF16, 2, width, hidden),
        vmem(BF16, 2, hidden, width),
        *[vmem(F32, count, width)] * 3,
        *[vmem(BF16, 3, count, width)] * 2,
        vmem(BF16, 3, 2, count, width),
        vmem(BF16, 3, capacity, width),
        vmem(BF16, 3, 2, capacity, width),
        vmem(BF16, 3, 4, capacity, width),
        vmem(BF16, every, 2 * hidden),
        vmem(F32, every, 2 * hidden),
        vmem(BF16, 2, 4, capacity, width),
        vmem(BF16, 2, capacity, width),
        vmem(BF16, 2, 2, capacity, width),
        vmem(BF16, 2, 2, count, width),
        vmem(BF16, 2, count, width),
        vmem(F32, count, width),
        vmem(F32, count, 128),
        *[vmem(BF16, count, width)] * 2,
        vmem(F32, count, width),
        vmem(BF16, count, width),
        vmem(F32, 4, 8, count),
        vmem(BF16, 2, 4, 2, capacity, count),
        vmem(F32, 2, 4, capacity, 128),
        dma(5),
        dma(6),
        dma(11),
        dma(3),
        dma(2),
        *[dma(3)] * 2,
        dma(1),
        dma(3, chunks),
        dma(3, 2, chunks),
        dma(3),
        dma(2),
        dma(2, pieces),
        dma(pieces),
        dma(1),
        dma(pieces),
        dma(1),
    ]
    in_vmem = pl.BlockSpec(memory_space=pltpu.VMEM)
    in_hbm = pl.BlockSpec(memory_space=pltpu.HBM)
    flops = 20 * every * width * hidden
    next_inputs, input_grads = pl.pallas_call(
        functools.partial(two_sided, sections, units, capacity, chunks, pieces),
        out_shape=(
            jax.ShapeDtypeStruct((count, width), F32),
            jax.ShapeDtypeStruct((count, width), BF16),
        ),
        in_specs=[in_hbm] * 11,
        out_specs=(in_vmem, in_vmem),
        scratch_shapes=scratch,
        compiler_params=pltpu.CompilerParams(
            collective_id=1, has_side_effects=True, vmem_limit_bytes=50 << 20
        ),
        cost_estimate=pl.CostEstimate(
            flops=flops, bytes_accessed=4 * width * hidden, transcendentals=0
        ),
    )(*[pltpu.with_memory_space_constraint(array, pltpu.HBM) for array in (
        section_inputs[0], stored_inputs[0], out_grads[0],
        fwd_routes[0].T, fwd_gates[0].T, jnp.transpose(fwd_modulation, (1, 0, 2)),
        bwd_routes[0].T, bwd_gates[0].T, jnp.transpose(bwd_modulation, (1, 0, 2)),
        up_weight[0, 0], down_weight[0, 0],
    )])
    next_inputs, input_grads = pl.pallas_call(
        write_out,
        out_shape=(
            jax.ShapeDtypeStruct((count, width), F32),
            jax.ShapeDtypeStruct((count, width), BF16),
        ),
        in_specs=[in_vmem] * 2,
        out_specs=(in_hbm, in_hbm),
        scratch_shapes=[dma(2)],
        compiler_params=pltpu.CompilerParams(vmem_limit_bytes=1 << 20),
    )(next_inputs, input_grads)
    return next_inputs[None], input_grads[None]


def on_device(*arrays):
    sides, inner_and_outer = 2, 2
    line = lax.axis_size("expert") == 2 * sides * inner_and_outer
    return (run_two_sided if line else run_many)(*arrays)


def solution(mesh):
    tokens = P("section", "expert", None)
    shared = P("section", None, None)
    weights = P("section", "expert", None, None)
    placed = (tokens,) * 5 + (shared,) + (tokens,) * 2 + (shared,) + (weights,) * 2
    return jax.shard_map(
        on_device,
        mesh=mesh,
        in_specs=placed,
        out_specs=(tokens, tokens),
        check_vma=False,
    )
```

```python
import functools

import jax
import jax.numpy as jnp
from jax import lax
from jax.experimental import pallas as pl
from jax.experimental.pallas import tpu as pltpu
from jax.sharding import PartitionSpec as P

norm_eps = 1e-06
F32, BF16 = jnp.float32, jnp.bfloat16
MESH = pl.DeviceIdType.MESH
ROOT, CUBE = 0.7978845608028654, 0.044715


def flip(index, mask, bits):
    total = 0
    for b in range(bits):
        bit = (index // (1 << b)) % 2
        total = total + (1 << b) * (1 - bit if mask >> b & 1 else bit)
    return total


def dot(a, b, ca=1, cb=0):
    return lax.dot_general(a, b, (((ca,), (cb,)), ((), ())), preferred_element_type=F32)


def slot_masks(routes, capacity, slots):
    count = routes.shape[0]
    lanes = lax.broadcasted_iota(jnp.int32, (count, 128), 1)
    hits = [routes[:, k : k + 1] == lanes for k in range(2)]
    choose = jnp.where(hits[0] | hits[1], 1.0, 0.0).astype(BF16)
    row = lax.broadcasted_iota(jnp.int32, (count, count), 0)
    col = lax.broadcasted_iota(jnp.int32, (count, count), 1)
    before = dot(jnp.where(col < row, 1.0, 0.0).astype(BF16), choose)
    places = lax.broadcasted_iota(jnp.int32, (count, slots), 1)
    masks = []
    for k in range(2):
        rank = jnp.sum(jnp.where(hits[k], before, 0.0), axis=1, keepdims=True)
        masks.append(places == routes[:, k : k + 1] * capacity + rank.astype(jnp.int32))
    return masks


def many_chips(
    sections, units, capacity,
    x_ref, st_ref, og_ref, fr_ref, fg_ref, fm_ref, br_ref, bg_ref, bm_ref, up_hbm, down_hbm,
    next_ref, grad_ref,
    up, down, snd_f, snd_r, snd_g, rcv_f, rcv_r, rcv_g, act, dgelu,
    px_f, px_b, pin_f, pin_b, ret_f, ret_b, rr_f, rr_b,
    hid, pair0, pair1, normed_b, inv_b, out_f, dh, out_b,
    w_sem, in_send, in_recv, fw_send, fw_recv, px_send, px_recv, rt_send, rt_recv,
    sf_send, sf_recv, sb_send, sb_recv,
):
    s, me = lax.axis_index("section"), lax.axis_index("expert")
    experts = units // 2
    bits = units.bit_length() - 1
    chip, core = me // 2, me % 2
    count, width = x_ref.shape
    half = width // 2
    hidden_units = up.shape[1]
    rows = units * capacity
    slots = experts * capacity
    tile = 256
    group = 16
    order = list(range(1, units))
    peer = {k: flip(me, k, bits) for k in order}

    w_up = pltpu.make_async_copy(up_hbm, up, w_sem.at[0])
    w_down = pltpu.make_async_copy(down_hbm, down, w_sem.at[1])
    w_up.start()
    w_down.start()

    barrier = pltpu.get_barrier_semaphore()
    for k in order:
        pl.semaphore_signal(barrier, inc=1, device_id=(s, peer[k]), device_id_type=MESH)
    for step in (1, sections - 1):
        pl.semaphore_signal(
            barrier, inc=1, device_id=((s + step) % sections, me), device_id_type=MESH
        )

    def remote(src, dst, send, recv, section, unit):
        return pltpu.make_async_remote_copy(
            src_ref=src, dst_ref=dst, send_sem=send, recv_sem=recv,
            device_id=(section, unit), device_id_type=MESH,
        )

    def inbound(phase, snd, rcv):
        copies = {}
        for k in order:
            d = peer[k]
            if k == 1:
                src, dst = snd.at[chip], rcv.at[:, me]
            else:
                src, dst = snd.at[d // 2, d % 2], rcv.at[d % 2, me]
            copies[k] = remote(src, dst, in_send.at[phase, k], in_recv.at[phase, k], s, d)
        return copies

    def hand_on(phase, rcv):
        copies = {}
        for k in order:
            if k > 1:
                block = rcv.at[core, peer[k]]
                copies[k] = remote(
                    block, block, fw_send.at[phase, k], fw_recv.at[phase, k], s, peer[1]
                )
        return copies

    def keep_own(snd, rcv):
        for h in range(2):
            rcv[h, me] = snd[chip, h]

    def receive(ins, fws):
        for k in order:
            ins[k].wait_recv()
            if k > 1:
                fws[k].start()
        for k in order:
            if k > 1:
                fws[k].wait_recv()

    def normalise(src, mod, keep):
        @pl.loop(0, count // group)
        def _(i):
            at = pl.ds(pl.multiple_of(i * group, group), group)
            x = src[at, :]
            centered = x - jnp.mean(x, axis=1, keepdims=True)
            inv = lax.rsqrt(jnp.mean(centered * centered, axis=1, keepdims=True) + norm_eps)
            normed = centered * inv
            hid[at, :] = (normed * (1.0 + mod[1:2, :]) + mod[0:1, :]).astype(BF16)
            if keep:
                normed_b[at, :] = normed
                inv_b[at, :] = jnp.broadcast_to(inv, (group, 128))

    def pack(terms, snd):
        for h in range(2):
            @pl.loop(0, half // tile)
            def _(n):
                src = pl.ds(pl.multiple_of(h * half + n * tile, tile), tile)
                value = sum(dot(mask, ref[:, src], 0, 0) for mask, ref in terms).astype(BF16)
                for e in range(experts):
                    snd[e, h, :, pl.ds(pl.multiple_of(n * tile, tile), tile)] = value[
                        e * capacity : (e + 1) * capacity, :
                    ]

    def onehot(mask):
        return jnp.where(mask, 1.0, 0.0).astype(BF16)

    normalise(x_ref, fm_ref, False)
    fwd = slot_masks(fr_ref[...], capacity, slots)
    pack([(onehot(fwd[0] | fwd[1]), hid)], snd_f)
    pl.semaphore_wait(barrier, units + 1)
    in_f, fw_f = inbound(0, snd_f, rcv_f), hand_on(0, rcv_f)
    for k in order:
        in_f[k].start()
    keep_own(snd_f, rcv_f)

    normalise(st_ref, bm_ref, True)
    bwd = slot_masks(br_ref[...], capacity, slots)
    bwd_hot = [onehot(mask) for mask in bwd]
    pack([(bwd_hot[0] + bwd_hot[1], hid)], snd_r)
    in_r, fw_r = inbound(1, snd_r, rcv_r), hand_on(1, rcv_r)
    for k in order:
        in_r[k].start()
    keep_own(snd_r, rcv_r)

    @pl.loop(0, count // group)
    def _(i):
        at = pl.ds(pl.multiple_of(i * group, group), group)
        scaled = bm_ref[2:3, :] * og_ref[at, :].astype(F32)
        pair0[at, :] = (bg_ref[at, 0:1] * scaled).astype(BF16)
        pair1[at, :] = (bg_ref[at, 1:2] * scaled).astype(BF16)

    pack([(bwd_hot[0], pair0), (bwd_hot[1], pair1)], snd_g)
    in_g, fw_g = inbound(2, snd_g, rcv_g), hand_on(2, rcv_g)
    for k in order:
        in_g[k].start()
    keep_own(snd_g, rcv_g)

    def flat(ref, h):
        return ref[h].reshape(rows, half)

    def cols(n, base=0):
        return pl.ds(pl.multiple_of(base + n * tile, tile), tile)

    def exchange(phase, px, pin, ret, result):
        def fill(dst, h):
            @pl.loop(0, half // tile)
            def _(n):
                value = result(h, n).astype(BF16).reshape(units, capacity, tile)
                dst[:, :, cols(n)] = value

        fill(px, 1 - core)
        swap = remote(px, pin, px_send.at[phase], px_recv.at[phase], s, peer[1])
        swap.start()
        fill(ret, core)
        swap.wait_recv()

        @pl.loop(0, units)
        def _(u):
            ret[u] = (ret[u].astype(F32) + pin[u].astype(F32)).astype(BF16)

        return swap

    def give_back(phase, ret, rr):
        copies = {}
        for k in order:
            copies[k] = remote(
                ret.at[peer[k]], rr.at[core, chip],
                rt_send.at[phase, k], rt_recv.at[phase, k], s, peer[k],
            )
            copies[k].start()
        rr[core, chip] = ret[me]
        return copies

    receive(in_f, fw_f)
    w_up.wait()
    w_down.wait()

    @pl.loop(0, hidden_units // tile)
    def _(n):
        pre = dot(flat(rcv_f, 0), up[:half, cols(n)]) + dot(flat(rcv_f, 1), up[half:, cols(n)])
        t = jnp.tanh(ROOT * (pre + CUBE * pre * pre * pre))
        act[:, cols(n)] = (0.5 * pre * (1.0 + t)).astype(BF16)

    swap_f = exchange(
        0, px_f, pin_f, ret_f, lambda h, n: dot(act[...], down[:, cols(n, h * half)])
    )
    back_f = give_back(0, ret_f, rr_f)

    receive(in_r, fw_r)

    @pl.loop(0, hidden_units // tile)
    def _(n):
        pre = dot(flat(rcv_r, 0), up[:half, cols(n)]) + dot(flat(rcv_r, 1), up[half:, cols(n)])
        t = jnp.tanh(ROOT * (pre + CUBE * pre * pre * pre))
        slope = ROOT * (1.0 + 3.0 * CUBE * pre * pre)
        dgelu[:, cols(n)] = 0.5 * (1.0 + t) + 0.5 * pre * (1.0 - t * t) * slope

    receive(in_g, fw_g)

    @pl.loop(0, hidden_units // tile)
    def _(n):
        back = dot(flat(rcv_g, 0), down[cols(n), :half], 1, 1) + dot(
            flat(rcv_g, 1), down[cols(n), half:], 1, 1
        )
        act[:, cols(n)] = (back * dgelu[:, cols(n)]).astype(BF16)

    swap_b = exchange(
        1, px_b, pin_b, ret_b, lambda h, n: dot(act[...], up[cols(n, h * half), :], 1, 1)
    )
    back_b = give_back(1, ret_b, rr_b)

    weight = sum(jnp.where(fwd[k], fg_ref[:, k : k + 1], 0.0) for k in range(2))
    high = weight.astype(BF16)
    low = (weight - high.astype(F32)).astype(BF16)
    for k in order:
        back_f[k].wait_recv()
    sends_f = []
    for h in range(2):
        side = pl.ds(h * half, half)

        @pl.loop(0, half // tile)
        def _(n):
            got = rr_f[h, :, :, cols(n)].reshape(slots, tile)
            moe = dot(high, got) + dot(low, got)
            at = cols(n, h * half)
            out_f[:, at] = x_ref[:, at] + fm_ref[2:3, at] * moe

        copy = remote(
            out_f.at[:, side], next_ref.at[:, side], sf_send.at[h], sf_recv.at[h],
            (s + 1) % sections, me,
        )
        sends_f.append(copy)

        @pl.when(s < sections - 1)
        def _():
            copy.start()

    @pl.when(s == 0)
    def _():
        next_ref[...] = jnp.zeros_like(next_ref)

    @pl.when(s == sections - 1)
    def _():
        grad_ref[...] = jnp.zeros_like(grad_ref)

    for k in order:
        back_b[k].wait_recv()
    both = bwd_hot[0] + bwd_hot[1]
    for h in range(2):
        @pl.loop(0, half // tile)
        def _(n):
            got = rr_b[h, :, :, cols(n)].reshape(slots, tile)
            dh[:, cols(n, h * half)] = dot(both, got)

    pieces = 4
    part = count // pieces
    sends_b = []
    for p in range(pieces):
        @pl.loop(0, part // group)
        def _(i):
            at = pl.ds(pl.multiple_of(p * part + i * group, group), group)
            dnorm = dh[at, :] * (1.0 + bm_ref[1:2, :])
            normed = normed_b[at, :]
            one = jnp.mean(dnorm, axis=1, keepdims=True)
            two = jnp.mean(dnorm * normed, axis=1, keepdims=True)
            out_b[at, :] = (
                og_ref[at, :].astype(F32) + (dnorm - one - normed * two) * inv_b[at, 0:1]
            ).astype(BF16)

        piece = pl.ds(p * part, part)
        copy = remote(
            out_b.at[piece], grad_ref.at[piece], sb_send.at[p], sb_recv.at[p],
            (s + sections - 1) % sections, me,
        )
        sends_b.append(copy)

        @pl.when(s > 0)
        def _():
            copy.start()

    for copies in (in_f, in_r, in_g, fw_f, fw_r, fw_g, back_f, back_b):
        for copy in copies.values():
            copy.wait_send()
    swap_f.wait_send()
    swap_b.wait_send()

    @pl.when(s < sections - 1)
    def _():
        for copy in sends_f:
            copy.wait_send()
        for copy in sends_b:
            copy.wait_recv()

    @pl.when(s > 0)
    def _():
        for copy in sends_f:
            copy.wait_recv()
        for copy in sends_b:
            copy.wait_send()


def run_many(
    section_inputs,
    stored_inputs,
    out_grads,
    fwd_routes,
    fwd_gates,
    fwd_modulation,
    bwd_routes,
    bwd_gates,
    bwd_modulation,
    up_weight,
    down_weight,
):
    sections, units = lax.axis_size("section"), lax.axis_size("expert")
    experts = units // 2
    count, width = section_inputs.shape[1:]
    hidden_units = up_weight.shape[3]
    half = width // 2
    capacity = -(-min(count, 5 * count // (2 * experts)) // 16) * 16
    rows = units * capacity

    def vmem(dtype, *shape):
        return pltpu.VMEM(shape, dtype)

    def dma(*shape):
        return pltpu.SemaphoreType.DMA(shape)

    scratch = [
        vmem(BF16, width, hidden_units),
        vmem(BF16, hidden_units, width),
        *[vmem(BF16, experts, 2, capacity, half)] * 3,
        *[vmem(BF16, 2, units, capacity, half)] * 3,
        vmem(BF16, rows, hidden_units),
        vmem(F32, rows, hidden_units),
        *[vmem(BF16, units, capacity, half)] * 6,
        *[vmem(BF16, 2, experts, capacity, half)] * 2,
        *[vmem(BF16, count, width)] * 3,
        vmem(F32, count, width),
        vmem(F32, count, 128),
        *[vmem(F32, count, width)] * 2,
        vmem(BF16, count, width),
        dma(2),
        *[dma(3, units)] * 4,
        *[dma(2)] * 2,
        *[dma(2, units)] * 2,
        *[dma(2)] * 2,
        *[dma(4)] * 2,
    ]
    in_vmem = pl.BlockSpec(memory_space=pltpu.VMEM)
    in_hbm = pl.BlockSpec(memory_space=pl.ANY)
    flops = 10 * rows * width * hidden_units
    next_inputs, input_grads = pl.pallas_call(
        functools.partial(many_chips, sections, units, capacity),
        out_shape=(
            jax.ShapeDtypeStruct((count, width), F32),
            jax.ShapeDtypeStruct((count, width), BF16),
        ),
        in_specs=[in_vmem] * 9 + [in_hbm] * 2,
        out_specs=(in_vmem, in_vmem),
        scratch_shapes=scratch,
        compiler_params=pltpu.CompilerParams(
            collective_id=0, has_side_effects=True, vmem_limit_bytes=67043328
        ),
        cost_estimate=pl.CostEstimate(
            flops=flops, bytes_accessed=4 * width * hidden_units, transcendentals=0
        ),
    )(
        section_inputs[0], stored_inputs[0], out_grads[0], fwd_routes[0], fwd_gates[0],
        fwd_modulation[0], bwd_routes[0], bwd_gates[0], bwd_modulation[0],
        up_weight[0, 0], down_weight[0, 0],
    )
    return next_inputs[None], input_grads[None]


def two_sided(
    sections, units, capacity, chunks, pieces,
    x_hbm, st_hbm, og_hbm, fr_hbm, fg_hbm, fm_hbm, br_hbm, bg_hbm, bm_hbm, up_hbm, down_hbm,
    next_ref, grad_ref,
    fr_ref, fg_ref, fm_ref, br_ref, bg_ref, bm_ref,
    up, down, x_v, x_prev, st_v, dense, near, cross, snd_p, relay, rows, act, agrad,
    res, ret_p, ret_x, comb, den, normed_b, inv_b, m_out, m_in, dh, out_b,
    meta, picks, gate,
    load_sem, small_sem, send_sem, near_send, w_recv, meta_send, meta_recv, x_recv, near_recv,
    cross_recv, rows_recv, retp_recv, retx_recv, den_recv, den_all_recv, sf_recv, sb_recv,
):
    s, me = lax.axis_index("section"), lax.axis_index("expert")
    z, c = me // 2, me % 2
    odd, side = z % 2, z // 2
    inner = odd + side - 2 * odd * side
    seat = 1 - inner
    partner = z + 1 - 2 * odd
    crossing = [2 - side, 3 - 3 * side]
    is_inner, is_outer = inner == 1, inner == 0
    count, width = x_v.shape
    hidden = up.shape[2]
    every = 4 * capacity
    tile, group = 256, 16
    chunk, piece = width // chunks, width // pieces
    OG, HB, HF = 0, 1, 2
    FWD, BWD = 0, 1
    scope = jax.named_scope

    def unit(chip):
        return 2 * chip + c

    def remote(src, dst, send, recv, section, to):
        return pltpu.make_async_remote_copy(
            src_ref=src, dst_ref=dst, send_sem=send, recv_sem=recv,
            device_id=(section, to), device_id_type=MESH,
        )

    def cols(n, size):
        return pl.ds(pl.multiple_of(n * size, size), size)

    barrier = pltpu.get_barrier_semaphore()
    for chip in (partner, crossing[0], crossing[1]):
        pl.semaphore_signal(barrier, inc=1, device_id=(s, unit(chip)), device_id_type=MESH)
    twin = me + 1 - 2 * c
    pl.semaphore_signal(barrier, inc=1, device_id=(s, twin), device_id_type=MESH)
    for step in (1, sections - 1):
        pl.semaphore_signal(
            barrier, inc=1, device_id=((s + step) % sections, me), device_id_type=MESH
        )

    loads = [
        pltpu.make_async_copy(og_hbm, dense.at[OG], load_sem.at[0]),
        pltpu.make_async_copy(st_hbm, st_v, load_sem.at[1]),
        pltpu.make_async_copy(x_hbm, x_v, load_sem.at[2]),
        pltpu.make_async_copy(up_hbm, up.at[c], load_sem.at[3]),
        pltpu.make_async_copy(down_hbm, down.at[c], load_sem.at[4]),
    ]
    smalls = [
        pltpu.make_async_copy(src, dst, small_sem.at[k])
        for k, (src, dst) in enumerate([
            (fr_hbm, fr_ref), (fg_hbm, fg_ref), (br_hbm, br_ref), (bg_hbm, bg_ref),
            (bm_hbm, bm_ref), (fm_hbm, fm_ref),
        ])
    ]
    for load in smalls[:4] + loads[:3] + smalls[4:]:
        load.start()

    for load in smalls[:4]:
        load.wait()
    meta[0, 0:2, :] = fr_ref[...].astype(F32)
    meta[0, 2:4, :] = fg_ref[...]
    meta[0, 4:6, :] = br_ref[...].astype(F32)
    meta[0, 6:8, :] = bg_ref[...]

    metas = [
        remote(meta.at[0], meta.at[1], meta_send.at[0], meta_recv.at[0], s, unit(partner)),
        remote(
            meta.at[0], meta.at[2 + seat], meta_send.at[1], meta_recv.at[1 + seat],
            s, unit(crossing[0]),
        ),
        remote(
            meta.at[0], meta.at[2 + seat], meta_send.at[2], meta_recv.at[1 + seat],
            s, unit(crossing[1]),
        ),
    ]
    shares = 4
    S_UP, S_DOWN, S_CROSS, S_PART, S_RELAY, S_RETP, S_RETX, S_DEN, S_AHEAD, S_BACK, S_X = [
        send_sem.at[k] for k in range(11)
    ]
    S_NEAR = near_send

    def twin_share(w, p):
        src, dst, sem = ((up_hbm, up, S_UP), (down_hbm, down, S_DOWN))[w]
        size = src.shape[0] // shares
        at = pl.ds(p * size, size)
        return remote(src.at[at], dst.at[c, at], sem, w_recv.at[w], s, twin)

    def twin_whole(w, slot):
        src, dst, sem = ((up_hbm, up, S_UP), (down_hbm, down, S_DOWN))[w]
        return remote(src, dst.at[slot], sem, w_recv.at[w], s, twin)

    def near_copy(q, n):
        at = cols(n, chunk)
        return remote(
            dense.at[q, :, at], near.at[q, :, at],
            S_NEAR.at[q], near_recv.at[q, n], s, unit(partner),
        )

    def cross_copy(q, i, n):
        at = cols(n, chunk)
        src = dense if i == 0 else near
        return remote(
            src.at[q, :, at], cross.at[q, i, :, at],
            S_CROSS, cross_recv.at[q, i, n], s, unit(crossing[0]),
        )

    def part_copy(q, n):
        at = cols(n, chunk)
        return remote(
            snd_p.at[q, :, at], rows.at[q, 1, :, at],
            S_PART, rows_recv.at[q], s, unit(partner),
        )

    def relay_copy(q, i, n):
        at = cols(n, chunk)
        return remote(
            relay.at[q, i, :, at], rows.at[q, 2 + i, :, at],
            S_RELAY, rows_recv.at[q], s, unit(partner),
        )

    def retp_copy(r, n):
        at = cols(n, piece)
        return remote(
            res.at[r, 1, :, at], ret_p.at[r, :, at],
            S_RETP, retp_recv.at[r], s, unit(partner),
        )

    def retx_copy(r, i, n):
        at = cols(n, piece)
        return remote(
            res.at[r, 2 + i, :, at], ret_x.at[r, i, :, at],
            S_RETX, retx_recv.at[r, n], s, unit(partner),
        )

    def den_copy(r, i, n):
        at = cols(n, piece)
        return remote(
            comb.at[r, i, :, at], den.at[r, :, at],
            S_DEN, den_all_recv.at[0] if r == BWD else den_recv.at[n], s, unit(crossing[i]),
        )

    x_copy = remote(x_v, x_prev, S_X, x_recv.at[0], (s + 1) % sections, me)

    def ahead_copy(n):
        at = cols(n, piece)
        return remote(
            m_out.at[:, at], m_in.at[:, at], S_AHEAD, sf_recv.at[n],
            (s + 1) % sections, me,
        )

    parts = 4
    part = count // parts

    def back_copy(p):
        at = cols(p, part)
        return remote(
            out_b.at[at], grad_ref.at[at], S_BACK, sb_recv.at[0],
            (s + sections - 1) % sections, me,
        )

    def each_chunk(body):
        pl.loop(0, chunks)(body)

    def each_piece(body):
        pl.loop(0, pieces)(body)

    row16 = lax.broadcasted_iota(jnp.int32, (16, count), 0)
    named = jnp.where(row16 % 2 == 0, z, partner).astype(F32)
    forward = row16 < 2
    earlier = lax.broadcasted_iota(jnp.int32, (count, count), 0)
    later = lax.broadcasted_iota(jnp.int32, (count, count), 1)
    upper = jnp.where(earlier < later, 1.0, 0.0).astype(BF16)
    places = lax.broadcasted_iota(jnp.int32, (capacity, count), 0).astype(F32)

    def find(j):
        first = jnp.where(forward, meta[j, 0:1, :], meta[j, 4:5, :]) == named
        second = jnp.where(forward, meta[j, 1:2, :], meta[j, 5:6, :]) == named
        weight = jnp.where(
            first,
            jnp.where(forward, meta[j, 2:3, :], meta[j, 6:7, :]),
            jnp.where(forward, meta[j, 3:4, :], meta[j, 7:8, :]),
        )
        chosen = first | second
        before = dot(jnp.where(chosen, 1.0, 0.0).astype(BF16), upper)
        place = jnp.where(chosen, before, -1.0)
        for b in range(2):
            for k in range(2):
                row = slice(2 * b + k, 2 * b + k + 1)
                hit = places == place[row]
                picks[b, j, k] = jnp.where(hit, 1.0, 0.0).astype(BF16)
                if k == 0:
                    value = jnp.sum(jnp.where(hit, weight[row], 0.0), axis=1, keepdims=True)
                    gate[b, j] = jnp.broadcast_to(value, (capacity, 128))

    def pack_own(q, b):
        @each_chunk
        def _(n):
            at = cols(n, chunk)

            @pl.when(is_inner)
            def _():
                snd_p[q, :, at] = dot(picks[b, 0, 1], dense[q, :, at]).astype(BF16)
                part_copy(q, n).start()

            rows[q, 0, :, at] = dot(picks[b, 0, 0], dense[q, :, at]).astype(BF16)

    def normalise(src, mod, q, keep):
        @pl.loop(0, count // group)
        def _(i):
            at = pl.ds(pl.multiple_of(i * group, group), group)
            x = src[at, :]
            centered = x - jnp.mean(x, axis=1, keepdims=True)
            inv = lax.rsqrt(jnp.mean(centered * centered, axis=1, keepdims=True) + norm_eps)
            normed = centered * inv
            dense[q, at, :] = (normed * (1.0 + mod[1]) + mod[0]).astype(BF16)
            if keep:
                normed_b[at, :] = normed
                inv_b[at, :] = jnp.broadcast_to(inv, (group, 128))

    def send_near(q):
        @pl.when(is_outer)
        def _():
            each_chunk(lambda n: near_copy(q, n).start())

    def send_cross(q, first, last):
        @pl.when(is_inner)
        def _():
            pl.loop(first, last)(lambda n: cross_copy(q, 0, n).start())

    def hand_over(q, b):
        @pl.when(is_inner)
        def _():
            @each_chunk
            def _(n):
                at = cols(n, chunk)
                near_copy(q, n).wait_recv()
                cross_copy(q, 1, n).start()
                rows[q, 1, :, at] = dot(picks[b, 1, 0], near[q, :, at]).astype(BF16)

    def pass_on(q, b, i, n):
        at = cols(n, chunk)
        cross_copy(q, i, n).wait_recv()
        relay[q, i, :, at] = dot(picks[b, 2 + i, 1], cross[q, i, :, at]).astype(BF16)
        relay_copy(q, i, n).start()
        rows[q, 2 + i, :, at] = dot(picks[b, 2 + i, 0], cross[q, i, :, at]).astype(BF16)

    def gather(q, b, i):
        @pl.when(is_inner)
        def _():
            each_chunk(lambda n: pass_on(q, b, i, n))

    def gathered(q):
        @pl.when(is_outer)
        def _():
            got = rows.at[q, 1:4]
            remote(got, got, S_RELAY, rows_recv.at[q], s, unit(partner)).wait_recv()

    def flat(q):
        return rows[q].reshape(every, width)

    def give(r, n, value):
        at = cols(n, piece)
        value = value.astype(BF16).reshape(4, capacity, piece)
        for j in range(4):
            res[r, j, :, at] = value[j]

        @pl.when(is_outer)
        def _():
            for i in range(2):
                retx_copy(r, i, n).start()

    def give_late(r):
        each_piece(lambda n: retp_copy(r, n).start())

    def combine(r, b, n):
        at = cols(n, piece)
        got = ret_x.at[r, :, :, at]
        remote(got, got, S_RETX, retx_recv.at[r, n], s, unit(partner)).wait_recv()
        for i in (1, 0):
            total = dot(picks[b, 2 + i, 0], res[r, 2 + i, :, at], 0, 0) + dot(
                picks[b, 2 + i, 1], ret_x[r, i, :, at], 0, 0
            )
            comb[r, i, :, at] = total.astype(BF16)
            den_copy(r, i, n).start()

    def wait_returned(r):
        got = ret_p.at[r]
        remote(got, got, S_RETP, retp_recv.at[r], s, unit(partner)).wait_recv()

    def own_total(r, b, n):
        at = cols(n, piece)
        if r == FWD:
            den_copy(r, 0, n).wait_recv()
        return (
            dot(picks[b, 0, 0], res[r, 0, :, at], 0, 0)
            + dot(picks[b, 0, 1], ret_p[r, :, at], 0, 0)
            + den[r, :, at].astype(F32)
        )

    with scope("bar"):
        pl.semaphore_wait(barrier, 6)
    for copy in metas:
        copy.start()
    with scope("load0"):
        loads[0].wait()
        send_near(OG)
        send_cross(OG, 0, chunks)
        loads[4].start()
        loads[3].start()
    with scope("find0"):
        find(0)
    with scope("pk_og"):
        pack_own(OG, BWD)
    with scope("norm1"):
        loads[1].wait()
        smalls[4].wait()
        normalise(st_v, bm_ref, HB, True)
        send_near(HB)
        send_cross(HB, 0, chunks // 2)
    with scope("pk_hb"):
        pack_own(HB, BWD)
    with scope("norm2"):
        loads[2].wait()
        smalls[5].wait()

        @pl.when(s < sections - 1)
        def _():
            x_copy.start()

        normalise(x_v, fm_ref, HF, False)
        send_near(HF)
        pack_own(HF, FWD)
    for j in range(1, 4):
        with scope(f"meta{j}"):
            remote(
                meta.at[0], meta.at[j], meta_send.at[j - 1], meta_recv.at[j - 1],
                s, unit(partner),
            ).wait_recv()
            find(j)
    def share(w, p):
        @pl.when(is_inner)
        def _():
            twin_share(w, p).start()

    def near_sent(q):
        @pl.when(is_outer)
        def _():
            remote(
                dense.at[q], near.at[q], S_NEAR.at[q], near_recv.at[q, 0], s, unit(partner)
            ).wait_send()

    def share_late(w, first, last):
        @pl.when(is_outer)
        def _():
            for p in range(first, last):
                twin_share(w, p).start()

    share(1, 0)
    with scope("over_og"):
        hand_over(OG, BWD)
        send_cross(HB, chunks // 2, chunks)
    share(1, 1)
    with scope("gat_og0"):
        gather(OG, BWD, 0)
    share(1, 2)
    with scope("over_hb"):
        hand_over(HB, BWD)
        send_cross(HF, 0, chunks)
    share(1, 3)
    with scope("gat_og1"):
        gather(OG, BWD, 1)
    share(0, 0)
    with scope("near_og"):
        near_sent(OG)
    share_late(1, 0, 2)
    with scope("near_hb"):
        near_sent(HB)
    share_late(1, 2, 4)
    with scope("gathered_og"):
        gathered(OG)

    with scope("pair"):
        for j in range(4):
            @pl.loop(0, width // tile)
            def _(n):
                at = cols(n, tile)
                scaled = bm_ref[2, :, at] * rows[OG, j, :, at].astype(F32)
                rows[OG, j, :, at] = (gate[BWD, j, :, 0:1] * scaled).astype(BF16)

    share(0, 1)
    with scope("wts"):
        loads[4].wait()
        twin_whole(1, 1 - c).wait_recv()

    with scope("agrad"):
        for h in range(2):
            @pl.loop(0, hidden // tile)
            def _(n):
                at = pl.ds(pl.multiple_of(h * hidden + n * tile, tile), tile)
                agrad[:, at] = dot(flat(OG), down[h, cols(n, tile), :], 1, 1)

    share(0, 2)
    with scope("near_hf"):
        near_sent(HF)
    share_late(0, 0, 4)
    with scope("gat_hb0"):
        gather(HB, BWD, 0)
    share(0, 3)
    with scope("over_hf"):
        hand_over(HF, FWD)
    with scope("gat_hb1"):
        gather(HB, BWD, 1)
    with scope("gathered_hb"):
        gathered(HB)
        loads[3].wait()
        twin_whole(0, 1 - c).wait_recv()

    with scope("pre"):
        for h in range(2):
            @pl.loop(0, hidden // tile)
            def _(n):
                at = pl.ds(pl.multiple_of(h * hidden + n * tile, tile), tile)
                pre = dot(flat(HB), up[h, :, cols(n, tile)])
                t = jnp.tanh(ROOT * (pre + CUBE * pre * pre * pre))
                slope = ROOT * (1.0 + 3.0 * CUBE * pre * pre)
                dgelu = 0.5 * (1.0 + t) + 0.5 * pre * (1.0 - t * t) * slope
                act[:, at] = (agrad[:, at] * dgelu).astype(BF16)

    with scope("partb"):
        @each_piece
        def _(n):
            at = cols(n, piece)
            give(
                BWD, n,
                dot(act[:, :hidden], up[0, at, :], 1, 1)
                + dot(act[:, hidden:], up[1, at, :], 1, 1),
            )

        @pl.when(is_outer)
        def _():
            give_late(BWD)

    with scope("gat_hf0"):
        gather(HF, FWD, 0)
    with scope("gat_hf1"):
        @pl.when(is_inner)
        def _():
            pl.loop(0, chunks - 1)(lambda n: pass_on(HF, FWD, 1, n))

    with scope("comb_b"):
        @pl.when(is_inner)
        def _():
            early = pieces // chunks
            pl.loop(0, early)(lambda n: combine(BWD, BWD, n))
            pass_on(HF, FWD, 1, chunks - 1)
            pl.loop(early, pieces)(lambda n: combine(BWD, BWD, n))
            give_late(BWD)

    with scope("gathered_hf"):
        gathered(HF)

    with scope("up"):
        for h in range(2):
            @pl.loop(0, hidden // tile)
            def _(n):
                at = pl.ds(pl.multiple_of(h * hidden + n * tile, tile), tile)
                pre = dot(flat(HF), up[h, :, cols(n, tile)])
                t = jnp.tanh(ROOT * (pre + CUBE * pre * pre * pre))
                act[:, at] = (0.5 * pre * (1.0 + t)).astype(BF16)

    weight = gate[FWD, :, :, 0:1].reshape(every, 1)

    with scope("down"):
        @each_piece
        def _(n):
            at = cols(n, piece)
            value = dot(act[:, :hidden], down[0, :, at]) + dot(act[:, hidden:], down[1, :, at])
            give(FWD, n, weight * value)

        give_late(FWD)

    with scope("comb_f"):
        @pl.when(is_inner)
        def _():
            pl.loop(0, pieces // 2)(lambda n: combine(FWD, FWD, n))

    @pl.when(s == 0)
    def _():
        next_ref[...] = jnp.zeros_like(next_ref)

    @pl.when(s == sections - 1)
    def _():
        grad_ref[...] = jnp.zeros_like(grad_ref)

    with scope("own_b"):
        wait_returned(BWD)
        got = den.at[BWD]
        remote(got, got, S_DEN, den_all_recv.at[0], s, unit(partner)).wait_recv()

        @each_piece
        def _(n):
            dh[:, cols(n, piece)] = own_total(BWD, BWD, n)

    with scope("fin_b"):
        for p in range(parts):
            @pl.loop(0, part // group)
            def _(i):
                at = pl.ds(pl.multiple_of(p * part + i * group, group), group)
                dnorm = dh[at, :] * (1.0 + bm_ref[1])
                normed = normed_b[at, :]
                one = jnp.mean(dnorm, axis=1, keepdims=True)
                two = jnp.mean(dnorm * normed, axis=1, keepdims=True)
                out_b[at, :] = (
                    dense[OG, at, :].astype(F32) + (dnorm - one - normed * two) * inv_b[at, 0:1]
                ).astype(BF16)

            @pl.when(s > 0)
            def _():
                back_copy(p).start()

    with scope("comb_f2"):
        @pl.when(is_inner)
        def _():
            pl.loop(pieces // 2, pieces)(lambda n: combine(FWD, FWD, n))

    def arrive(n):
        at = cols(n, piece)

        @pl.when(s > 0)
        def _():
            ahead_copy(n).wait_recv()
            next_ref[:, at] = x_prev[:, at] + m_in[:, at].astype(F32)

    with scope("own_f"):
        @pl.when(s > 0)
        def _():
            x_copy.wait_recv()

        wait_returned(FWD)
        lag = 2

        @each_piece
        def _(n):
            at = cols(n, piece)
            m_out[:, at] = (fm_ref[2, :, at] * own_total(FWD, FWD, n)).astype(BF16)

            @pl.when(s < sections - 1)
            def _():
                ahead_copy(n).start()

            @pl.when(n >= lag)
            def _():
                arrive(n - lag)

        for n in range(pieces - lag, pieces):
            arrive(n)

    with scope("tail_send"):
        def sent(sem, src):
            remote(src, src, sem, rows_recv.at[0], s, unit(partner)).wait_send()

        for copy in metas:
            copy.wait_send()
        for w in range(2):
            twin_whole(w, c).wait_send()
        sent(S_RETP, res.at[:, 1])

        @pl.when(is_outer)
        def _():
            sent(S_RETX, res.at[:, 2:4])

        @pl.when(is_inner)
        def _():
            sent(S_PART, snd_p)
            sent(S_CROSS, cross)
            sent(S_RELAY, relay)
            sent(S_DEN, comb)

    with scope("tail_hop"):
        @pl.when(s < sections - 1)
        def _():
            x_copy.wait_send()
            sent(S_AHEAD, m_out)
            remote(grad_ref, grad_ref, S_BACK, sb_recv.at[0], s, twin).wait_recv()

        @pl.when(s > 0)
        def _():
            sent(S_BACK, out_b)


def write_out(next_ref, grad_ref, next_hbm, grad_hbm, sem):
    copies = [
        pltpu.make_async_copy(next_ref, next_hbm, sem.at[0]),
        pltpu.make_async_copy(grad_ref, grad_hbm, sem.at[1]),
    ]
    for copy in copies:
        copy.start()
    for copy in copies:
        copy.wait()


def run_two_sided(
    section_inputs,
    stored_inputs,
    out_grads,
    fwd_routes,
    fwd_gates,
    fwd_modulation,
    bwd_routes,
    bwd_gates,
    bwd_modulation,
    up_weight,
    down_weight,
):
    sections, units = lax.axis_size("section"), lax.axis_size("expert")
    experts = units // 2
    count, width = section_inputs.shape[1:]
    hidden = up_weight.shape[3]
    capacity = -(-min(count, 5 * count // (2 * experts)) // 16) * 16
    every = 4 * capacity
    chunks, pieces = 4, 8

    def vmem(dtype, *shape):
        return pltpu.VMEM(shape, dtype)

    def dma(*shape):
        return pltpu.SemaphoreType.DMA(shape)

    scratch = [
        vmem(jnp.int32, 2, count),
        vmem(F32, 2, count),
        vmem(F32, 3, 1, width),
        vmem(jnp.int32, 2, count),
        vmem(F32, 2, count),
        vmem(F32, 3, 1, width),
        vmem(BF16, 2, width, hidden),
        vmem(BF16, 2, hidden, width),
        *[vmem(F32, count, width)] * 3,
        *[vmem(BF16, 3, count, width)] * 2,
        vmem(BF16, 3, 2, count, width),
        vmem(BF16, 3, capacity, width),
        vmem(BF16, 3, 2, capacity, width),
        vmem(BF16, 3, 4, capacity, width),
        vmem(BF16, every, 2 * hidden),
        vmem(F32, every, 2 * hidden),
        vmem(BF16, 2, 4, capacity, width),
        vmem(BF16, 2, capacity, width),
        vmem(BF16, 2, 2, capacity, width),
        vmem(BF16, 2, 2, count, width),
        vmem(BF16, 2, count, width),
        vmem(F32, count, width),
        vmem(F32, count, 128),
        *[vmem(BF16, count, width)] * 2,
        vmem(F32, count, width),
        vmem(BF16, count, width),
        vmem(F32, 4, 8, count),
        vmem(BF16, 2, 4, 2, capacity, count),
        vmem(F32, 2, 4, capacity, 128),
        dma(5),
        dma(6),
        dma(11),
        dma(3),
        dma(2),
        *[dma(3)] * 2,
        dma(1),
        dma(3, chunks),
        dma(3, 2, chunks),
        dma(3),
        dma(2),
        dma(2, pieces),
        dma(pieces),
        dma(1),
        dma(pieces),
        dma(1),
    ]
    in_vmem = pl.BlockSpec(memory_space=pltpu.VMEM)
    in_hbm = pl.BlockSpec(memory_space=pltpu.HBM)
    flops = 20 * every * width * hidden
    next_inputs, input_grads = pl.pallas_call(
        functools.partial(two_sided, sections, units, capacity, chunks, pieces),
        out_shape=(
            jax.ShapeDtypeStruct((count, width), F32),
            jax.ShapeDtypeStruct((count, width), BF16),
        ),
        in_specs=[in_hbm] * 11,
        out_specs=(in_vmem, in_vmem),
        scratch_shapes=scratch,
        compiler_params=pltpu.CompilerParams(
            collective_id=1, has_side_effects=True, vmem_limit_bytes=50 << 20
        ),
        cost_estimate=pl.CostEstimate(
            flops=flops, bytes_accessed=4 * width * hidden, transcendentals=0
        ),
    )(*[pltpu.with_memory_space_constraint(array, pltpu.HBM) for array in (
        section_inputs[0], stored_inputs[0], out_grads[0],
        fwd_routes[0].T, fwd_gates[0].T, jnp.transpose(fwd_modulation, (1, 0, 2)),
        bwd_routes[0].T, bwd_gates[0].T, jnp.transpose(bwd_modulation, (1, 0, 2)),
        up_weight[0, 0], down_weight[0, 0],
    )])
    next_inputs, input_grads = pl.pallas_call(
        write_out,
        out_shape=(
            jax.ShapeDtypeStruct((count, width), F32),
            jax.ShapeDtypeStruct((count, width), BF16),
        ),
        in_specs=[in_vmem] * 2,
        out_specs=(in_hbm, in_hbm),
        scratch_shapes=[dma(2)],
        compiler_params=pltpu.CompilerParams(vmem_limit_bytes=1 << 20),
    )(next_inputs, input_grads)
    return next_inputs[None], input_grads[None]


def on_device(*arrays):
    sides, inner_and_outer = 2, 2
    line = lax.axis_size("expert") == 2 * sides * inner_and_outer
    return (run_two_sided if line else run_many)(*arrays)


def solution(mesh):
    tokens = P("section", "expert", None)
    shared = P("section", None, None)
    weights = P("section", "expert", None, None)
    placed = (tokens,) * 5 + (shared,) + (tokens,) * 2 + (shared,) + (weights,) * 2
    return jax.shard_map(
        on_device,
        mesh=mesh,
        in_specs=placed,
        out_specs=(tokens, tokens),
        check_vma=False,
    )
```
